256 devices in a mesh: shock: 32 (over z, x_lo, core), trans: 8 (over x_hi, y).
Axes of the slice: x: 4 (x_hi: 2, x_lo: 2; x = x_hi * 2 + x_lo), y: 4, z: 8, core: 2. Of those that a mesh axis runs over, the one named last changes fastest.
Arguments:
- displacement: float32 [3, 65536], P(None, ('shock', 'trans')), may hold values from -0.32 to 0.32
- velocity: float32 [3, 65536], P(None, ('shock', 'trans')), may hold values from -4 to 4
- force_before: float32 [3, 65536], P(None, ('shock', 'trans')), may hold values from -4 to 4
- beta: float32 [50], replicated, may hold values from -0.875 to 0.875
- alpha: float32 [50, 50], replicated, may hold values from -0.125 to 0.125
- live_count: int32 [256], P(('shock', 'trans')), may hold values from 128 to 256, as said below
- trans_send: int32 [2, 8192], P(None, ('shock', 'trans')), may hold values from 0 to 127, as said below
- shock_send: int32 [2, 32768], P(None, ('shock', 'trans')), may hold values from 0 to 319, as said below
- neighbour_block: int32 [26, 65536], P(None, ('shock', 'trans')), may hold values from -1 to 4, as said below
- neighbour_lane: int32 [26, 65536], P(None, ('shock', 'trans')), may hold values from 0 to 127, as said below
- leaving_slots: int32 [4096], P(('shock', 'trans')), may hold values from 0 to 127, as said below
- leaving_count: int32 [256], P(('shock', 'trans')), may hold values from 8 to 16, as said below
Outputs:
- displacement_next: float32 [3, 65536], P(None, ('shock', 'trans'))
- velocity_next: float32 [3, 65536], P(None, ('shock', 'trans'))
- force_next: float32 [3, 65536], P(None, ('shock', 'trans'))
- atom_energy: float32 [65536], P(('shock', 'trans'))
- arrivals: float32 [3, 3, 4096], P(None, None, ('shock', 'trans'))
The draws below stay inside these ranges and needn't reach their ends.
Inputs may be any that keep to these rules, and one draw needn't show every extreme that they name: A store's live atoms are its slots 0 to live_count - 1; stores at the lowest shock indices, behind the front, are full, and some store holds 256. `trans_send`: entries are live atoms of the sending store. `shock_send`: entries are live atoms or transverse ghost columns of the sending store's first section. `neighbour_block`: -1 marks an absent neighbour; slots at or above live_count have none; otherwise the column names a live own atom or a ghost column, never a ghost block beyond an open end of the shock axis. `neighbour_lane`: read together with neighbour_block. `leaving_slots`: distinct live atoms of the store. `leaving_count`: some store uses all 16 entries.
All inputs are finite; a program needn't handle non-finite values.
Results may differ from the reference program's by a relative error of at most 0.0003.
Values sent between devices are 32-bit elements; how exact they have to be, the bound alone decides.
A program may use at most 64 MiB of HBM per device.

```python
import math
import jax
import jax.numpy as jnp
import numpy as np
from jax import lax

ATOM_SLOTS = 256
NEIGHBOURS = 26
DESCRIPTORS = 50
TRANS_GHOSTS = 32
SHOCK_GHOSTS = 128
LEAVE_SLOTS = 16
ATOMS_ALL = 65536
N_SHOCK = 32
N_TRANS = 8
DEVICES = 256


def store_counts(key):
    front_index = jax.random.randint(jax.random.fold_in(key, 101), (), N_SHOCK // 4, N_SHOCK - N_SHOCK // 4 + 1)
    shock_index = jnp.arange(DEVICES, dtype=jnp.int32) // N_TRANS
    uncompressed = jax.random.randint(jax.random.fold_in(key, 102), (DEVICES,), ATOM_SLOTS // 2, ATOM_SLOTS // 2 + ATOM_SLOTS // 8 + 1)
    return jnp.where(shock_index < front_index, ATOM_SLOTS, uncompressed).astype(jnp.int32)


def neighbour_index(key):
    counts = store_counts(key)
    compressed = counts == ATOM_SLOTS
    full_shape = (NEIGHBOURS, DEVICES, ATOM_SLOTS)
    slot_index = jnp.arange(ATOM_SLOTS, dtype=jnp.int32)[None, None, :]
    entry_index = jnp.arange(NEIGHBOURS, dtype=jnp.int32)[:, None, None]
    shock_index = (jnp.arange(DEVICES, dtype=jnp.int32) // N_TRANS)[None, :, None]
    additional = jax.random.randint(jax.random.fold_in(key, 201), full_shape, 0, 4) == 0
    occupied = (slot_index < counts[None, :, None]) & (compressed[None, :, None] | (entry_index < 14) | additional)
    category = jax.random.randint(jax.random.fold_in(key, 202), full_shape, 0, 10)
    own_pick = jax.random.randint(jax.random.fold_in(key, 203), full_shape, 0, counts[None, :, None])
    trans_pick = jax.random.randint(jax.random.fold_in(key, 204), full_shape, 0, TRANS_GHOSTS)
    shock_pick = jax.random.randint(jax.random.fold_in(key, 205), full_shape, 0, SHOCK_GHOSTS)
    first_width = ATOM_SLOTS + 2 * TRANS_GHOSTS
    chosen = jnp.where(category == 0, ATOM_SLOTS + trans_pick, own_pick)
    chosen = jnp.where(category == 1, ATOM_SLOTS + TRANS_GHOSTS + trans_pick, chosen)
    chosen = jnp.where((category == 2) & (shock_index > 0), first_width + shock_pick, chosen)
    chosen = jnp.where((category == 3) & (shock_index < N_SHOCK - 1), first_width + SHOCK_GHOSTS + shock_pick, chosen)
    chosen = jnp.where(occupied, chosen, -1).astype(jnp.int32)
    return chosen.reshape(NEIGHBOURS, DEVICES * ATOM_SLOTS)


def draw_live_count(key, part):
    return store_counts(key)


def draw_trans_send(key, part):
    picks = jax.random.randint(jax.random.fold_in(key, 301), (2, DEVICES, TRANS_GHOSTS), 0, ATOM_SLOTS // 2)
    return picks.reshape(2, DEVICES * TRANS_GHOSTS).astype(jnp.int32)


def draw_shock_send(key, part):
    full_shape = (2, DEVICES, SHOCK_GHOSTS)
    category = jax.random.randint(jax.random.fold_in(key, 401), full_shape, 0, 8)
    own_pick = jax.random.randint(jax.random.fold_in(key, 402), full_shape, 0, ATOM_SLOTS // 2)
    ghost_pick = ATOM_SLOTS + jax.random.randint(jax.random.fold_in(key, 403), full_shape, 0, 2 * TRANS_GHOSTS)
    return jnp.where(category == 0, ghost_pick, own_pick).reshape(2, DEVICES * SHOCK_GHOSTS).astype(jnp.int32)


def draw_neighbour_block(key, part):
    return neighbour_index(key) // 128


def draw_neighbour_lane(key, part):
    return neighbour_index(key) % 128


def draw_leaving_slots(key, part):
    stride = ATOM_SLOTS // 2 // LEAVE_SLOTS
    starting = jnp.arange(LEAVE_SLOTS, dtype=jnp.int32) * stride
    jitter = jax.random.randint(jax.random.fold_in(key, 501), (DEVICES, LEAVE_SLOTS), 0, stride)
    return (starting[None, :] + jitter).reshape(DEVICES * LEAVE_SLOTS).astype(jnp.int32)


def draw_leaving_count(key, part):
    counts = jax.random.randint(jax.random.fold_in(key, 601), (DEVICES,), LEAVE_SLOTS // 2, LEAVE_SLOTS + 1)
    fullest = jax.random.randint(jax.random.fold_in(key, 602), (), 0, DEVICES)
    return jnp.where(jnp.arange(DEVICES) == fullest, LEAVE_SLOTS, counts).astype(jnp.int32)


def block_levels(stream_key, extent, cuts, least, top_value):
    def one(axis_at, shards_of):
        heights = jax.random.uniform(jax.random.fold_in(jax.random.fold_in(stream_key, 6), axis_at), (shards_of,), jnp.float32, least / len(cuts), top_value / len(cuts))
        return jnp.repeat(jnp.exp(heights), extent[axis_at] // shards_of).reshape((-1,) + (1,) * (len(extent) - axis_at - 1))

    level = one(*cuts[0])
    for cut in cuts[1:]:
        level = level * one(*cut)
    return level


def normal_values(key, dims, spread, reach, pieces=(), kind=jnp.bfloat16):
    drawn = jax.random.normal(key, dims, jnp.float32) * spread
    if len(pieces) > 0:
        drawn = block_levels(key, dims, pieces, -0.22, 0.18) * drawn
    return jnp.clip(drawn, min=-reach, max=reach).astype(kind)


def setup_inputs(seed: int = 0) -> dict:
    key_of = jax.random.split(jax.random.key(seed), 13)
    displacement = normal_values(key_of[0], (3, ATOMS_ALL), 0.08, 0.32, ((1, 256),), jnp.float32)
    velocity = normal_values(key_of[1], (3, ATOMS_ALL), 1.0, 4.0, ((1, 256),), jnp.float32)
    force_before = normal_values(key_of[2], (3, ATOMS_ALL), 1.0, 4.0, ((1, 256),), jnp.float32)
    beta = normal_values(key_of[3], (DESCRIPTORS,), DESCRIPTORS ** -0.5, 0.875, (), jnp.float32)
    alpha = normal_values(key_of[4], (DESCRIPTORS, DESCRIPTORS), (DESCRIPTORS * DESCRIPTORS) ** -0.5, 0.125, (), jnp.float32)
    live_count = draw_live_count(jax.random.fold_in(key_of[12], 71), 0)
    trans_send = draw_trans_send(jax.random.fold_in(key_of[12], 71), 0)
    shock_send = draw_shock_send(jax.random.fold_in(key_of[12], 71), 0)
    neighbour_block = draw_neighbour_block(jax.random.fold_in(key_of[12], 71), 0)
    neighbour_lane = draw_neighbour_lane(jax.random.fold_in(key_of[12], 71), 0)
    leaving_slots = draw_leaving_slots(jax.random.fold_in(key_of[12], 71), 0)
    leaving_count = draw_leaving_count(jax.random.fold_in(key_of[12], 71), 0)
    return {"displacement": displacement, "velocity": velocity, "force_before": force_before, "beta": beta, "alpha": alpha, "live_count": live_count, "trans_send": trans_send, "shock_send": shock_send, "neighbour_block": neighbour_block, "neighbour_lane": neighbour_lane, "leaving_slots": leaving_slots, "leaving_count": leaving_count}


kick_factor = 0.5
drift_step = 0.02
cutoff_radius = 4.2
radial_width = 0.35
radial_centers = (1.4, 1.9, 2.4, 2.9)
moment_scale = 0.25
pair_list = ((0, 0), (0, 1), (0, 2), (0, 3), (1, 1), (1, 2), (1, 3), (2, 2), (2, 3), (3, 3))
highest = lax.Precision.HIGHEST

def lattice_table():
    entries = []
    for number in range(8):
        entries.append([1.0 - 2.0 * (number >> 2 & 1), 1.0 - 2.0 * (number >> 1 & 1), 1.0 - 2.0 * (number & 1)])
    for axis_pick in range(3):
        for signed in (2.0, -2.0):
            vector = [0.0, 0.0, 0.0]
            vector[axis_pick] = signed
            entries.append(vector)
    for zero_pick in (2, 1, 0):
        others = [axis_pick for axis_pick in range(3) if axis_pick != zero_pick]
        for leading in (2.0, -2.0):
            for trailing in (2.0, -2.0):
                vector = [0.0, 0.0, 0.0]
                vector[others[0]] = leading
                vector[others[1]] = trailing
                entries.append(vector)
    return np.array(entries, dtype=np.float32).T

def exponent_table():
    triples = []
    for degree in range(5):
        for first_power in range(degree, -1, -1):
            for second_power in range(degree - first_power, -1, -1):
                triples.append((degree, first_power, second_power, degree - first_power - second_power))
    return triples

def contraction_weights():
    triples = exponent_table()
    matrix = np.zeros((5, len(triples)), dtype=np.float32)
    for column, (degree, first_power, second_power, third_power) in enumerate(triples):
        matrix[degree, column] = math.factorial(degree) / (math.factorial(first_power) * math.factorial(second_power) * math.factorial(third_power))
    return matrix

def block_energy(vectors, present, beta, alpha):
    distance = jnp.sqrt(lax.optimization_barrier(jnp.sum(vectors * vectors, axis=0)))
    direction = vectors / distance[None]
    smooth = 0.5 * (jnp.cos(jnp.pi * distance / cutoff_radius) + 1.0) * present
    radial = jnp.stack([smooth * jnp.exp(-jnp.square((distance - center) / radial_width)) for center in radial_centers])
    powers_first = [jnp.ones_like(distance)]
    powers_second = [jnp.ones_like(distance)]
    powers_third = [jnp.ones_like(distance)]
    for degree in range(4):
        powers_first.append(powers_first[-1] * direction[0])
        powers_second.append(powers_second[-1] * direction[1])
        powers_third.append(powers_third[-1] * direction[2])
    monomials = jnp.stack([powers_first[first_power] * powers_second[second_power] * powers_third[third_power] for degree, first_power, second_power, third_power in exponent_table()])
    moments = moment_scale * jnp.einsum('nkb,mkb->nmb', radial, monomials, precision=highest)
    products = jnp.stack([moments[first_index] * moments[second_index] for first_index, second_index in pair_list])
    weights = jnp.asarray(contraction_weights())
    descriptor = jnp.einsum('lm,pmb->plb', weights, products, precision=highest)
    descriptor = descriptor.reshape(len(pair_list) * 5, descriptor.shape[2])
    linear = jnp.dot(beta, descriptor, precision=highest)
    quadratic = lax.optimization_barrier(jnp.sum(descriptor * jnp.dot(alpha, descriptor, precision=highest), axis=0))
    return linear + 0.5 * quadratic

def store_terms(extended, own_rows, neighbour_block, neighbour_lane, beta, alpha):
    slot_count = own_rows.shape[1]
    block_rows = min(slot_count, 2048)
    groups = slot_count // block_rows
    offsets = jnp.asarray(lattice_table())
    present = neighbour_block >= 0
    clamped = jnp.where(present, neighbour_block * 128 + neighbour_lane, 0).astype(jnp.int32)
    weight_live = present.astype(extended.dtype)

    def one_group(inputs):
        clamped_rows, live_rows, own_group = inputs
        vectors = offsets[:, :, None] + extended[:, clamped_rows] - own_group[:, None, :]
        energies, pullback = jax.vjp(lambda moved: block_energy(moved, live_rows, beta, alpha), vectors)
        pair_grad, = pullback(jnp.ones_like(energies))
        return (energies, pair_grad)

    def grouped(array):
        return jnp.moveaxis(array.reshape(array.shape[:-1] + (groups, block_rows)), -2, 0)
    energies, pair_grad = lax.map(one_group, (grouped(clamped), grouped(weight_live), grouped(own_rows)))
    energies = energies.reshape(slot_count)
    pair_grad = jnp.moveaxis(pair_grad, 0, -2).reshape(3, clamped.shape[0], slot_count)
    total = jnp.zeros((3, extended.shape[1]), extended.dtype)
    total = total.at[:, clamped.reshape(-1)].add(pair_grad.reshape(3, -1))
    total = total.at[:, :slot_count].add(-lax.optimization_barrier(jnp.sum(pair_grad, axis=1)))
    return (energies, total)

def pick_columns(stores, lists):
    return jax.vmap(lambda store_rows, index_rows: store_rows[:, index_rows], in_axes=(1, 1), out_axes=2)(stores, lists)

def add_columns(stores, lists, values):

    def one_store(store_rows, index_rows, value_rows):
        return store_rows.at[:, index_rows[0]].add(value_rows[:, 0]).at[:, index_rows[1]].add(value_rows[:, 1])
    return jax.vmap(one_store, in_axes=(1, 1, 2), out_axes=1)(stores, lists, values)

def reference(displacement, velocity, force_before, beta, alpha, live_count, trans_send, shock_send, neighbour_block, neighbour_lane, leaving_slots, leaving_count):
    half_velocity = velocity + kick_factor * force_before
    displaced = displacement + drift_step * half_velocity
    own_grid = displaced.reshape(3, DEVICES, ATOM_SLOTS)
    trans_lists = trans_send.reshape(2, DEVICES, TRANS_GHOSTS)
    shock_lists = shock_send.reshape(2, DEVICES, SHOCK_GHOSTS)
    first_width = ATOM_SLOTS + 2 * TRANS_GHOSTS
    sent = pick_columns(own_grid, trans_lists).reshape(3, 2, N_SHOCK, N_TRANS, TRANS_GHOSTS)
    from_lower = jnp.roll(sent[:, 1], 1, axis=2)
    from_upper = jnp.roll(sent[:, 0], -1, axis=2)
    first_section = jnp.concatenate([own_grid.reshape(3, N_SHOCK, N_TRANS, ATOM_SLOTS), from_lower, from_upper], axis=3)
    sent = pick_columns(first_section.reshape(3, DEVICES, first_width), shock_lists).reshape(3, 2, N_SHOCK, N_TRANS, SHOCK_GHOSTS)
    empty = jnp.zeros((3, 1, N_TRANS, SHOCK_GHOSTS), displaced.dtype)
    from_lower = jnp.concatenate([empty, sent[:, 1, :-1]], axis=1)
    from_upper = jnp.concatenate([sent[:, 0, 1:], empty], axis=1)
    extended = jnp.concatenate([first_section, from_lower, from_upper], axis=3).reshape(3, DEVICES, -1)
    block_grid = neighbour_block.reshape(NEIGHBOURS, DEVICES, ATOM_SLOTS)
    lane_grid = neighbour_lane.reshape(NEIGHBOURS, DEVICES, ATOM_SLOTS)

    def one_store(inputs):
        extended_rows, own_rows, block_rows, lane_rows = inputs
        return store_terms(extended_rows, own_rows, block_rows, lane_rows, beta, alpha)
    energies, gradients = lax.map(one_store, (jnp.moveaxis(extended, 1, 0), jnp.moveaxis(own_grid, 1, 0), jnp.moveaxis(block_grid, 1, 0), jnp.moveaxis(lane_grid, 1, 0)))
    gradient_grid = jnp.moveaxis(gradients, 0, 1).reshape(3, N_SHOCK, N_TRANS, -1)
    lower_ghosts = gradient_grid[..., first_width:first_width + SHOCK_GHOSTS]
    upper_ghosts = gradient_grid[..., first_width + SHOCK_GHOSTS:]
    back_lower = jnp.concatenate([empty, upper_ghosts[:, :-1]], axis=1)
    back_upper = jnp.concatenate([lower_ghosts[:, 1:], empty], axis=1)
    returned = jnp.stack([back_lower, back_upper], axis=1).reshape(3, 2, DEVICES, SHOCK_GHOSTS)
    first_grad = add_columns(gradient_grid[..., :first_width].reshape(3, DEVICES, first_width), shock_lists, returned)
    first_grid = first_grad.reshape(3, N_SHOCK, N_TRANS, first_width)
    lower_trans = first_grid[..., ATOM_SLOTS:ATOM_SLOTS + TRANS_GHOSTS]
    upper_trans = first_grid[..., ATOM_SLOTS + TRANS_GHOSTS:]
    back_lower = jnp.roll(upper_trans, 1, axis=2)
    back_upper = jnp.roll(lower_trans, -1, axis=2)
    returned = jnp.stack([back_lower, back_upper], axis=1).reshape(3, 2, DEVICES, TRANS_GHOSTS)
    own_grad = add_columns(first_grid[..., :ATOM_SLOTS].reshape(3, DEVICES, ATOM_SLOTS), trans_lists, returned)
    force_new = -own_grad
    velocity_new = half_velocity.reshape(3, DEVICES, ATOM_SLOTS) + kick_factor * force_new
    slot_index = jnp.arange(ATOM_SLOTS, dtype=jnp.int32)
    leave_index = jnp.arange(LEAVE_SLOTS, dtype=jnp.int32)
    leaving_grid = leaving_slots.reshape(DEVICES, LEAVE_SLOTS)
    sending = leave_index[None, :] < leaving_count[:, None]

    def departures(slot_rows, sending_rows):
        marked = jnp.zeros((ATOM_SLOTS + 1,), jnp.float32).at[jnp.where(sending_rows, slot_rows, ATOM_SLOTS).astype(jnp.int32)].set(1.0)
        return marked[:ATOM_SLOTS]
    departed = jax.vmap(departures)(leaving_grid, sending)
    retained = (slot_index[None, :] < live_count[:, None]).astype(jnp.float32) * (1.0 - departed)
    payload = jnp.stack([own_grid, velocity_new, force_new])
    chosen = jax.vmap(lambda quantities, index_rows: quantities[:, :, index_rows], in_axes=(2, 0), out_axes=2)(payload, leaving_grid)
    chosen = chosen * sending[None, None].astype(chosen.dtype)
    chosen = chosen.reshape(3, 3, N_SHOCK, N_TRANS, LEAVE_SLOTS)
    arrivals = jnp.concatenate([chosen[:, :, 1:], jnp.zeros_like(chosen[:, :, :1])], axis=2).reshape(3, 3, DEVICES * LEAVE_SLOTS)
    displacement_next = (own_grid * retained[None]).reshape(3, ATOMS_ALL)
    velocity_next = (velocity_new * retained[None]).reshape(3, ATOMS_ALL)
    force_next = (force_new * retained[None]).reshape(3, ATOMS_ALL)
    atom_energy = (energies * retained).reshape(ATOMS_ALL)
    return (displacement_next, velocity_next, force_next, atom_energy, arrivals)
```

```python
import functools
import math

import jax
import jax.numpy as jnp
import numpy as np
from jax import lax
from jax.experimental import pallas as pl
from jax.experimental.pallas import tpu as pltpu
from jax.sharding import PartitionSpec as P

F32 = jnp.float32
BF16 = jnp.bfloat16
MESH = pl.DeviceIdType.MESH

kick_factor = 0.5
drift_step = 0.02
cutoff_radius = 4.2
radial_width = 0.35
radial_centers = (1.4, 1.9, 2.4, 2.9)
moment_scale = 0.25
pair_list = ((0, 0), (0, 1), (0, 2), (0, 3), (1, 1), (1, 2), (1, 3), (2, 2), (2, 3), (3, 3))
LANES = 128
ROWS = 32
MROWS = 40
DROWS = 64


def exponents():
    triples = []
    for degree in range(5):
        for p in range(degree, -1, -1):
            for q in range(degree - p, -1, -1):
                triples.append((p, q, degree - p - q))
    return triples


TRIPLES = exponents()
INDEX = {t: i for i, t in enumerate(TRIPLES)}


def lattice_rows():
    entries = []
    for number in range(8):
        entries.append(
            [1.0 - 2.0 * (number >> 2 & 1), 1.0 - 2.0 * (number >> 1 & 1), 1.0 - 2.0 * (number & 1)]
        )
    for axis_pick in range(3):
        for signed in (2.0, -2.0):
            vector = [0.0, 0.0, 0.0]
            vector[axis_pick] = signed
            entries.append(vector)
    for zero_pick in (2, 1, 0):
        others = [axis_pick for axis_pick in range(3) if axis_pick != zero_pick]
        for leading in (2.0, -2.0):
            for trailing in (2.0, -2.0):
                vector = [0.0, 0.0, 0.0]
                vector[others[0]] = leading
                vector[others[1]] = trailing
                entries.append(vector)
    while len(entries) < ROWS:
        entries.append([1.0, 1.0, 1.0])
    table = np.array(entries, dtype=np.float32).T
    return np.broadcast_to(table[:, :, None], (3, ROWS, LANES)).copy()


def contraction_table():
    table = np.zeros((DROWS, len(pair_list) * MROWS), dtype=np.float32)
    for i in range(len(pair_list)):
        for m, (p, q, w) in enumerate(TRIPLES):
            degree = p + q + w
            table[5 * i + degree, MROWS * i + m] = math.factorial(degree) / (
                math.factorial(p) * math.factorial(q) * math.factorial(w)
            )
    return table


def split(x):
    hi = x.astype(BF16)
    lo = (x - hi.astype(F32)).astype(BF16)
    return hi, lo


def mm(a, b):
    return lax.dot_general(a, b, (((1,), (0,)), ((), ())), preferred_element_type=F32)


def mm_nt(a, b):
    return lax.dot_general(a, b, (((1,), (1,)), ((), ())), preferred_element_type=F32)


def lane_gather(x, index):
    numbers = lax.GatherDimensionNumbers(
        offset_dims=(),
        collapsed_slice_dims=(1,),
        start_index_map=(1,),
        operand_batching_dims=(0,),
        start_indices_batching_dims=(0,),
    )
    return lax.gather(
        x,
        index[:, :, None],
        numbers,
        slice_sizes=(1, 1),
        mode=lax.GatherScatterMode.PROMISE_IN_BOUNDS,
    )


def rows_of(row, count):
    return jnp.broadcast_to(row, (count, row.shape[1]))


def sin_of(u):
    s = u * u
    r = -1.0 / 39916800.0
    for c in (1.0 / 362880.0, -1.0 / 5040.0, 1.0 / 120.0, -1.0 / 6.0, 1.0):
        r = r * s + c
    return r * u


def cos_of(u):
    s = u * u
    r = 1.0 / 479001600.0
    for c in (-1.0 / 3628800.0, 1.0 / 40320.0, -1.0 / 720.0, 1.0 / 24.0, -0.5, 1.0):
        r = r * s + c
    return r


def kernel(
    n_shock,
    n_trans,
    disp,
    vel,
    force,
    beta,
    alpha,
    live,
    trans_idx,
    shock_idx,
    nb_block,
    nb_lane,
    leave_idx,
    leave_count,
    offs,
    wmat,
    wmat_t,
    out_disp,
    out_vel,
    out_force,
    out_energy,
    out_arr,
    t_send,
    t_recv,
    s_send,
    s_recv,
    r_send,
    r_recv,
    u_send,
    u_recv,
    v_send,
    v_recv,
    send_sems,
    recv_sems,
    ext,
    blk,
    lan,
    idx_pad,
    geom,
    monos,
    mom,
    dmom,
    onehot,
    grows,
    apad,
    shock_hot,
    trans_hot,
    grads,
    own_sum,
):
    s_me = lax.axis_index("shock")
    t_me = lax.axis_index("trans")
    s_up = lax.rem(s_me + 1, n_shock)
    s_down = lax.rem(s_me + n_shock - 1, n_shock)
    t_up = lax.rem(t_me + 1, n_trans)
    t_down = lax.rem(t_me + n_trans - 1, n_trans)
    near = {
        "t_up": (s_me, t_up),
        "t_down": (s_me, t_down),
        "s_up": (s_up, t_me),
        "s_down": (s_down, t_me),
    }
    barrier = pltpu.get_barrier_semaphore()
    for where in near.values():
        pl.semaphore_signal(barrier, inc=1, device_id=where, device_id_type=MESH)

    def remote(src, dst, k, where):
        return pltpu.make_async_remote_copy(
            src_ref=src,
            dst_ref=dst,
            send_sem=send_sems.at[k],
            recv_sem=recv_sems.at[k],
            device_id=near[where],
            device_id_type=MESH,
        )

    t_copies = (
        remote(t_send, t_recv.at[0], 0, "t_up"),
        remote(t_send, t_recv.at[1], 1, "t_down"),
    )
    s_copies = (
        remote(s_send, s_recv.at[0], 2, "s_up"),
        remote(s_send, s_recv.at[1], 3, "s_down"),
    )
    r_copies = (
        remote(r_send, r_recv.at[0], 4, "s_up"),
        remote(r_send, r_recv.at[1], 5, "s_down"),
    )
    u_copies = (
        remote(u_send, u_recv.at[0], 6, "t_up"),
        remote(u_send, u_recv.at[1], 7, "t_down"),
    )
    v_copy = remote(v_send, v_recv, 8, "s_down")

    lane_row = lax.broadcasted_iota(jnp.int32, (1, LANES), 1)
    lane8 = lax.broadcasted_iota(jnp.int32, (8, LANES), 1)
    sub8 = lax.broadcasted_iota(jnp.int32, (8, LANES), 0)

    half_velocity = vel[...] + kick_factor * force[...]
    displaced = disp[...] + drift_step * half_velocity
    ext[...] = jnp.zeros_like(ext)
    for h in range(2):
        ext[h, 0:3, :] = displaced[:, h * LANES : (h + 1) * LANES]

    idx_pad[...] = jnp.zeros_like(idx_pad)
    idx_pad[0:1, 0:32] = trans_idx[1:2, :]
    idx_pad[1:2, 0:32] = trans_idx[0:1, :]
    idx_pad[2:4, :] = shock_idx[...]
    idx_pad[4:5, 0:16] = leave_idx[...]
    t_row = jnp.where(lane_row < 32, idx_pad[0:1, :], pltpu.roll(idx_pad[1:2, :], 32, 1))
    t_send[...] = lane_gather(ext[0], rows_of(t_row, 8))

    pl.semaphore_wait(barrier, 4)
    for copy in t_copies:
        copy.start()

    shock8 = jnp.where(sub8 < 4, rows_of(idx_pad[2:3, :], 8), rows_of(idx_pad[3:4, :], 8))
    shock_block = shock8 >> 7
    shock_lane = shock8 & 127
    doubled = [jnp.where(sub8 < 4, ext[b], pltpu.roll(ext[b], 4, 0)) for b in range(2)]
    s_own = jnp.where(
        shock_block == 0,
        lane_gather(doubled[0], shock_lane),
        lane_gather(doubled[1], shock_lane),
    )

    blk[...] = jnp.full_like(blk, -1)
    lan[...] = jnp.zeros_like(lan)
    blk[0:26, :] = nb_block[...]
    lan[0:26, :] = nb_lane[...] & 127

    for copy in t_copies:
        copy.wait_recv()
    t_ghost = jnp.where(lane8 < 32, t_recv[0], jnp.where(lane8 < 64, t_recv[1], 0.0))
    t_double = jnp.where(sub8 < 4, t_ghost, pltpu.roll(t_ghost, 4, 0))
    s_send[...] = jnp.where(shock_block == 2, lane_gather(t_double, shock_lane), s_own)
    for copy in s_copies:
        copy.start()

    column = lax.broadcasted_iota(jnp.int32, (LANES, 2 * LANES), 0)

    def fill_onehot(k, carry):
        row = lan[pl.ds(k, 1), :]
        hot = jnp.where(column == rows_of(row, LANES), 1.0, 0.0).astype(BF16)
        onehot[:, pl.ds(pl.multiple_of(k * 2 * LANES, 2 * LANES), 2 * LANES)] = hot
        return carry

    lax.fori_loop(0, 26, fill_onehot, 0)

    column384 = lax.broadcasted_iota(jnp.int32, (3 * LANES, LANES), 0)
    for d in range(2):
        shock_hot[:, d * LANES : (d + 1) * LANES] = jnp.where(
            column384 == rows_of(idx_pad[2 + d : 3 + d, :], 3 * LANES), 1.0, 0.0
        ).astype(BF16)
    column128 = lax.broadcasted_iota(jnp.int32, (LANES, LANES), 0)
    trans_hot[...] = jnp.where(column128 == rows_of(t_row, LANES), 1.0, 0.0).astype(BF16)
    leave_row = idx_pad[4:5, :]
    sending = jnp.where(lane_row < leave_count[0], 1.0, 0.0)
    leave_hot = jnp.where(column128 == rows_of(leave_row, LANES), 1.0, 0.0).astype(BF16)
    departed = mm_nt(rows_of(sending, 16).astype(BF16), leave_hot)[0:1, :]
    keep0 = jnp.where(lane_row < live[0], 1.0, 0.0) * (1.0 - departed)
    keep1 = jnp.where(lane_row + LANES < live[0], 1.0, 0.0)

    apad[...] = jnp.zeros_like(apad)
    apad[0:50, 0:50] = alpha[...]
    sym = 0.5 * (apad[...] + apad[...].T)
    sym_hi, sym_lo = split(sym[0:DROWS, 0:DROWS])
    apad[0:1, :] = jnp.zeros((1, LANES), F32)
    apad[0:1, 0:50] = beta[...]
    beta_col = rows_of(apad[0:1, :], LANES).T[0:DROWS, :]
    beta_col = jnp.concatenate([beta_col, beta_col], axis=1)
    for n in range(4):
        mom[n * MROWS + 32 : (n + 1) * MROWS, :] = jnp.zeros((8, 2 * LANES), F32)

    for copy in s_copies:
        copy.wait_recv()
    lower = jnp.where(s_me > 0, s_recv[0], 0.0)
    upper = jnp.where(s_me < n_shock - 1, s_recv[1], 0.0)
    both = jnp.where(sub8 < 4, pltpu.roll(lower, 4, 0), pltpu.roll(upper, 4, 0))
    turned = pltpu.roll(both, 64, 1)
    swapped = pltpu.roll(turned, 4, 0)
    ext[2] = jnp.where(lane8 < 64, t_ghost, turned)
    ext[3] = jnp.where(lane8 < 64, turned, swapped)
    ext[4] = swapped

    for h in range(2):
        hs = slice(h * LANES, (h + 1) * LANES)
        block = blk[:, hs]
        lane = lan[:, hs]
        parts = []
        for c in range(3):
            found = jnp.zeros((ROWS, LANES), F32)
            for b in range(5):
                value = lane_gather(rows_of(ext[b, c : c + 1, :], ROWS), lane)
                found = jnp.where(block == b, value, found)
            parts.append(offs[c] + found - rows_of(ext[h, c : c + 1, :], ROWS))
        px, py, pz = parts
        square = px * px + py * py + pz * pz
        inverse = lax.rsqrt(square)
        distance = square * inverse
        ux, uy, uz = px * inverse, py * inverse, pz * inverse
        angle = (0.5 * math.pi) - (0.5 * math.pi / cutoff_radius) * distance
        sine, cosine = sin_of(angle), cos_of(angle)
        scale = jnp.where(block >= 0, moment_scale, 0.0)
        smooth = scale * sine * sine
        slope = scale * (-math.pi / cutoff_radius) * sine * cosine
        radial = []
        for n, center in enumerate(radial_centers):
            z = (distance - center) * (1.0 / radial_width)
            e = jnp.exp(-(z * z))
            r = smooth * e
            radial.append(r)
            geom[n, :, hs] = r
            geom[4 + n, :, hs] = slope * e - (2.0 / radial_width) * z * r
        geom[8, :, hs] = ux
        geom[9, :, hs] = uy
        geom[10, :, hs] = uz
        geom[11, :, hs] = inverse
        values = {}
        for m, (p, q, w) in enumerate(TRIPLES):
            if m == 0:
                value = None
            elif p > 0:
                prior = values[(p - 1, q, w)]
                value = ux if prior is None else prior * ux
            elif q > 0:
                prior = values[(p, q - 1, w)]
                value = uy if prior is None else prior * uy
            else:
                prior = values[(p, q, w - 1)]
                value = uz if prior is None else prior * uz
            values[(p, q, w)] = value
            if value is not None:
                monos[m, :, hs] = value
            for n in range(4):
                term = radial[n] if value is None else radial[n] * value
                mom[n * MROWS + m : n * MROWS + m + 1, hs] = jnp.sum(term, axis=0, keepdims=True)

    moments = [mom[n * MROWS : (n + 1) * MROWS, :] for n in range(4)]
    products = jnp.concatenate([moments[n] * moments[o] for n, o in pair_list], axis=0)
    prod_hi, prod_lo = split(products)
    weights = wmat[...]
    descriptor = mm(weights, prod_hi) + mm(weights, prod_lo)
    desc_hi, desc_lo = split(descriptor)
    quadratic = mm(sym_hi, desc_hi) + mm(sym_lo, desc_hi) + mm(sym_hi, desc_lo)
    energy = jnp.sum(descriptor * (beta_col + 0.5 * quadratic), axis=0, keepdims=True)
    slope_hi, slope_lo = split(beta_col + quadratic)
    weights_t = wmat_t[...]
    dproducts = mm(weights_t, slope_hi) + mm(weights_t, slope_lo)
    for n in range(4):
        total = None
        for i, (a, b) in enumerate(pair_list):
            if n not in (a, b):
                continue
            part = dproducts[i * MROWS : (i + 1) * MROWS, :]
            if a == b:
                part = 2.0 * part * moments[n]
            else:
                part = part * moments[b if n == a else a]
            total = part if total is None else total + part
        dmom[n * MROWS : (n + 1) * MROWS, :] = total

    for h in range(2):
        hs = slice(h * LANES, (h + 1) * LANES)
        radial = [geom[n, :, hs] for n in range(4)]
        dradial = [None] * 4
        sums = {}
        for m, (p, q, w) in enumerate(TRIPLES):
            coefficient = None
            for n in range(4):
                row = rows_of(dmom[n * MROWS + m : n * MROWS + m + 1, hs], ROWS)
                term = row if m == 0 else row * monos[m, :, hs]
                dradial[n] = term if dradial[n] is None else dradial[n] + term
                if m > 0:
                    term = row * radial[n]
                    coefficient = term if coefficient is None else coefficient + term
            if m == 0:
                continue
            for c, (power, prior) in enumerate(
                ((p, (p - 1, q, w)), (q, (p, q - 1, w)), (w, (p, q, w - 1)))
            ):
                if power == 0:
                    continue
                at = INDEX[prior]
                term = coefficient if at == 0 else coefficient * monos[at, :, hs]
                key = (c, power)
                sums[key] = term if key not in sums else sums[key] + term
        unit = [geom[8 + c, :, hs] for c in range(3)]
        inverse = geom[11, :, hs]
        along = None
        for n in range(4):
            term = geom[4 + n, :, hs] * dradial[n]
            along = term if along is None else along + term
        tangent = []
        for c in range(3):
            total = sums[(c, 1)]
            for power in (2, 3, 4):
                total = total + float(power) * sums[(c, power)]
            tangent.append(total * inverse)
        inner = unit[0] * tangent[0] + unit[1] * tangent[1] + unit[2] * tangent[2]
        along = along - inner
        for c in range(3):
            g = tangent[c] + unit[c] * along
            grads[c, :, hs] = g
            own_sum[h, c : c + 1, :] = jnp.sum(g, axis=0, keepdims=True)

    sub24 = lax.broadcasted_iota(jnp.int32, (24, 2 * LANES), 0)
    row_block = sub24 >> 2
    row_part = sub24 & 3

    def fill_rows(k, carry):
        gx = rows_of(grads[0, pl.ds(k, 1), :], 24)
        gy = rows_of(grads[1, pl.ds(k, 1), :], 24)
        gz = rows_of(grads[2, pl.ds(k, 1), :], 24)
        value = jnp.where(row_part == 0, gx, jnp.where(row_part == 1, gy, gz))
        value = jnp.where(row_block == rows_of(blk[pl.ds(k, 1), :], 24), value, 0.0)
        hi = value.astype(BF16).astype(F32)
        at = pl.ds(pl.multiple_of(k * 2 * LANES, 2 * LANES), 2 * LANES)
        grows[:, at] = jnp.concatenate([hi, value - hi], axis=0).astype(BF16)
        return carry

    lax.fori_loop(0, 26, fill_rows, 0)
    spread = mm_nt(grows[...], onehot[...])
    spread = spread[0:24, :] + spread[24:48, :]
    first = spread[0:8, :]
    second = spread[8:16, :]
    third = spread[16:24, :]
    second_turned = pltpu.roll(second, 64, 1)
    third_turned = pltpu.roll(third, 64, 1)
    shifted = jnp.where(
        sub8 < 4, pltpu.roll(second_turned, 4, 0), pltpu.roll(third_turned, 4, 0)
    )
    r_send[...] = jnp.where(lane8 < 64, second_turned, shifted)
    for copy in r_copies:
        copy.start()
    for copy in r_copies:
        copy.wait_recv()

    from_lower = jnp.where(s_me > 0, pltpu.roll(r_recv[0], 4, 0), 0.0)
    from_upper = jnp.where(s_me < n_shock - 1, r_recv[1], 0.0)
    back = jnp.concatenate([from_lower, from_upper], axis=1)
    back_hi = back.astype(BF16).astype(F32)
    back2 = jnp.concatenate([back_hi, back - back_hi], axis=0).astype(BF16)
    added = mm_nt(back2, shock_hot[...])
    added = added[0:8, :] + added[8:16, :]
    u_send[...] = second + added[:, 2 * LANES : 3 * LANES]
    for copy in u_copies:
        copy.start()

    first_swapped = pltpu.roll(first, 4, 0)
    grad0 = first + added[:, 0:LANES] - own_sum[0]
    grad1 = first_swapped + added[:, LANES : 2 * LANES] - own_sum[1]
    force1 = -grad1[0:3, :]
    half1 = half_velocity[:, LANES:]
    out_disp[:, LANES:] = displaced[:, LANES:] * rows_of(keep1, 3)
    out_vel[:, LANES:] = (half1 + kick_factor * force1) * rows_of(keep1, 3)
    out_force[:, LANES:] = force1 * rows_of(keep1, 3)
    out_energy[:, 0:LANES] = energy[:, 0:LANES] * keep0
    out_energy[:, LANES:] = energy[:, LANES:] * keep1
    out_disp[:, 0:LANES] = displaced[:, 0:LANES] * rows_of(keep0, 3)

    for copy in u_copies:
        copy.wait_recv()
    merged = jnp.where(lane8 < 32, u_recv[1], jnp.where(lane8 < 64, u_recv[0], 0.0))
    merged_hi = merged.astype(BF16).astype(F32)
    merged2 = jnp.concatenate([merged_hi, merged - merged_hi], axis=0).astype(BF16)
    added = mm_nt(merged2, trans_hot[...])
    force0 = -(grad0 + added[0:8, :] + added[8:16, :])[0:3, :]
    velocity0 = half_velocity[:, 0:LANES] + kick_factor * force0
    ext[5, 0:3, :] = velocity0
    ext[6, 0:3, :] = force0
    leave3 = rows_of(leave_row, 8)
    for q, at in enumerate((0, 5, 6)):
        v_send[q] = lane_gather(ext[at], leave3) * rows_of(sending, 8)
    v_copy.start()
    out_vel[:, 0:LANES] = velocity0 * rows_of(keep0, 3)
    out_force[:, 0:LANES] = force0 * rows_of(keep0, 3)
    v_copy.wait_recv()
    for q in range(3):
        out_arr[q] = jnp.where(s_me < n_shock - 1, v_recv[q, 0:3, 0:16], 0.0)
    for copy in (*t_copies, *s_copies, *r_copies, *u_copies, v_copy):
        copy.wait_send()


def whole_step(n_shock, n_trans, *args):
    (disp, vel, force, beta, alpha, live, trans_idx, shock_idx, block, lane, leave, count) = args
    table = contraction_table()
    vmem = pl.BlockSpec(memory_space=pltpu.VMEM)
    smem = pl.BlockSpec(memory_space=pltpu.SMEM)
    tile = (8, LANES)
    outs = pl.pallas_call(
        functools.partial(kernel, n_shock, n_trans),
        out_shape=(
            jax.ShapeDtypeStruct((3, 256), F32),
            jax.ShapeDtypeStruct((3, 256), F32),
            jax.ShapeDtypeStruct((3, 256), F32),
            jax.ShapeDtypeStruct((1, 256), F32),
            jax.ShapeDtypeStruct((3, 3, 16), F32),
        ),
        in_specs=[vmem] * 5 + [smem] + [vmem] * 5 + [smem] + [vmem] * 3,
        out_specs=(vmem,) * 5,
        scratch_shapes=[
            pltpu.VMEM(tile, F32),
            pltpu.VMEM((2, *tile), F32),
            pltpu.VMEM(tile, F32),
            pltpu.VMEM((2, *tile), F32),
            pltpu.VMEM(tile, F32),
            pltpu.VMEM((2, *tile), F32),
            pltpu.VMEM(tile, F32),
            pltpu.VMEM((2, *tile), F32),
            pltpu.VMEM((3, *tile), F32),
            pltpu.VMEM((3, *tile), F32),
            pltpu.SemaphoreType.DMA((9,)),
            pltpu.SemaphoreType.DMA((9,)),
            pltpu.VMEM((7, *tile), F32),
            pltpu.VMEM((ROWS, 256), jnp.int32),
            pltpu.VMEM((ROWS, 256), jnp.int32),
            pltpu.VMEM(tile, jnp.int32),
            pltpu.VMEM((12, ROWS, 256), F32),
            pltpu.VMEM((35, ROWS, 256), F32),
            pltpu.VMEM((4 * MROWS, 256), F32),
            pltpu.VMEM((4 * MROWS, 256), F32),
            pltpu.VMEM((LANES, 26 * 256), BF16),
            pltpu.VMEM((48, 26 * 256), BF16),
            pltpu.VMEM((LANES, LANES), F32),
            pltpu.VMEM((3 * LANES, 2 * LANES), BF16),
            pltpu.VMEM((LANES, LANES), BF16),
            pltpu.VMEM((3, ROWS, 256), F32),
            pltpu.VMEM((2, *tile), F32),
        ],
        compiler_params=pltpu.CompilerParams(collective_id=0, has_side_effects=True),
        name="whole_step",
    )(
        disp,
        vel,
        force,
        beta.reshape(1, 50),
        alpha,
        live,
        trans_idx,
        shock_idx,
        block,
        lane,
        leave.reshape(1, 16),
        count,
        jnp.asarray(lattice_rows()),
        jnp.asarray(table, BF16),
        jnp.asarray(table.T, BF16),
    )
    return outs[0], outs[1], outs[2], outs[3].reshape(256), outs[4]


def solution(mesh):
    split_1 = P(None, ("shock", "trans"))
    split_0 = P(("shock", "trans"))
    in_specs = (
        split_1,
        split_1,
        split_1,
        P(),
        P(),
        split_0,
        split_1,
        split_1,
        split_1,
        split_1,
        split_0,
        split_0,
    )
    out_specs = (split_1, split_1, split_1, split_0, P(None, None, ("shock", "trans")))
    body = functools.partial(whole_step, mesh.shape["shock"], mesh.shape["trans"])
    return jax.shard_map(body, mesh=mesh, in_specs=in_specs, out_specs=out_specs, check_vma=False)
```

```python
import functools
import math

import jax
import jax.numpy as jnp
import numpy as np
from jax import lax
from jax.experimental import pallas as pl
from jax.experimental.pallas import tpu as pltpu
from jax.sharding import PartitionSpec as P

F32 = jnp.float32
BF16 = jnp.bfloat16
MESH = pl.DeviceIdType.MESH

kick_factor = 0.5
drift_step = 0.02
cutoff_radius = 4.2
radial_width = 0.35
radial_centers = (1.4, 1.9, 2.4, 2.9)
moment_scale = 0.25
pair_list = ((0, 0), (0, 1), (0, 2), (0, 3), (1, 1), (1, 2), (1, 3), (2, 2), (2, 3), (3, 3))
LANES = 128
ROWS = 32
MROWS = 40
DROWS = 64


def exponents():
    triples = []
    for degree in range(5):
        for p in range(degree, -1, -1):
            for q in range(degree - p, -1, -1):
                triples.append((p, q, degree - p - q))
    return triples


TRIPLES = exponents()
INDEX = {t: i for i, t in enumerate(TRIPLES)}


def lattice_rows():
    entries = []
    for number in range(8):
        entries.append(
            [1.0 - 2.0 * (number >> 2 & 1), 1.0 - 2.0 * (number >> 1 & 1), 1.0 - 2.0 * (number & 1)]
        )
    for axis_pick in range(3):
        for signed in (2.0, -2.0):
            vector = [0.0, 0.0, 0.0]
            vector[axis_pick] = signed
            entries.append(vector)
    for zero_pick in (2, 1, 0):
        others = [axis_pick for axis_pick in range(3) if axis_pick != zero_pick]
        for leading in (2.0, -2.0):
            for trailing in (2.0, -2.0):
                vector = [0.0, 0.0, 0.0]
                vector[others[0]] = leading
                vector[others[1]] = trailing
                entries.append(vector)
    while len(entries) < ROWS:
        entries.append([1.0, 1.0, 1.0])
    table = np.array(entries, dtype=np.float32).T
    return np.broadcast_to(table[:, :, None], (3, ROWS, LANES)).copy()


def contraction_table():
    table = np.zeros((DROWS, len(pair_list) * MROWS), dtype=np.float32)
    for i in range(len(pair_list)):
        for m, (p, q, w) in enumerate(TRIPLES):
            degree = p + q + w
            table[5 * i + degree, MROWS * i + m] = math.factorial(degree) / (
                math.factorial(p) * math.factorial(q) * math.factorial(w)
            )
    return table


def split(x):
    hi = x.astype(BF16)
    lo = (x - hi.astype(F32)).astype(BF16)
    return hi, lo


def mm(a, b):
    return lax.dot_general(a, b, (((1,), (0,)), ((), ())), preferred_element_type=F32)


def mm_nt(a, b):
    return lax.dot_general(a, b, (((1,), (1,)), ((), ())), preferred_element_type=F32)


def lane_gather(x, index):
    numbers = lax.GatherDimensionNumbers(
        offset_dims=(),
        collapsed_slice_dims=(1,),
        start_index_map=(1,),
        operand_batching_dims=(0,),
        start_indices_batching_dims=(0,),
    )
    return lax.gather(
        x,
        index[:, :, None],
        numbers,
        slice_sizes=(1, 1),
        mode=lax.GatherScatterMode.PROMISE_IN_BOUNDS,
    )


def rows_of(row, count):
    return jnp.broadcast_to(row, (count, row.shape[1]))


def sin_of(u):
    s = u * u
    r = -1.0 / 39916800.0
    for c in (1.0 / 362880.0, -1.0 / 5040.0, 1.0 / 120.0, -1.0 / 6.0, 1.0):
        r = r * s + c
    return r * u


def cos_of(u):
    s = u * u
    r = 1.0 / 479001600.0
    for c in (-1.0 / 3628800.0, 1.0 / 40320.0, -1.0 / 720.0, 1.0 / 24.0, -0.5, 1.0):
        r = r * s + c
    return r


DIRS = ((0, 1), (0, -1), (1, 0), (-1, 0), (1, 1), (1, -1), (-1, 1), (-1, -1))
N_IN = 15


def kernel(n_shock, n_trans, *refs):
    hbm = refs[:N_IN]
    out_disp, out_vel, out_force, out_energy, out_arr = refs[N_IN : N_IN + 5]
    (
        disp,
        vel,
        force,
        beta,
        alpha,
        live,
        trans_idx,
        shock_idx,
        nb_block,
        nb_lane,
        leave_idx,
        leave_count,
        offs,
        wmat,
        wmat_t,
        in_sems,
        t_send,
        s_send,
        f_recv,
        u_send,
        r_send,
        b_recv,
        v_send,
        v_recv,
        f_send_sems,
        f_recv_sems,
        b_send_sems,
        b_recv_sems,
        v_sems,
        ext,
        blk,
        lan,
        idx_pad,
        near_own,
        geom,
        monos,
        mom,
        dmom,
        onehot,
        apad,
        hot0,
        hot1,
        grads,
        own_sum,
    ) = refs[N_IN + 5 :]
    local = (
        disp,
        vel,
        force,
        beta,
        alpha,
        live,
        trans_idx,
        shock_idx,
        nb_block,
        nb_lane,
        leave_idx,
        leave_count,
        offs,
        wmat,
        wmat_t,
    )
    loads = [
        pltpu.make_async_copy(src, dst, in_sems.at[i])
        for i, (src, dst) in enumerate(zip(hbm, local, strict=True))
    ]
    for i in (0, 1, 2, 6, 7, 8, 9, 10, 5, 11, 4, 3, 12, 13, 14):
        loads[i].start()

    s_me = lax.axis_index("shock")
    t_me = lax.axis_index("trans")

    def place(ds, dt):
        return (
            lax.rem(s_me + (ds + n_shock), n_shock),
            lax.rem(t_me + (dt + n_trans), n_trans),
        )

    barrier = pltpu.get_barrier_semaphore()
    for ds, dt in DIRS:
        pl.semaphore_signal(barrier, inc=1, device_id=place(ds, dt), device_id_type=MESH)

    def remote(src, dst, send_sem, recv_sem, where):
        return pltpu.make_async_remote_copy(
            src_ref=src,
            dst_ref=dst,
            send_sem=send_sem,
            recv_sem=recv_sem,
            device_id=place(*where),
            device_id_type=MESH,
        )

    forward = [
        remote(
            s_send if dt == 0 else t_send,
            f_recv.at[k],
            f_send_sems.at[k],
            f_recv_sems.at[k],
            (ds, dt),
        )
        for k, (ds, dt) in enumerate(DIRS)
    ]
    backward = [
        remote(
            u_send if ds == 0 else r_send,
            b_recv.at[k],
            b_send_sems.at[k],
            b_recv_sems.at[k],
            (ds, dt),
        )
        for k, (ds, dt) in enumerate(DIRS)
    ]
    v_copy = remote(v_send, v_recv, v_sems.at[0], v_sems.at[1], (-1, 0))

    def slot(ds, dt):
        return DIRS.index((-ds, -dt))

    lane_row = lax.broadcasted_iota(jnp.int32, (1, LANES), 1)
    lane8 = lax.broadcasted_iota(jnp.int32, (8, LANES), 1)
    sub8 = lax.broadcasted_iota(jnp.int32, (8, LANES), 0)
    has_lower = jnp.where(s_me > 0, 1, 0)
    has_upper = jnp.where(s_me < n_shock - 1, 1, 0)

    idx_pad[...] = jnp.zeros_like(idx_pad)
    ext[...] = jnp.zeros_like(ext)
    for i in (0, 1, 2, 6, 7):
        loads[i].wait()
    half_velocity = vel[...] + kick_factor * force[...]
    displaced = disp[...] + drift_step * half_velocity
    for h in range(2):
        ext[h, 0:3, :] = displaced[:, h * LANES : (h + 1) * LANES]
    idx_pad[0:1, 0:32] = trans_idx[1:2, :]
    idx_pad[1:2, 0:32] = trans_idx[0:1, :]
    idx_pad[2:4, :] = shock_idx[...]
    t_row = jnp.where(lane_row < 32, idx_pad[0:1, :], pltpu.roll(idx_pad[1:2, :], 32, 1))
    shock8 = jnp.where(sub8 < 4, rows_of(idx_pad[2:3, :], 8), rows_of(idx_pad[3:4, :], 8))
    shock_block = shock8 >> 7
    shock_lane = shock8 & 127
    doubled = [jnp.where(sub8 < 4, ext[b], pltpu.roll(ext[b], 4, 0)) for b in range(2)]
    t_send[...] = lane_gather(ext[0], rows_of(t_row, 8))
    t_send[4:6, :] = shock_idx[...].astype(F32)
    s_own = jnp.where(
        shock_block == 0,
        lane_gather(doubled[0], shock_lane),
        jnp.where(shock_block == 1, lane_gather(doubled[1], shock_lane), 0.0),
    )
    s_send[...] = jnp.where((sub8 & 3) == 3, shock8.astype(F32), s_own)

    pl.semaphore_wait(barrier, len(DIRS))
    for k in (4, 5, 6, 7, 0, 1, 2, 3):
        forward[k].start()

    for i in (8, 9, 10, 5, 11, 4, 3):
        loads[i].wait()
    blk[...] = jnp.full_like(blk, -1)
    lan[...] = jnp.zeros_like(lan)
    blk[0:26, :] = nb_block[...]
    lan[0:26, :] = nb_lane[...] & 127
    idx_pad[4:5, 0:16] = leave_idx[...]
    column = lax.broadcasted_iota(jnp.int32, (LANES, 2 * LANES), 0)

    def fill_onehot(k, carry):
        row = lan[pl.ds(k, 1), :]
        hot = jnp.where(column == rows_of(row, LANES), 1.0, 0.0).astype(BF16)
        onehot[:, pl.ds(pl.multiple_of(k * 2 * LANES, 2 * LANES), 2 * LANES)] = hot
        return carry

    lax.fori_loop(0, 26, fill_onehot, 0)
    for i in (12, 13, 14):
        loads[i].wait()
    for h in range(2):
        hs = slice(h * LANES, (h + 1) * LANES)
        for c in range(3):
            found = offs[c] - rows_of(ext[h, c : c + 1, :], ROWS)
            parts = [
                lane_gather(rows_of(ext[b, c : c + 1, :], ROWS), lan[:, hs]) for b in range(2)
            ]
            block = blk[:, hs]
            near_own[c, :, hs] = found + jnp.where(
                block == 0, parts[0], jnp.where(block == 1, parts[1], 0.0)
            )

    column128 = lax.broadcasted_iota(jnp.int32, (LANES, LANES), 0)
    leave_row = idx_pad[4:5, :]
    sending = jnp.where(lane_row < leave_count[0], 1.0, 0.0)
    leave_hot = jnp.where(column128 == rows_of(leave_row, LANES), 1.0, 0.0).astype(BF16)
    departed = mm_nt(rows_of(sending, 16).astype(BF16), leave_hot)[0:1, :]
    keep0 = jnp.where(lane_row < live[0], 1.0, 0.0) * (1.0 - departed)
    keep1 = jnp.where(lane_row + LANES < live[0], 1.0, 0.0)
    out_disp[:, 0:LANES] = displaced[:, 0:LANES] * rows_of(keep0, 3)
    out_disp[:, LANES:] = displaced[:, LANES:] * rows_of(keep1, 3)

    apad[...] = jnp.zeros_like(apad)
    apad[0:50, 0:50] = alpha[...]
    sym = 0.5 * (apad[...] + apad[...].T)
    sym_hi, sym_lo = split(sym[0:DROWS, 0:DROWS])
    apad[0:1, :] = jnp.zeros((1, LANES), F32)
    apad[0:1, 0:50] = beta[...]
    beta_col = rows_of(apad[0:1, :], LANES).T[0:DROWS, :]
    beta_col = jnp.concatenate([beta_col, beta_col], axis=1)
    for n in range(4):
        mom[n * MROWS + 32 : (n + 1) * MROWS, :] = jnp.zeros((8, 2 * LANES), F32)

    for copy in forward:
        copy.wait_recv()

    def between(lower, upper):
        return jnp.where(lane8 < 32, lower, jnp.where(lane8 < 64, upper, 0.0))

    t_ghost = between(f_recv[slot(0, -1)], f_recv[slot(0, 1)])
    from_low = f_recv[slot(-1, 0)]
    from_up = f_recv[slot(1, 0)]
    lists = jnp.where(sub8 < 4, rows_of(from_low[7:8, :], 8), rows_of(from_up[3:4, :], 8))
    lists = lists.astype(jnp.int32)
    across = jnp.where(
        sub8 < 4,
        between(f_recv[slot(-1, -1)], f_recv[slot(-1, 1)]),
        pltpu.roll(between(f_recv[slot(1, -1)], f_recv[slot(1, 1)]), 4, 0),
    )
    direct = jnp.where(sub8 < 4, pltpu.roll(from_low, 4, 0), pltpu.roll(from_up, 4, 0))
    both = jnp.where(lists >= 256, lane_gather(across, lists & 127), direct)
    both = jnp.where(jnp.where(sub8 < 4, has_lower, has_upper) > 0, both, 0.0)
    turned = pltpu.roll(both, 64, 1)
    swapped = pltpu.roll(turned, 4, 0)
    ext[2] = jnp.where(lane8 < 64, t_ghost, turned)
    ext[3] = jnp.where(lane8 < 64, turned, swapped)
    ext[4] = swapped

    for h in range(2):
        hs = slice(h * LANES, (h + 1) * LANES)
        block = blk[:, hs]
        lane = lan[:, hs]
        parts = []
        for c in range(3):
            found = jnp.zeros((ROWS, LANES), F32)
            for b in range(2, 5):
                value = lane_gather(rows_of(ext[b, c : c + 1, :], ROWS), lane)
                found = jnp.where(block == b, value, found)
            parts.append(near_own[c, :, hs] + found)
        px, py, pz = parts
        square = px * px + py * py + pz * pz
        inverse = lax.rsqrt(square)
        distance = square * inverse
        ux, uy, uz = px * inverse, py * inverse, pz * inverse
        angle = (0.5 * math.pi) - (0.5 * math.pi / cutoff_radius) * distance
        sine, cosine = sin_of(angle), cos_of(angle)
        scale = jnp.where(block >= 0, moment_scale, 0.0)
        smooth = scale * sine * sine
        slope = scale * (-math.pi / cutoff_radius) * sine * cosine
        radial = []
        for n, center in enumerate(radial_centers):
            z = (distance - center) * (1.0 / radial_width)
            e = jnp.exp(-(z * z))
            r = smooth * e
            radial.append(r)
            geom[n, :, hs] = r
            geom[4 + n, :, hs] = slope * e - (2.0 / radial_width) * z * r
        geom[8, :, hs] = ux
        geom[9, :, hs] = uy
        geom[10, :, hs] = uz
        geom[11, :, hs] = inverse
        values = {}
        for m, (p, q, w) in enumerate(TRIPLES):
            if m == 0:
                value = None
            elif p > 0:
                prior = values[(p - 1, q, w)]
                value = ux if prior is None else prior * ux
            elif q > 0:
                prior = values[(p, q - 1, w)]
                value = uy if prior is None else prior * uy
            else:
                prior = values[(p, q, w - 1)]
                value = uz if prior is None else prior * uz
            values[(p, q, w)] = value
            if value is not None:
                monos[m, :, hs] = value
            for n in range(4):
                term = radial[n] if value is None else radial[n] * value
                mom[n * MROWS + m : n * MROWS + m + 1, hs] = jnp.sum(term, axis=0, keepdims=True)

    moments = [mom[n * MROWS : (n + 1) * MROWS, :] for n in range(4)]
    products = jnp.concatenate([moments[n] * moments[o] for n, o in pair_list], axis=0)
    prod_hi, prod_lo = split(products)
    weights = wmat[...]
    descriptor = mm(weights, prod_hi) + mm(weights, prod_lo)
    desc_hi, desc_lo = split(descriptor)
    quadratic = mm(sym_hi, desc_hi) + mm(sym_lo, desc_hi) + mm(sym_hi, desc_lo)
    energy = jnp.sum(descriptor * (beta_col + 0.5 * quadratic), axis=0, keepdims=True)
    slope_hi, slope_lo = split(beta_col + quadratic)
    weights_t = wmat_t[...]
    dproducts = mm(weights_t, slope_hi) + mm(weights_t, slope_lo)
    for n in range(4):
        total = None
        for i, (a, b) in enumerate(pair_list):
            if n not in (a, b):
                continue
            part = dproducts[i * MROWS : (i + 1) * MROWS, :]
            if a == b:
                part = 2.0 * part * moments[n]
            else:
                part = part * moments[b if n == a else a]
            total = part if total is None else total + part
        dmom[n * MROWS : (n + 1) * MROWS, :] = total

    for h in range(2):
        hs = slice(h * LANES, (h + 1) * LANES)
        radial = [geom[n, :, hs] for n in range(4)]
        dradial = [None] * 4
        sums = {}
        for m, (p, q, w) in enumerate(TRIPLES):
            coefficient = None
            for n in range(4):
                row = rows_of(dmom[n * MROWS + m : n * MROWS + m + 1, hs], ROWS)
                term = row if m == 0 else row * monos[m, :, hs]
                dradial[n] = term if dradial[n] is None else dradial[n] + term
                if m > 0:
                    term = row * radial[n]
                    coefficient = term if coefficient is None else coefficient + term
            if m == 0:
                continue
            for c, (power, prior) in enumerate(
                ((p, (p - 1, q, w)), (q, (p, q - 1, w)), (w, (p, q, w - 1)))
            ):
                if power == 0:
                    continue
                at = INDEX[prior]
                term = coefficient if at == 0 else coefficient * monos[at, :, hs]
                key = (c, power)
                sums[key] = term if key not in sums else sums[key] + term
        unit = [geom[8 + c, :, hs] for c in range(3)]
        inverse = geom[11, :, hs]
        along = None
        for n in range(4):
            term = geom[4 + n, :, hs] * dradial[n]
            along = term if along is None else along + term
        tangent = []
        for c in range(3):
            total = sums[(c, 1)]
            for power in (2, 3, 4):
                total = total + float(power) * sums[(c, power)]
            tangent.append(total * inverse)
        inner = unit[0] * tangent[0] + unit[1] * tangent[1] + unit[2] * tangent[2]
        along = along - inner
        for c in range(3):
            g = tangent[c] + unit[c] * along
            grads[c, :, hs] = g
            own_sum[h, c : c + 1, :] = jnp.sum(g, axis=0, keepdims=True)

    sub24 = lax.broadcasted_iota(jnp.int32, (24, 2 * LANES), 0)
    row_block = sub24 >> 2
    row_part = sub24 & 3
    spread = jnp.zeros((48, LANES), F32)
    for k in range(26):
        gx = rows_of(grads[0, k : k + 1, :], 24)
        gy = rows_of(grads[1, k : k + 1, :], 24)
        gz = rows_of(grads[2, k : k + 1, :], 24)
        value = jnp.where(row_part == 0, gx, jnp.where(row_part == 1, gy, gz))
        value = jnp.where(row_block == rows_of(blk[k : k + 1, :], 24), value, 0.0)
        hi = value.astype(BF16).astype(F32)
        pieces = jnp.concatenate([hi, value - hi], axis=0).astype(BF16)
        spread = spread + mm_nt(pieces, onehot[:, k * 2 * LANES : (k + 1) * 2 * LANES])
    spread = spread[0:24, :] + spread[24:48, :]
    first = spread[0:8, :]
    second = spread[8:16, :]
    third = spread[16:24, :]
    u_send[...] = second
    second_turned = pltpu.roll(second, 64, 1)
    third_turned = pltpu.roll(third, 64, 1)
    shifted = jnp.where(
        sub8 < 4, pltpu.roll(second_turned, 4, 0), pltpu.roll(third_turned, 4, 0)
    )
    r_send[...] = jnp.where(lane8 < 64, second_turned, shifted)
    for k in (4, 5, 6, 7, 0, 1, 2, 3):
        backward[k].start()

    t_row8 = rows_of(t_row, 8)
    up_tile = f_recv[slot(0, 1)]
    down_tile = f_recv[slot(0, -1)]
    table = jnp.where(sub8 < 4, pltpu.roll(up_tile, 6, 0), down_tile).astype(jnp.int32)
    through = lane_gather(t_row8, table & 127)
    start = jnp.where(sub8 < 4, 256, 288)
    through = jnp.where(table >= start, jnp.where(table < start + 32, through, -1), -1)
    direct = idx_pad[2:4, :]
    direct = jnp.where(direct < 256, direct, -1)
    open_rows = jnp.where((sub8 & 1) == 0, has_lower, has_upper) > 0
    through = jnp.where(open_rows, through, -1)
    direct = jnp.where(open_rows[0:2, :], direct, -1)
    rows = [direct[0:1, :], direct[1:2, :]] + [through[i : i + 1, :] for i in range(2, 6)]
    rows.append(jnp.where(lane_row < 64, t_row, -1))
    for i, row in enumerate(rows):
        at = slice(i * LANES, (i + 1) * LANES)
        hot0[:, at] = jnp.where(column128 == rows_of(row, LANES), 1.0, 0.0).astype(BF16)
        if i < 2:
            hot1[:, at] = jnp.where(
                column128 + LANES == rows_of(row, LANES), 1.0, 0.0
            ).astype(BF16)
    out_energy[:, 0:LANES] = energy[:, 0:LANES] * keep0
    out_energy[:, LANES:] = energy[:, LANES:] * keep1
    grad0 = first - own_sum[0]
    grad1 = pltpu.roll(first, 4, 0) - own_sum[1]

    for copy in backward:
        copy.wait_recv()
    back = jnp.concatenate(
        [
            pltpu.roll(b_recv[slot(-1, 0)], 4, 0),
            b_recv[slot(1, 0)],
            pltpu.roll(b_recv[slot(-1, 1)], 4, 0),
            b_recv[slot(1, 1)],
            pltpu.roll(b_recv[slot(-1, -1)], 4, 0),
            b_recv[slot(1, -1)],
            between(b_recv[slot(0, 1)], b_recv[slot(0, -1)]),
        ],
        axis=1,
    )
    back_hi = back.astype(BF16).astype(F32)
    back2 = jnp.concatenate([back_hi, back - back_hi], axis=0).astype(BF16)
    added0 = mm_nt(back2, hot0[...])
    added1 = mm_nt(back2[:, 0 : 2 * LANES], hot1[...])
    force0 = -(grad0 + added0[0:8, :] + added0[8:16, :])[0:3, :]
    velocity0 = half_velocity[:, 0:LANES] + kick_factor * force0
    ext[5, 0:3, :] = velocity0
    ext[6, 0:3, :] = force0
    leave8 = rows_of(leave_row, 8)
    for q, at in enumerate((0, 5, 6)):
        v_send[q] = lane_gather(ext[at], leave8) * rows_of(sending, 8)
    v_copy.start()
    force1 = -(grad1 + added1[0:8, :] + added1[8:16, :])[0:3, :]
    velocity1 = half_velocity[:, LANES:] + kick_factor * force1
    out_vel[:, 0:LANES] = velocity0 * rows_of(keep0, 3)
    out_force[:, 0:LANES] = force0 * rows_of(keep0, 3)
    out_vel[:, LANES:] = velocity1 * rows_of(keep1, 3)
    out_force[:, LANES:] = force1 * rows_of(keep1, 3)
    for copy in (*forward, *backward):
        copy.wait_send()
    v_copy.wait_send()
    v_copy.wait_recv()
    for q in range(3):
        out_arr[q] = jnp.where(s_me < n_shock - 1, v_recv[q, 0:3, 0:16], 0.0)


def kept(shape):
    return pltpu.VMEM(shape, F32)


def in_place(x):
    return pltpu.with_memory_space_constraint(x, pltpu.VMEM)


def finish(*refs):
    for i in range(5):
        refs[5 + i][...] = refs[i][...]


def whole_step(n_shock, n_trans, *args):
    (disp, vel, force, beta, alpha, live, trans_idx, shock_idx, block, lane, leave, count) = args
    table = contraction_table()
    inputs = (
        disp,
        vel,
        force,
        beta.reshape(1, 50),
        alpha,
        live,
        trans_idx,
        shock_idx,
        block,
        lane,
        leave.reshape(1, 16),
        count,
        jnp.asarray(lattice_rows()),
        jnp.asarray(table, BF16),
        jnp.asarray(table.T, BF16),
    )
    vmem = pl.BlockSpec(memory_space=pltpu.VMEM)
    tile = (8, LANES)
    shapes = ((3, 256), (3, 256), (3, 256), (1, 256), (3, 3, 16))
    outs = pl.pallas_call(
        functools.partial(kernel, n_shock, n_trans),
        out_shape=tuple(kept(shape) for shape in shapes),
        in_specs=[pl.BlockSpec(memory_space=pltpu.HBM)] * N_IN,
        out_specs=(vmem,) * 5,
        scratch_shapes=[
            (pltpu.SMEM if i in (5, 11) else pltpu.VMEM)(x.shape, x.dtype)
            for i, x in enumerate(inputs)
        ]
        + [
            pltpu.SemaphoreType.DMA((N_IN,)),
            pltpu.VMEM(tile, F32),
            pltpu.VMEM(tile, F32),
            pltpu.VMEM((8, *tile), F32),
            pltpu.VMEM(tile, F32),
            pltpu.VMEM(tile, F32),
            pltpu.VMEM((8, *tile), F32),
            pltpu.VMEM((3, *tile), F32),
            pltpu.VMEM((3, *tile), F32),
            pltpu.SemaphoreType.DMA((8,)),
            pltpu.SemaphoreType.DMA((8,)),
            pltpu.SemaphoreType.DMA((8,)),
            pltpu.SemaphoreType.DMA((8,)),
            pltpu.SemaphoreType.DMA((2,)),
            pltpu.VMEM((7, *tile), F32),
            pltpu.VMEM((ROWS, 256), jnp.int32),
            pltpu.VMEM((ROWS, 256), jnp.int32),
            pltpu.VMEM(tile, jnp.int32),
            pltpu.VMEM((3, ROWS, 256), F32),
            pltpu.VMEM((12, ROWS, 256), F32),
            pltpu.VMEM((35, ROWS, 256), F32),
            pltpu.VMEM((4 * MROWS, 256), F32),
            pltpu.VMEM((4 * MROWS, 256), F32),
            pltpu.VMEM((LANES, 26 * 256), BF16),
            pltpu.VMEM((LANES, LANES), F32),
            pltpu.VMEM((LANES, 7 * LANES), BF16),
            pltpu.VMEM((LANES, 2 * LANES), BF16),
            pltpu.VMEM((3, ROWS, 256), F32),
            pltpu.VMEM((2, *tile), F32),
        ],
        compiler_params=pltpu.CompilerParams(collective_id=0, has_side_effects=True),
        name="whole_step",
    )(*inputs)
    outs = [in_place(x) for x in outs]
    outs = pl.pallas_call(
        finish,
        out_shape=tuple(jax.ShapeDtypeStruct(shape, F32) for shape in shapes),
        in_specs=[vmem] * 5,
        out_specs=(vmem,) * 5,
        name="finish",
    )(*outs)
    return outs[0], outs[1], outs[2], outs[3].reshape(256), outs[4]


def solution(mesh):
    split_1 = P(None, ("shock", "trans"))
    split_0 = P(("shock", "trans"))
    in_specs = (
        split_1,
        split_1,
        split_1,
        P(),
        P(),
        split_0,
        split_1,
        split_1,
        split_1,
        split_1,
        split_0,
        split_0,
    )
    out_specs = (split_1, split_1, split_1, split_0, P(None, None, ("shock", "trans")))
    body = functools.partial(whole_step, mesh.shape["shock"], mesh.shape["trans"])
    return jax.shard_map(body, mesh=mesh, in_specs=in_specs, out_specs=out_specs, check_vma=False)
```

```python
import functools
import math

import jax
import jax.numpy as jnp
import numpy as np
from jax import lax
from jax.experimental import pallas as pl
from jax.experimental.pallas import tpu as pltpu
from jax.sharding import PartitionSpec as P

F32 = jnp.float32
BF16 = jnp.bfloat16
MESH = pl.DeviceIdType.MESH

kick_factor = 0.5
drift_step = 0.02
cutoff_radius = 4.2
radial_width = 0.35
radial_centers = (1.4, 1.9, 2.4, 2.9)
moment_scale = 0.25
pair_list = ((0, 0), (0, 1), (0, 2), (0, 3), (1, 1), (1, 2), (1, 3), (2, 2), (2, 3), (3, 3))
LANES = 128
ROWS = 32
MROWS = 40
DROWS = 64


def exponents():
    triples = []
    for degree in range(5):
        for p in range(degree, -1, -1):
            for q in range(degree - p, -1, -1):
                triples.append((p, q, degree - p - q))
    return triples


TRIPLES = exponents()
INDEX = {t: i for i, t in enumerate(TRIPLES)}


def lattice_rows():
    entries = []
    for number in range(8):
        entries.append(
            [1.0 - 2.0 * (number >> 2 & 1), 1.0 - 2.0 * (number >> 1 & 1), 1.0 - 2.0 * (number & 1)]
        )
    for axis_pick in range(3):
        for signed in (2.0, -2.0):
            vector = [0.0, 0.0, 0.0]
            vector[axis_pick] = signed
            entries.append(vector)
    for zero_pick in (2, 1, 0):
        others = [axis_pick for axis_pick in range(3) if axis_pick != zero_pick]
        for leading in (2.0, -2.0):
            for trailing in (2.0, -2.0):
                vector = [0.0, 0.0, 0.0]
                vector[others[0]] = leading
                vector[others[1]] = trailing
                entries.append(vector)
    while len(entries) < ROWS:
        entries.append([1.0, 1.0, 1.0])
    table = np.array(entries, dtype=np.float32).T
    return np.broadcast_to(table[:, :, None], (3, ROWS, LANES)).copy()


def contraction_table():
    table = np.zeros((DROWS, len(pair_list) * MROWS), dtype=np.float32)
    for i in range(len(pair_list)):
        for m, (p, q, w) in enumerate(TRIPLES):
            degree = p + q + w
            table[5 * i + degree, MROWS * i + m] = math.factorial(degree) / (
                math.factorial(p) * math.factorial(q) * math.factorial(w)
            )
    return table


def split(x):
    hi = x.astype(BF16)
    lo = (x - hi.astype(F32)).astype(BF16)
    return hi, lo


def mm(a, b):
    return lax.dot_general(a, b, (((1,), (0,)), ((), ())), preferred_element_type=F32)


def mm_nt(a, b):
    return lax.dot_general(a, b, (((1,), (1,)), ((), ())), preferred_element_type=F32)


def lane_gather(x, index):
    numbers = lax.GatherDimensionNumbers(
        offset_dims=(),
        collapsed_slice_dims=(1,),
        start_index_map=(1,),
        operand_batching_dims=(0,),
        start_indices_batching_dims=(0,),
    )
    return lax.gather(
        x,
        index[:, :, None],
        numbers,
        slice_sizes=(1, 1),
        mode=lax.GatherScatterMode.PROMISE_IN_BOUNDS,
    )


def rows_of(row, count):
    return jnp.broadcast_to(row, (count, row.shape[1]))


def sin_of(u):
    s = u * u
    r = -1.0 / 39916800.0
    for c in (1.0 / 362880.0, -1.0 / 5040.0, 1.0 / 120.0, -1.0 / 6.0, 1.0):
        r = r * s + c
    return r * u


def cos_of(u):
    s = u * u
    r = 1.0 / 479001600.0
    for c in (-1.0 / 3628800.0, 1.0 / 40320.0, -1.0 / 720.0, 1.0 / 24.0, -0.5, 1.0):
        r = r * s + c
    return r


DIRS = (
    (1, 1),
    (1, -1),
    (-1, 1),
    (-1, -1),
    (0, 1),
    (0, -1),
    (1, 0),
    (-1, 0),
    (-2, 1),
    (-2, -1),
    (-2, 0),
)
NEAR = 8
N_IN = 15


def kernel(n_shock, n_trans, *refs):
    hbm = refs[:N_IN]
    out_disp, out_vel, out_force, out_energy, out_arr = refs[N_IN : N_IN + 5]
    (
        disp,
        vel,
        force,
        beta,
        alpha,
        live,
        trans_idx,
        shock_idx,
        nb_block,
        nb_lane,
        leave_idx,
        leave_count,
        offs,
        wmat,
        wmat_t,
        in_sems,
        t_send,
        s_send,
        f_recv,
        m_send,
        b_recv,
        w_send,
        w_recv,
        c_send,
        c_recv,
        p_send,
        p_recv,
        f_send_sems,
        f_recv_sems,
        b_send_sems,
        b_recv_sems,
        x_send_sems,
        x_recv_sems,
        ext,
        blk,
        lan,
        idx_pad,
        near_own,
        geom,
        monos,
        mom,
        dmom,
        onehot,
        apad,
        hot0,
        hot1,
        arr_hot,
        grads,
        own_sum,
    ) = refs[N_IN + 5 :]
    local = (
        disp,
        vel,
        force,
        beta,
        alpha,
        live,
        trans_idx,
        shock_idx,
        nb_block,
        nb_lane,
        leave_idx,
        leave_count,
        offs,
        wmat,
        wmat_t,
    )
    loads = [
        pltpu.make_async_copy(src, dst, in_sems.at[i])
        for i, (src, dst) in enumerate(zip(hbm, local, strict=True))
    ]
    for i in (0, 1, 2, 6, 7, 8, 9, 10, 5, 11, 4, 3, 12, 13, 14):
        loads[i].start()

    s_me = lax.axis_index("shock")
    t_me = lax.axis_index("trans")

    def place(ds, dt):
        return (
            lax.rem(s_me + (ds + n_shock), n_shock),
            lax.rem(t_me + (dt + n_trans), n_trans),
        )

    inside = {
        -2: s_me > 1,
        -1: s_me > 0,
        0: None,
        1: s_me < n_shock - 1,
        2: s_me < n_shock - 2,
    }

    def where_inside(ds, action):
        if inside[ds] is None:
            action()
        else:
            pl.when(inside[ds])(action)

    def clear(ds):
        def action():
            for dt in (-1, 0, 1):
                k = DIRS.index((-ds, -dt))
                b_recv[k] = jnp.zeros((2, 8, LANES), F32)
                if k < NEAR:
                    f_recv[k] = jnp.zeros((8, LANES), F32)
            if ds == 1:
                w_recv[...] = jnp.zeros((8, LANES), F32)
                c_recv[...] = jnp.zeros((8, LANES), F32)
                p_recv[...] = jnp.zeros((8, LANES), F32)

        pl.when(jnp.logical_not(inside[ds]))(action)

    for ds in (-1, 1, 2):
        clear(ds)

    barrier = pltpu.get_barrier_semaphore()

    def greet(ds):
        def action():
            for dt in (-1, 0, 1):
                if (ds, dt) != (0, 0):
                    pl.semaphore_signal(
                        barrier, inc=1, device_id=place(ds, dt), device_id_type=MESH
                    )

        return action

    for ds in (0, 1, -1, 2, -2):
        where_inside(ds, greet(ds))
    peers = 2
    for ds in (1, -1, 2, -2):
        peers = peers + jnp.where(inside[ds], 3, 0)

    def remote(src, dst, send_sem, recv_sem, where):
        return pltpu.make_async_remote_copy(
            src_ref=src,
            dst_ref=dst,
            send_sem=send_sem,
            recv_sem=recv_sem,
            device_id=place(*where),
            device_id_type=MESH,
        )

    forward = [
        (
            ds,
            remote(
                s_send if dt == 0 else t_send,
                f_recv.at[k],
                f_send_sems.at[k],
                f_recv_sems.at[k],
                (ds, dt),
            ),
        )
        for k, (ds, dt) in enumerate(DIRS[:NEAR])
    ]
    backward = [
        (
            ds,
            remote(
                m_send if whole else m_send.at[0],
                b_recv.at[k] if whole else b_recv.at[k, 0],
                b_send_sems.at[k],
                b_recv_sems.at[k],
                (ds, dt),
            ),
        )
        for k, (ds, dt) in enumerate(DIRS)
        for whole in (dt != 0 and ds in (0, -1),)
    ]
    extra = [
        (-1, remote(src, dst, x_send_sems.at[i], x_recv_sems.at[i], (-1, 0)))
        for i, (src, dst) in enumerate(((w_send, w_recv), (c_send, c_recv), (p_send, p_recv)))
    ]

    def start(copies):
        for ds in (1, -1, 0, -2):
            chosen = [copy for at, copy in copies if at == ds]

            def action(chosen=chosen):
                for copy in chosen:
                    copy.start()

            if chosen:
                where_inside(ds, action)

    def receive(copies):
        for ds in (0, 1, -1, -2):
            chosen = [copy for at, copy in copies if at == ds]

            def action(chosen=chosen):
                for copy in chosen:
                    copy.wait_recv()

            if chosen:
                where_inside(-ds, action)

    def drain(copies):
        for ds in (0, 1, -1, -2):
            chosen = [copy for at, copy in copies if at == ds]

            def action(chosen=chosen):
                for copy in chosen:
                    copy.wait_send()

            if chosen:
                where_inside(ds, action)

    def slot(ds, dt):
        return DIRS.index((-ds, -dt))

    lane_row = lax.broadcasted_iota(jnp.int32, (1, LANES), 1)
    lane8 = lax.broadcasted_iota(jnp.int32, (8, LANES), 1)
    sub8 = lax.broadcasted_iota(jnp.int32, (8, LANES), 0)

    idx_pad[...] = jnp.zeros_like(idx_pad)
    ext[...] = jnp.zeros_like(ext)
    for i in (0, 1, 2, 6, 7, 10, 11):
        loads[i].wait()
    half_velocity = vel[...] + kick_factor * force[...]
    displaced = disp[...] + drift_step * half_velocity
    for h in range(2):
        ext[h, 0:3, :] = displaced[:, h * LANES : (h + 1) * LANES]
    idx_pad[0:1, 0:32] = trans_idx[1:2, :]
    idx_pad[1:2, 0:32] = trans_idx[0:1, :]
    idx_pad[2:4, :] = shock_idx[...]
    t_row = jnp.where(lane_row < 32, idx_pad[0:1, :], pltpu.roll(idx_pad[1:2, :], 32, 1))
    shock8 = jnp.where(sub8 < 4, rows_of(idx_pad[2:3, :], 8), rows_of(idx_pad[3:4, :], 8))
    shock_block = shock8 >> 7
    shock_lane = shock8 & 127
    doubled = [jnp.where(sub8 < 4, ext[b], pltpu.roll(ext[b], 4, 0)) for b in range(2)]
    t_send[...] = lane_gather(ext[0], rows_of(t_row, 8))
    t_send[4:6, :] = shock_idx[...].astype(F32)
    s_own = jnp.where(
        shock_block == 0,
        lane_gather(doubled[0], shock_lane),
        jnp.where(shock_block == 1, lane_gather(doubled[1], shock_lane), 0.0),
    )
    s_send[...] = jnp.where((sub8 & 3) == 3, shock8.astype(F32), s_own)

    idx_pad[4:5, 0:16] = leave_idx[...]
    leave_row = idx_pad[4:5, :]
    sending = jnp.where(lane_row < leave_count[0], 1.0, 0.0)
    for h in range(2):
        ext[5 + h, 0:3, :] = half_velocity[:, h * LANES : (h + 1) * LANES]
    leaving = jnp.where(sub8 < 4, ext[0], pltpu.roll(ext[5], 4, 0))
    w_send[...] = lane_gather(leaving, rows_of(leave_row, 8)) * rows_of(sending, 8)

    pl.semaphore_wait(barrier, peers)
    start(forward)
    start(extra[0:1])

    for i in (8, 9, 5, 4, 3):
        loads[i].wait()
    blk[...] = jnp.full_like(blk, -1)
    lan[...] = jnp.zeros_like(lan)
    blk[0:26, :] = nb_block[...]
    lan[0:26, :] = nb_lane[...] & 127
    column = lax.broadcasted_iota(jnp.int32, (LANES, 2 * LANES), 0)

    def fill_onehot(k, carry):
        row = lan[pl.ds(k, 1), :]
        hot = jnp.where(column == rows_of(row, LANES), 1.0, 0.0).astype(BF16)
        onehot[:, pl.ds(pl.multiple_of(k * 2 * LANES, 2 * LANES), 2 * LANES)] = hot
        return carry

    lax.fori_loop(0, 26, fill_onehot, 0)
    for i in (12, 13, 14):
        loads[i].wait()
    for h in range(2):
        hs = slice(h * LANES, (h + 1) * LANES)
        for c in range(3):
            found = offs[c] - rows_of(ext[h, c : c + 1, :], ROWS)
            parts = [
                lane_gather(rows_of(ext[b, c : c + 1, :], ROWS), lan[:, hs]) for b in range(2)
            ]
            block = blk[:, hs]
            near_own[c, :, hs] = found + jnp.where(
                block == 0, parts[0], jnp.where(block == 1, parts[1], 0.0)
            )

    column128 = lax.broadcasted_iota(jnp.int32, (LANES, LANES), 0)
    leave_hot = jnp.where(column128 == rows_of(leave_row, LANES), 1.0, 0.0).astype(BF16)
    departed = mm_nt(rows_of(sending, 16).astype(BF16), leave_hot)[0:1, :]
    keep0 = jnp.where(lane_row < live[0], 1.0, 0.0) * (1.0 - departed)
    keep1 = jnp.where(lane_row + LANES < live[0], 1.0, 0.0)
    out_disp[:, 0:LANES] = displaced[:, 0:LANES] * rows_of(keep0, 3)
    out_disp[:, LANES:] = displaced[:, LANES:] * rows_of(keep1, 3)

    apad[...] = jnp.zeros_like(apad)
    apad[0:50, 0:50] = alpha[...]
    sym = 0.5 * (apad[...] + apad[...].T)
    sym_hi, sym_lo = split(sym[0:DROWS, 0:DROWS])
    apad[0:1, :] = jnp.zeros((1, LANES), F32)
    apad[0:1, 0:50] = beta[...]
    beta_col = rows_of(apad[0:1, :], LANES).T[0:DROWS, :]
    beta_col = jnp.concatenate([beta_col, beta_col], axis=1)
    for n in range(4):
        mom[n * MROWS + 32 : (n + 1) * MROWS, :] = jnp.zeros((8, 2 * LANES), F32)

    receive(forward)

    def between(lower, upper):
        return jnp.where(lane8 < 32, lower, jnp.where(lane8 < 64, upper, 0.0))

    t_ghost = between(f_recv[slot(0, -1)], f_recv[slot(0, 1)])
    from_low = f_recv[slot(-1, 0)]
    from_up = f_recv[slot(1, 0)]
    lists = jnp.where(sub8 < 4, rows_of(from_low[7:8, :], 8), rows_of(from_up[3:4, :], 8))
    lists = lists.astype(jnp.int32)
    across = jnp.where(
        sub8 < 4,
        between(f_recv[slot(-1, -1)], f_recv[slot(-1, 1)]),
        pltpu.roll(between(f_recv[slot(1, -1)], f_recv[slot(1, 1)]), 4, 0),
    )
    direct = jnp.where(sub8 < 4, pltpu.roll(from_low, 4, 0), pltpu.roll(from_up, 4, 0))
    both = jnp.where(lists >= 256, lane_gather(across, lists & 127), direct)
    turned = pltpu.roll(both, 64, 1)
    swapped = pltpu.roll(turned, 4, 0)
    ext[2] = jnp.where(lane8 < 64, t_ghost, turned)
    ext[3] = jnp.where(lane8 < 64, turned, swapped)
    ext[4] = swapped

    table = jnp.where(
        sub8 < 4, pltpu.roll(f_recv[slot(0, 1)], 6, 0), f_recv[slot(0, -1)]
    ).astype(jnp.int32)
    through = lane_gather(rows_of(t_row, 8), table & 127)
    first_of = jnp.where(sub8 < 4, 256, 288)
    through = jnp.where(table >= first_of, jnp.where(table < first_of + 32, through, -1), -1)
    direct = idx_pad[2:4, :]
    c_send[...] = through.astype(F32)
    c_send[0:2, :] = jnp.where(direct < 256, direct, -1).astype(F32)
    c_send[6:7, :] = jnp.where(lane_row < 64, t_row, -1).astype(F32)
    c_send[7:8, :] = jnp.where(sending > 0.0, leave_row, -2).astype(F32)

    for h in range(2):
        hs = slice(h * LANES, (h + 1) * LANES)
        block = blk[:, hs]
        lane = lan[:, hs]
        parts = []
        for c in range(3):
            found = jnp.zeros((ROWS, LANES), F32)
            for b in range(2, 5):
                value = lane_gather(rows_of(ext[b, c : c + 1, :], ROWS), lane)
                found = jnp.where(block == b, value, found)
            parts.append(near_own[c, :, hs] + found)
        px, py, pz = parts
        square = px * px + py * py + pz * pz
        inverse = lax.rsqrt(square)
        distance = square * inverse
        ux, uy, uz = px * inverse, py * inverse, pz * inverse
        angle = (0.5 * math.pi) - (0.5 * math.pi / cutoff_radius) * distance
        sine, cosine = sin_of(angle), cos_of(angle)
        scale = jnp.where(block >= 0, moment_scale, 0.0)
        smooth = scale * sine * sine
        slope = scale * (-math.pi / cutoff_radius) * sine * cosine
        radial = []
        for n, center in enumerate(radial_centers):
            z = (distance - center) * (1.0 / radial_width)
            e = jnp.exp(-(z * z))
            r = smooth * e
            radial.append(r)
            geom[n, :, hs] = r
            geom[4 + n, :, hs] = slope * e - (2.0 / radial_width) * z * r
        geom[8, :, hs] = ux
        geom[9, :, hs] = uy
        geom[10, :, hs] = uz
        geom[11, :, hs] = inverse
        values = {}
        for m, (p, q, w) in enumerate(TRIPLES):
            if m == 0:
                value = None
            elif p > 0:
                prior = values[(p - 1, q, w)]
                value = ux if prior is None else prior * ux
            elif q > 0:
                prior = values[(p, q - 1, w)]
                value = uy if prior is None else prior * uy
            else:
                prior = values[(p, q, w - 1)]
                value = uz if prior is None else prior * uz
            values[(p, q, w)] = value
            if value is not None:
                monos[m, :, hs] = value
            for n in range(4):
                term = radial[n] if value is None else radial[n] * value
                mom[n * MROWS + m : n * MROWS + m + 1, hs] = jnp.sum(term, axis=0, keepdims=True)

    moments = [mom[n * MROWS : (n + 1) * MROWS, :] for n in range(4)]
    products = jnp.concatenate([moments[n] * moments[o] for n, o in pair_list], axis=0)
    prod_hi, prod_lo = split(products)
    weights = wmat[...]
    descriptor = mm(weights, prod_hi) + mm(weights, prod_lo)
    desc_hi, desc_lo = split(descriptor)
    quadratic = mm(sym_hi, desc_hi) + mm(sym_lo, desc_hi) + mm(sym_hi, desc_lo)
    energy = jnp.sum(descriptor * (beta_col + 0.5 * quadratic), axis=0, keepdims=True)
    slope_hi, slope_lo = split(beta_col + quadratic)
    weights_t = wmat_t[...]
    dproducts = mm(weights_t, slope_hi) + mm(weights_t, slope_lo)
    for n in range(4):
        total = None
        for i, (a, b) in enumerate(pair_list):
            if n not in (a, b):
                continue
            part = dproducts[i * MROWS : (i + 1) * MROWS, :]
            if a == b:
                part = 2.0 * part * moments[n]
            else:
                part = part * moments[b if n == a else a]
            total = part if total is None else total + part
        dmom[n * MROWS : (n + 1) * MROWS, :] = total

    for h in range(2):
        hs = slice(h * LANES, (h + 1) * LANES)
        radial = [geom[n, :, hs] for n in range(4)]
        dradial = [None] * 4
        sums = {}
        for m, (p, q, w) in enumerate(TRIPLES):
            coefficient = None
            for n in range(4):
                row = rows_of(dmom[n * MROWS + m : n * MROWS + m + 1, hs], ROWS)
                term = row if m == 0 else row * monos[m, :, hs]
                dradial[n] = term if dradial[n] is None else dradial[n] + term
                if m > 0:
                    term = row * radial[n]
                    coefficient = term if coefficient is None else coefficient + term
            if m == 0:
                continue
            for c, (power, prior) in enumerate(
                ((p, (p - 1, q, w)), (q, (p, q - 1, w)), (w, (p, q, w - 1)))
            ):
                if power == 0:
                    continue
                at = INDEX[prior]
                term = coefficient if at == 0 else coefficient * monos[at, :, hs]
                key = (c, power)
                sums[key] = term if key not in sums else sums[key] + term
        unit = [geom[8 + c, :, hs] for c in range(3)]
        inverse = geom[11, :, hs]
        along = None
        for n in range(4):
            term = geom[4 + n, :, hs] * dradial[n]
            along = term if along is None else along + term
        tangent = []
        for c in range(3):
            total = sums[(c, 1)]
            for power in (2, 3, 4):
                total = total + float(power) * sums[(c, power)]
            tangent.append(total * inverse)
        inner = unit[0] * tangent[0] + unit[1] * tangent[1] + unit[2] * tangent[2]
        along = along - inner
        for c in range(3):
            g = tangent[c] + unit[c] * along
            grads[c, :, hs] = g
            own_sum[h, c : c + 1, :] = jnp.sum(g, axis=0, keepdims=True)

    sub24 = lax.broadcasted_iota(jnp.int32, (24, 2 * LANES), 0)
    row_block = sub24 >> 2
    row_part = sub24 & 3
    spread = jnp.zeros((48, LANES), F32)
    for k in range(26):
        gx = rows_of(grads[0, k : k + 1, :], 24)
        gy = rows_of(grads[1, k : k + 1, :], 24)
        gz = rows_of(grads[2, k : k + 1, :], 24)
        value = jnp.where(row_part == 0, gx, jnp.where(row_part == 1, gy, gz))
        value = jnp.where(row_block == rows_of(blk[k : k + 1, :], 24), value, 0.0)
        hi = value.astype(BF16).astype(F32)
        pieces = jnp.concatenate([hi, value - hi], axis=0).astype(BF16)
        spread = spread + mm_nt(pieces, onehot[:, k * 2 * LANES : (k + 1) * 2 * LANES])
    spread = spread[0:24, :] + spread[24:48, :]
    first = spread[0:8, :]
    second = spread[8:16, :]
    third = spread[16:24, :]
    second_turned = pltpu.roll(second, 64, 1)
    third_turned = pltpu.roll(third, 64, 1)
    shifted = jnp.where(
        sub8 < 4, pltpu.roll(second_turned, 4, 0), pltpu.roll(third_turned, 4, 0)
    )
    grad0 = first - own_sum[0]
    m_send[1] = second
    m_send[0] = jnp.where(lane8 < 64, second_turned, shifted)
    p_send[...] = jnp.where(sub8 < 3, grad0, 0.0)
    start(backward)
    start(extra[1:3])

    rows = [c_send[i : i + 1, :].astype(jnp.int32) for i in range(7)]
    for i, row in enumerate(rows):
        at = slice(i * LANES, (i + 1) * LANES)
        hot0[:, at] = jnp.where(column128 == rows_of(row, LANES), 1.0, 0.0).astype(BF16)
        if i < 2:
            hot1[:, at] = jnp.where(
                column128 + LANES == rows_of(row, LANES), 1.0, 0.0
            ).astype(BF16)
    out_energy[:, 0:LANES] = energy[:, 0:LANES] * keep0
    out_energy[:, LANES:] = energy[:, LANES:] * keep1
    grad1 = pltpu.roll(first, 4, 0) - own_sum[1]

    receive(extra[0:2])
    slots = rows_of(c_recv[7:8, :], LANES).T[0:16, :]
    for i in range(8):
        row = lane_row.astype(F32) if i == 7 else c_recv[i : i + 1, :]
        arr_hot[:, i * LANES : (i + 1) * LANES] = jnp.where(
            rows_of(row, 16) == slots, 1.0, 0.0
        ).astype(BF16)

    receive(backward)
    receive(extra[2:3])

    def lower_of(ds, dt):
        return b_recv[slot(ds, dt), 0]

    def upper_of(ds, dt):
        return pltpu.roll(b_recv[slot(ds, dt), 0], 4, 0)

    def pieces_of(tiles):
        back = jnp.concatenate([jnp.where(sub8 < 3, tile, 0.0) for tile in tiles], axis=1)
        hi = back.astype(BF16).astype(F32)
        return jnp.concatenate([hi, back - hi], axis=0).astype(BF16)

    back = pieces_of(
        (
            upper_of(-1, 0),
            lower_of(1, 0),
            upper_of(-1, 1),
            lower_of(1, 1),
            upper_of(-1, -1),
            lower_of(1, -1),
            between(b_recv[slot(0, 1), 1], b_recv[slot(0, -1), 1]),
        )
    )
    added0 = mm_nt(back, hot0[...])
    added1 = mm_nt(back[:, 0 : 2 * LANES], hot1[...])
    arriving = pieces_of(
        (
            pltpu.roll(m_send[0], 4, 0),
            lower_of(2, 0),
            upper_of(0, 1),
            lower_of(2, 1),
            upper_of(0, -1),
            lower_of(2, -1),
            between(b_recv[slot(1, 1), 1], b_recv[slot(1, -1), 1]),
            p_recv[...],
        )
    )
    added2 = mm_nt(arriving, arr_hot[...])
    force0 = -(grad0 + added0[0:8, :] + added0[8:16, :])[0:3, :]
    velocity0 = half_velocity[:, 0:LANES] + kick_factor * force0
    force1 = -(grad1 + added1[0:8, :] + added1[8:16, :])[0:3, :]
    velocity1 = half_velocity[:, LANES:] + kick_factor * force1
    force2 = -(added2[0:8, :] + added2[8:16, :])[0:3, :]
    state = w_recv[...]
    out_vel[:, 0:LANES] = velocity0 * rows_of(keep0, 3)
    out_force[:, 0:LANES] = force0 * rows_of(keep0, 3)
    out_vel[:, LANES:] = velocity1 * rows_of(keep1, 3)
    out_force[:, LANES:] = force1 * rows_of(keep1, 3)
    for q, value in enumerate(
        (state[0:3, 0:16], state[4:7, 0:16] + kick_factor * force2, force2)
    ):
        out_arr[q] = jnp.where(s_me < n_shock - 1, value, 0.0)
    drain(forward)
    drain(backward)
    drain(extra)


def kept(shape):
    return pltpu.VMEM(shape, F32)


def in_place(x):
    return pltpu.with_memory_space_constraint(x, pltpu.VMEM)


def finish(*refs):
    for i in range(5):
        refs[5 + i][...] = refs[i][...]


def whole_step(n_shock, n_trans, *args):
    (disp, vel, force, beta, alpha, live, trans_idx, shock_idx, block, lane, leave, count) = args
    table = contraction_table()
    inputs = (
        disp,
        vel,
        force,
        beta.reshape(1, 50),
        alpha,
        live,
        trans_idx,
        shock_idx,
        block,
        lane,
        leave.reshape(1, 16),
        count,
        jnp.asarray(lattice_rows()),
        jnp.asarray(table, BF16),
        jnp.asarray(table.T, BF16),
    )
    vmem = pl.BlockSpec(memory_space=pltpu.VMEM)
    tile = (8, LANES)
    shapes = ((3, 256), (3, 256), (3, 256), (1, 256), (3, 3, 16))
    outs = pl.pallas_call(
        functools.partial(kernel, n_shock, n_trans),
        out_shape=tuple(kept(shape) for shape in shapes),
        in_specs=[pl.BlockSpec(memory_space=pltpu.HBM)] * N_IN,
        out_specs=(vmem,) * 5,
        scratch_shapes=[
            (pltpu.SMEM if i in (5, 11) else pltpu.VMEM)(x.shape, x.dtype)
            for i, x in enumerate(inputs)
        ]
        + [
            pltpu.SemaphoreType.DMA((N_IN,)),
            pltpu.VMEM(tile, F32),
            pltpu.VMEM(tile, F32),
            pltpu.VMEM((NEAR, *tile), F32),
            pltpu.VMEM((2, *tile), F32),
            pltpu.VMEM((len(DIRS), 2, *tile), F32),
            pltpu.VMEM(tile, F32),
            pltpu.VMEM(tile, F32),
            pltpu.VMEM(tile, F32),
            pltpu.VMEM(tile, F32),
            pltpu.VMEM(tile, F32),
            pltpu.VMEM(tile, F32),
            pltpu.SemaphoreType.DMA((NEAR,)),
            pltpu.SemaphoreType.DMA((NEAR,)),
            pltpu.SemaphoreType.DMA((len(DIRS),)),
            pltpu.SemaphoreType.DMA((len(DIRS),)),
            pltpu.SemaphoreType.DMA((3,)),
            pltpu.SemaphoreType.DMA((3,)),
            pltpu.VMEM((7, *tile), F32),
            pltpu.VMEM((ROWS, 256), jnp.int32),
            pltpu.VMEM((ROWS, 256), jnp.int32),
            pltpu.VMEM(tile, jnp.int32),
            pltpu.VMEM((3, ROWS, 256), F32),
            pltpu.VMEM((12, ROWS, 256), F32),
            pltpu.VMEM((35, ROWS, 256), F32),
            pltpu.VMEM((4 * MROWS, 256), F32),
            pltpu.VMEM((4 * MROWS, 256), F32),
            pltpu.VMEM((LANES, 26 * 256), BF16),
            pltpu.VMEM((LANES, LANES), F32),
            pltpu.VMEM((LANES, 7 * LANES), BF16),
            pltpu.VMEM((LANES, 2 * LANES), BF16),
            pltpu.VMEM((16, 8 * LANES), BF16),
            pltpu.VMEM((3, ROWS, 256), F32),
            pltpu.VMEM((2, *tile), F32),
        ],
        compiler_params=pltpu.CompilerParams(collective_id=0, has_side_effects=True),
        name="whole_step",
    )(*inputs)
    outs = [in_place(x) for x in outs]
    outs = pl.pallas_call(
        finish,
        out_shape=tuple(jax.ShapeDtypeStruct(shape, F32) for shape in shapes),
        in_specs=[vmem] * 5,
        out_specs=(vmem,) * 5,
        name="finish",
    )(*outs)
    return outs[0], outs[1], outs[2], outs[3].reshape(256), outs[4]


def solution(mesh):
    split_1 = P(None, ("shock", "trans"))
    split_0 = P(("shock", "trans"))
    in_specs = (
        split_1,
        split_1,
        split_1,
        P(),
        P(),
        split_0,
        split_1,
        split_1,
        split_1,
        split_1,
        split_0,
        split_0,
    )
    out_specs = (split_1, split_1, split_1, split_0, P(None, None, ("shock", "trans")))
    body = functools.partial(whole_step, mesh.shape["shock"], mesh.shape["trans"])
    return jax.shard_map(body, mesh=mesh, in_specs=in_specs, out_specs=out_specs, check_vma=False)
```

```python
import functools
import math

import jax
import jax.numpy as jnp
import numpy as np
from jax import lax
from jax.experimental import pallas as pl
from jax.experimental.pallas import tpu as pltpu
from jax.sharding import PartitionSpec as P

F32 = jnp.float32
BF16 = jnp.bfloat16
MESH = pl.DeviceIdType.MESH

kick_factor = 0.5
drift_step = 0.02
cutoff_radius = 4.2
radial_width = 0.35
radial_centers = (1.4, 1.9, 2.4, 2.9)
moment_scale = 0.25
pair_list = ((0, 0), (0, 1), (0, 2), (0, 3), (1, 1), (1, 2), (1, 3), (2, 2), (2, 3), (3, 3))
LANES = 128
ROWS = 56
CHUNKS = ((0, 16), (16, 32), (32, 48), (48, 56))
MROWS = 40
DROWS = 64


def exponents():
    triples = []
    for degree in range(5):
        for p in range(degree, -1, -1):
            for q in range(degree - p, -1, -1):
                triples.append((p, q, degree - p - q))
    return triples


TRIPLES = exponents()
INDEX = {t: i for i, t in enumerate(TRIPLES)}
BASIS = [t for t in TRIPLES if t[2] < 2]
PLACE = {t: i for i, t in enumerate(BASIS)}


def reduced(t):
    p, q, w = t
    return (p, q, w - 2), (p + 2, q, w - 2), (p, q + 2, w - 2)


def lattice_rows():
    entries = []
    for number in range(8):
        entries.append(
            [1.0 - 2.0 * (number >> 2 & 1), 1.0 - 2.0 * (number >> 1 & 1), 1.0 - 2.0 * (number & 1)]
        )
    for axis_pick in range(3):
        for signed in (2.0, -2.0):
            vector = [0.0, 0.0, 0.0]
            vector[axis_pick] = signed
            entries.append(vector)
    for zero_pick in (2, 1, 0):
        others = [axis_pick for axis_pick in range(3) if axis_pick != zero_pick]
        for leading in (2.0, -2.0):
            for trailing in (2.0, -2.0):
                vector = [0.0, 0.0, 0.0]
                vector[others[0]] = leading
                vector[others[1]] = trailing
                entries.append(vector)
    while len(entries) < ROWS // 2:
        entries.append([1.0, 1.0, 1.0])
    table = np.repeat(np.array(entries, dtype=np.float32), 2, axis=0).T
    return np.broadcast_to(table[:, :, None], (3, ROWS, LANES)).copy()


def contraction_table():
    table = np.zeros((DROWS, len(pair_list) * MROWS), dtype=np.float32)
    for i in range(len(pair_list)):
        for m, (p, q, w) in enumerate(TRIPLES):
            degree = p + q + w
            table[5 * i + degree, MROWS * i + m] = math.factorial(degree) / (
                math.factorial(p) * math.factorial(q) * math.factorial(w)
            )
    return table


def split(x):
    hi = x.astype(BF16)
    lo = (x - hi.astype(F32)).astype(BF16)
    return hi, lo


def mm(a, b):
    return lax.dot_general(a, b, (((1,), (0,)), ((), ())), preferred_element_type=F32)


def mm_nt(a, b):
    return lax.dot_general(a, b, (((1,), (1,)), ((), ())), preferred_element_type=F32)


def lane_gather(x, index):
    numbers = lax.GatherDimensionNumbers(
        offset_dims=(),
        collapsed_slice_dims=(1,),
        start_index_map=(1,),
        operand_batching_dims=(0,),
        start_indices_batching_dims=(0,),
    )
    return lax.gather(
        x,
        index[:, :, None],
        numbers,
        slice_sizes=(1, 1),
        mode=lax.GatherScatterMode.PROMISE_IN_BOUNDS,
    )


def rows_of(row, count):
    return jnp.broadcast_to(row, (count, row.shape[1]))


def over(tile, count):
    return jnp.concatenate([tile] * count, axis=0) if count > 1 else tile


def row_sums(x):
    total = x[0:8, :]
    for i in range(8, x.shape[0], 8):
        total = total + x[i : i + 8, :]
    total = total + pltpu.roll(total, 4, 0)
    return total + pltpu.roll(total, 2, 0)


def horner(x, value, slope, term):
    if value is None:
        return term, None
    slope = value if slope is None else slope * x + value
    return value * x + term, slope


def sin_of(u):
    s = u * u
    r = -1.0 / 39916800.0
    for c in (1.0 / 362880.0, -1.0 / 5040.0, 1.0 / 120.0, -1.0 / 6.0, 1.0):
        r = r * s + c
    return r * u


def cos_of(u):
    s = u * u
    r = 1.0 / 479001600.0
    for c in (-1.0 / 3628800.0, 1.0 / 40320.0, -1.0 / 720.0, 1.0 / 24.0, -0.5, 1.0):
        r = r * s + c
    return r


DIRS = (
    (1, 1),
    (1, -1),
    (-1, 1),
    (-1, -1),
    (0, 1),
    (0, -1),
    (1, 0),
    (-1, 0),
    (-2, 1),
    (-2, -1),
    (-2, 0),
)
NEAR = 8
N_IN = 13


def kernel(n_shock, n_trans, *refs):
    hbm = refs[:N_IN]
    live, leave_count = refs[N_IN : N_IN + 2]
    out_disp, out_vel, out_force, out_energy, out_arr = refs[N_IN + 2 : N_IN + 7]
    (
        disp,
        vel,
        force,
        beta,
        alpha,
        trans_idx,
        shock_idx,
        nb_block,
        nb_lane,
        leave_idx,
        offs,
        wmat,
        wmat_t,
        in_sems,
        t_send,
        s_send,
        f_recv,
        m_send,
        b_recv,
        w_send,
        w_recv,
        c_send,
        c_recv,
        p_send,
        p_recv,
        f_send_sems,
        f_recv_sems,
        b_send_sems,
        b_recv_sems,
        x_send_sems,
        x_recv_sems,
        ext,
        blk,
        lan,
        idx_pad,
        near_own,
        geom,
        tiles,
        mom,
        dmom,
        onehot,
        apad,
        hot0,
        hot1,
        arr_hot,
        grads,
        own_sum,
    ) = refs[N_IN + 7 :]
    local = (
        disp,
        vel,
        force,
        beta,
        alpha,
        trans_idx,
        shock_idx,
        nb_block,
        nb_lane,
        leave_idx,
        offs,
        wmat,
        wmat_t,
    )
    loads = [
        pltpu.make_async_copy(src, dst, in_sems.at[i])
        for i, (src, dst) in enumerate(zip(hbm, local, strict=True))
    ]
    s_me = lax.axis_index("shock")
    t_me = lax.axis_index("trans")

    t_near = {
        -1: jnp.where(t_me > 0, t_me - 1, n_trans - 1),
        0: t_me,
        1: jnp.where(t_me < n_trans - 1, t_me + 1, 0),
    }

    def place(ds, dt):
        return s_me + ds, t_near[dt]

    inside = {
        -2: s_me > 1,
        -1: s_me > 0,
        0: None,
        1: s_me < n_shock - 1,
        2: s_me < n_shock - 2,
    }

    def where_inside(ds, action):
        if inside[ds] is None:
            action()
        else:
            pl.when(inside[ds])(action)

    def clear(ds):
        def action():
            for dt in (-1, 0, 1):
                k = DIRS.index((-ds, -dt))
                b_recv[k] = jnp.zeros((2, 8, LANES), F32)
                if k < NEAR:
                    f_recv[k] = jnp.zeros((8, LANES), F32)
            if ds == 1:
                w_recv[...] = jnp.zeros((8, LANES), F32)
                c_recv[...] = jnp.zeros((8, LANES), F32)
                p_recv[...] = jnp.zeros((8, LANES), F32)

        pl.when(jnp.logical_not(inside[ds]))(action)

    barrier = pltpu.get_barrier_semaphore()

    def greet(ds):
        def action():
            for dt in (-1, 0, 1):
                if (ds, dt) != (0, 0):
                    pl.semaphore_signal(
                        barrier, inc=1, device_id=place(ds, dt), device_id_type=MESH
                    )

        return action

    for ds in (0, 1, -1, 2, -2):
        where_inside(ds, greet(ds))
    for i in (0, 1, 2, 5, 6, 7, 8, 9, 4, 3, 10, 11, 12):
        loads[i].start()
    peers = 2
    for ds in (1, -1, 2, -2):
        peers = peers + jnp.where(inside[ds], 3, 0)

    def remote(src, dst, send_sem, recv_sem, where):
        return pltpu.make_async_remote_copy(
            src_ref=src,
            dst_ref=dst,
            send_sem=send_sem,
            recv_sem=recv_sem,
            device_id=place(*where),
            device_id_type=MESH,
        )

    forward = [
        (
            ds,
            remote(
                s_send if dt == 0 else t_send,
                f_recv.at[k],
                f_send_sems.at[k],
                f_recv_sems.at[k],
                (ds, dt),
            ),
        )
        for k, (ds, dt) in enumerate(DIRS[:NEAR])
    ]
    backward = [
        (
            ds,
            remote(
                m_send if whole else m_send.at[0],
                b_recv.at[k] if whole else b_recv.at[k, 0],
                b_send_sems.at[k],
                b_recv_sems.at[k],
                (ds, dt),
            ),
        )
        for k, (ds, dt) in enumerate(DIRS)
        for whole in (dt != 0 and ds in (0, -1),)
    ]
    extra = [
        (-1, remote(src, dst, x_send_sems.at[i], x_recv_sems.at[i], (-1, 0)))
        for i, (src, dst) in enumerate(((w_send, w_recv), (c_send, c_recv), (p_send, p_recv)))
    ]

    def start(copies):
        for ds in (1, -1, 0, -2):
            chosen = [copy for at, copy in copies if at == ds]

            def action(chosen=chosen):
                for copy in chosen:
                    copy.start()

            if chosen:
                where_inside(ds, action)

    def receive(copies):
        for ds in (0, 1, -1, -2):
            chosen = [copy for at, copy in copies if at == ds]

            def action(chosen=chosen):
                for copy in chosen:
                    copy.wait_recv()

            if chosen:
                where_inside(-ds, action)

    def drain(copies):
        for ds in (0, 1, -1, -2):
            chosen = [copy for at, copy in copies if at == ds]

            def action(chosen=chosen):
                for copy in chosen:
                    copy.wait_send()

            if chosen:
                where_inside(ds, action)

    def slot(ds, dt):
        return DIRS.index((-ds, -dt))

    lane_row = lax.broadcasted_iota(jnp.int32, (1, LANES), 1)
    lane8 = lax.broadcasted_iota(jnp.int32, (8, LANES), 1)
    sub8 = lax.broadcasted_iota(jnp.int32, (8, LANES), 0)

    idx_pad[...] = jnp.zeros_like(idx_pad)
    ext[...] = jnp.zeros_like(ext)
    for i in (0, 1, 2, 5, 6):
        loads[i].wait()
    half_velocity = vel[...] + kick_factor * force[...]
    displaced = disp[...] + drift_step * half_velocity
    for h in range(2):
        ext[h, 0:3, :] = displaced[:, h * LANES : (h + 1) * LANES]
    idx_pad[0:1, 0:32] = trans_idx[1:2, :]
    idx_pad[1:2, 0:32] = trans_idx[0:1, :]
    idx_pad[2:4, :] = shock_idx[...]
    t_row = jnp.where(lane_row < 32, idx_pad[0:1, :], pltpu.roll(idx_pad[1:2, :], 32, 1))
    shock8 = jnp.where(sub8 < 4, rows_of(idx_pad[2:3, :], 8), rows_of(idx_pad[3:4, :], 8))
    shock_block = shock8 >> 7
    shock_lane = shock8 & 127
    doubled = [jnp.where(sub8 < 4, ext[b], pltpu.roll(ext[b], 4, 0)) for b in range(2)]
    t_send[...] = lane_gather(ext[0], rows_of(t_row, 8))
    t_send[4:6, :] = shock_idx[...].astype(F32)
    s_own = jnp.where(
        shock_block == 0,
        lane_gather(doubled[0], shock_lane),
        jnp.where(shock_block == 1, lane_gather(doubled[1], shock_lane), 0.0),
    )
    s_send[...] = jnp.where((sub8 & 3) == 3, shock8.astype(F32), s_own)

    pl.semaphore_wait(barrier, peers)
    start(forward)
    for ds in (-1, 1, 2):
        clear(ds)

    loads[9].wait()
    idx_pad[4:5, 0:16] = leave_idx[...]
    leave_row = idx_pad[4:5, :]
    sending = jnp.where(lane_row < leave_count[0], 1.0, 0.0)
    for h in range(2):
        ext[5 + h, 0:3, :] = half_velocity[:, h * LANES : (h + 1) * LANES]
    leaving = jnp.where(sub8 < 4, ext[0], pltpu.roll(ext[5], 4, 0))
    w_send[...] = lane_gather(leaving, rows_of(leave_row, 8)) * rows_of(sending, 8)
    start(extra[0:1])

    for i in (7, 8, 4, 3):
        loads[i].wait()
    blk[...] = jnp.full_like(blk, -1)
    lan[...] = jnp.zeros_like(lan)
    for h in range(2):
        hs = slice(h * LANES, (h + 1) * LANES)
        blk[pl.ds(h, 26, stride=2), :] = nb_block[:, hs]
        lan[pl.ds(h, 26, stride=2), :] = nb_lane[:, hs] & 127

    column128 = lax.broadcasted_iota(jnp.int32, (LANES, LANES), 0)

    def fill_onehot(k, carry):
        for h in range(2):
            row = lan[pl.ds(2 * k + h, 1), :]
            hot = jnp.where(column128 == rows_of(row, LANES), 1.0, 0.0).astype(BF16)
            at = pl.multiple_of((2 * k + h) * LANES, LANES)
            onehot[:, pl.ds(at, LANES)] = hot
        return carry

    lax.fori_loop(0, 26, fill_onehot, 0)
    for i in (10, 11, 12):
        loads[i].wait()
    even = (sub8 & 1) == 0
    block = blk[...]
    lane = lan[...]
    for c in range(3):
        own = jnp.where(even, rows_of(ext[0, c : c + 1, :], 8), rows_of(ext[1, c : c + 1, :], 8))
        parts = [lane_gather(rows_of(ext[b, c : c + 1, :], ROWS), lane) for b in range(2)]
        near_own[c] = (
            offs[c]
            - over(own, ROWS // 8)
            + jnp.where(block == 0, parts[0], jnp.where(block == 1, parts[1], 0.0))
        )

    leave_hot = jnp.where(column128 == rows_of(leave_row, LANES), 1.0, 0.0).astype(BF16)
    departed = mm_nt(rows_of(sending, 16).astype(BF16), leave_hot)[0:1, :]
    keep0 = jnp.where(lane_row < live[0], 1.0, 0.0) * (1.0 - departed)
    keep1 = jnp.where(lane_row + LANES < live[0], 1.0, 0.0)
    out_disp[:, 0:LANES] = displaced[:, 0:LANES] * rows_of(keep0, 3)
    out_disp[:, LANES:] = displaced[:, LANES:] * rows_of(keep1, 3)

    apad[...] = jnp.zeros_like(apad)
    apad[0:50, 0:50] = alpha[...]
    sym = 0.5 * (apad[...] + apad[...].T)
    sym_hi, sym_lo = split(sym[0:DROWS, 0:DROWS])
    apad[0:1, :] = jnp.zeros((1, LANES), F32)
    apad[0:1, 0:50] = beta[...]
    beta_col = rows_of(apad[0:1, :], LANES).T[0:DROWS, :]
    beta_col = jnp.concatenate([beta_col, beta_col], axis=1)
    for n in range(4):
        mom[n * MROWS + 32 : (n + 1) * MROWS, :] = jnp.zeros((8, 2 * LANES), F32)

    receive(forward)

    def between(lower, upper):
        return jnp.where(lane8 < 32, lower, jnp.where(lane8 < 64, upper, 0.0))

    t_ghost = between(f_recv[slot(0, -1)], f_recv[slot(0, 1)])
    from_low = f_recv[slot(-1, 0)]
    from_up = f_recv[slot(1, 0)]
    lists = jnp.where(sub8 < 4, rows_of(from_low[7:8, :], 8), rows_of(from_up[3:4, :], 8))
    lists = lists.astype(jnp.int32)
    across = jnp.where(
        sub8 < 4,
        between(f_recv[slot(-1, -1)], f_recv[slot(-1, 1)]),
        pltpu.roll(between(f_recv[slot(1, -1)], f_recv[slot(1, 1)]), 4, 0),
    )
    direct = jnp.where(sub8 < 4, pltpu.roll(from_low, 4, 0), pltpu.roll(from_up, 4, 0))
    both = jnp.where(lists >= 256, lane_gather(across, lists & 127), direct)
    turned = pltpu.roll(both, 64, 1)
    swapped = pltpu.roll(turned, 4, 0)
    ext[2] = jnp.where(lane8 < 64, t_ghost, turned)
    ext[3] = jnp.where(lane8 < 64, turned, swapped)
    ext[4] = swapped

    table = jnp.where(
        sub8 < 4, pltpu.roll(f_recv[slot(0, 1)], 6, 0), f_recv[slot(0, -1)]
    ).astype(jnp.int32)
    through = lane_gather(rows_of(t_row, 8), table & 127)
    first_of = jnp.where(sub8 < 4, 256, 288)
    through = jnp.where(table >= first_of, jnp.where(table < first_of + 32, through, -1), -1)
    direct = idx_pad[2:4, :]
    c_send[...] = through.astype(F32)
    c_send[0:2, :] = jnp.where(direct < 256, direct, -1).astype(F32)
    c_send[6:7, :] = jnp.where(lane_row < 64, t_row, -1).astype(F32)
    c_send[7:8, :] = jnp.where(sending > 0.0, leave_row, -2).astype(F32)

    block = blk[...]
    lane = lan[...]
    parts = []
    for c in range(3):
        found = jnp.zeros((ROWS, LANES), F32)
        for b in range(2, 5):
            value = lane_gather(rows_of(ext[b, c : c + 1, :], ROWS), lane)
            found = jnp.where(block == b, value, found)
        parts.append(near_own[c] + found)
    px, py, pz = parts
    square = px * px + py * py + pz * pz
    inverse = lax.rsqrt(square)
    distance = square * inverse
    ux, uy, uz = px * inverse, py * inverse, pz * inverse
    angle = (0.5 * math.pi) - (0.5 * math.pi / cutoff_radius) * distance
    sine, cosine = sin_of(angle), cos_of(angle)
    scale = jnp.where(block >= 0, moment_scale, 0.0)
    smooth = scale * sine * sine
    slope = scale * (-math.pi / cutoff_radius) * sine * cosine
    radial = []
    for n, center in enumerate(radial_centers):
        z = (distance - center) * (1.0 / radial_width)
        e = jnp.exp(-(z * z))
        r = smooth * e
        radial.append(r)
        geom[n] = r
        geom[4 + n] = slope * e - (2.0 / radial_width) * z * r
    geom[8] = ux
    geom[9] = uy
    geom[10] = uz
    geom[11] = inverse
    values = {}
    sums = {}
    for t in TRIPLES:
        p, q, w = t
        m = INDEX[t]
        if w > 1:
            low, left, right = reduced(t)
            for n in range(4):
                sums[(n, t)] = sums[(n, low)] - sums[(n, left)] - sums[(n, right)]
        else:
            if p > 0:
                prior, factor = values[(p - 1, q, w)], ux
            elif q > 0:
                prior, factor = values[(p, q - 1, w)], uy
            elif w > 0:
                prior, factor = values[(p, q, w - 1)], uz
            else:
                prior, factor = None, None
            value = factor if prior is None else prior * factor
            values[t] = value
            for n in range(4):
                sums[(n, t)] = row_sums(radial[n] if value is None else radial[n] * value)
        for n in range(4):
            at = n * MROWS + m
            mom[at : at + 1, 0:LANES] = sums[(n, t)][0:1, :]
            mom[at : at + 1, LANES:] = sums[(n, t)][1:2, :]

    moments = [mom[n * MROWS : (n + 1) * MROWS, :] for n in range(4)]
    products = jnp.concatenate([moments[n] * moments[o] for n, o in pair_list], axis=0)
    prod_hi, prod_lo = split(products)
    weights = wmat[...]
    descriptor = mm(weights, prod_hi) + mm(weights, prod_lo)
    desc_hi, desc_lo = split(descriptor)
    quadratic = mm(sym_hi, desc_hi) + mm(sym_lo, desc_hi) + mm(sym_hi, desc_lo)
    energy = jnp.sum(descriptor * (beta_col + 0.5 * quadratic), axis=0, keepdims=True)
    slope_hi, slope_lo = split(beta_col + quadratic)
    weights_t = wmat_t[...]
    dproducts = mm(weights_t, slope_hi) + mm(weights_t, slope_lo)
    for n in range(4):
        total = None
        for i, (a, b) in enumerate(pair_list):
            if n not in (a, b):
                continue
            part = dproducts[i * MROWS : (i + 1) * MROWS, :]
            if a == b:
                part = 2.0 * part * moments[n]
            else:
                part = part * moments[b if n == a else a]
            total = part if total is None else total + part
        dmom[n * MROWS : (n + 1) * MROWS, :] = total

    for n in range(4):
        slopes = {}
        for t in TRIPLES:
            at = n * MROWS + INDEX[t]
            slopes[t] = jnp.where(
                even,
                rows_of(dmom[at : at + 1, 0:LANES], 8),
                rows_of(dmom[at : at + 1, LANES:], 8),
            )
        for t in sorted(TRIPLES, key=lambda t: -t[2]):
            if t[2] > 1:
                low, left, right = reduced(t)
                slopes[low] = slopes[low] + slopes[t]
                slopes[left] = slopes[left] - slopes[t]
                slopes[right] = slopes[right] - slopes[t]
        for t in BASIS:
            tiles[n * len(BASIS) + PLACE[t]] = slopes[t]

    part8 = sub8 & 3
    half_block = sub8 >> 2
    spread = jnp.zeros((48, LANES), F32)
    own_total = [None] * 3
    for begin, end in CHUNKS:
        count = (end - begin) // 8
        at = slice(begin, end)
        radial = [geom[n, at, :] for n in range(4)]
        unit = [geom[8 + c, at, :] for c in range(3)]
        ux, uy, uz = unit
        found = []
        for w in range(2):
            size = 4 - w
            value_x = slope_x = slope_y = None
            heights = [None] * 4
            for p in range(size, -1, -1):
                value = slope = None
                rows = [None] * 4
                for q in range(size - p, -1, -1):
                    coefficient = None
                    for n in range(4):
                        b = over(tiles[n * len(BASIS) + PLACE[(p, q, w)]], count)
                        rows[n] = b if rows[n] is None else rows[n] * uy + b
                        term = b * radial[n]
                        coefficient = term if coefficient is None else coefficient + term
                    value, slope = horner(uy, value, slope, coefficient)
                for n in range(4):
                    heights[n] = rows[n] if heights[n] is None else heights[n] * ux + rows[n]
                value_x, slope_x = horner(ux, value_x, slope_x, value)
                if slope is not None:
                    slope_y = slope if slope_y is None else slope_y * ux + slope
            found.append((value_x, slope_x, slope_y, heights))
        inverse = geom[11, at, :]
        tangent = [
            (found[0][1] + uz * found[1][1]) * inverse,
            (found[0][2] + uz * found[1][2]) * inverse,
            found[1][0] * inverse,
        ]
        along = None
        for n in range(4):
            term = geom[4 + n, at, :] * (found[0][3][n] + uz * found[1][3][n])
            along = term if along is None else along + term
        along = along - (ux * tangent[0] + uy * tangent[1] + uz * tangent[2])
        for c in range(3):
            g = tangent[c] + unit[c] * along
            grads[c, at, :] = g
            for i in range(count):
                row = g[8 * i : 8 * i + 8, :]
                own_total[c] = row if own_total[c] is None else own_total[c] + row
        columns = []
        for r in range(begin, min(end, 52)):
            gx, gy, gz = (rows_of(grads[c, r : r + 1, :], 8) for c in range(3))
            value = jnp.where(part8 == 0, gx, jnp.where(part8 == 1, gy, gz))
            hi = value.astype(BF16).astype(F32)
            lo = value - hi
            place_of = rows_of(blk[r : r + 1, :], 8) - half_block
            masks = [place_of == 2 * i for i in range(3)]
            columns.append(
                jnp.concatenate(
                    [jnp.where(mask, x, 0.0) for x in (hi, lo) for mask in masks], axis=0
                ).astype(BF16)
            )
        last = min(end, 52)
        spread = spread + mm_nt(
            jnp.concatenate(columns, axis=1), onehot[:, begin * LANES : last * LANES]
        )
    for c in range(3):
        total = own_total[c] + pltpu.roll(own_total[c], 4, 0)
        total = total + pltpu.roll(total, 2, 0)
        for h in range(2):
            own_sum[h, c : c + 1, :] = total[h : h + 1, :]
    spread = spread[0:24, :] + spread[24:48, :]
    first = spread[0:8, :]
    second = spread[8:16, :]
    third = spread[16:24, :]
    second_turned = pltpu.roll(second, 64, 1)
    third_turned = pltpu.roll(third, 64, 1)
    shifted = jnp.where(
        sub8 < 4, pltpu.roll(second_turned, 4, 0), pltpu.roll(third_turned, 4, 0)
    )
    grad0 = first - own_sum[0]
    m_send[1] = second
    m_send[0] = jnp.where(lane8 < 64, second_turned, shifted)
    p_send[...] = jnp.where(sub8 < 3, grad0, 0.0)
    start(backward)
    start(extra[1:3])

    rows = [c_send[i : i + 1, :].astype(jnp.int32) for i in range(7)]
    for i, row in enumerate(rows):
        at = slice(i * LANES, (i + 1) * LANES)
        hot0[:, at] = jnp.where(column128 == rows_of(row, LANES), 1.0, 0.0).astype(BF16)
        if i < 2:
            hot1[:, at] = jnp.where(
                column128 + LANES == rows_of(row, LANES), 1.0, 0.0
            ).astype(BF16)
    out_energy[:, 0:LANES] = energy[:, 0:LANES] * keep0
    out_energy[:, LANES:] = energy[:, LANES:] * keep1
    grad1 = pltpu.roll(first, 4, 0) - own_sum[1]

    receive(extra[0:2])
    slots = rows_of(c_recv[7:8, :], LANES).T[0:16, :]
    for i in range(8):
        row = lane_row.astype(F32) if i == 7 else c_recv[i : i + 1, :]
        arr_hot[:, i * LANES : (i + 1) * LANES] = jnp.where(
            rows_of(row, 16) == slots, 1.0, 0.0
        ).astype(BF16)

    receive(backward)
    receive(extra[2:3])

    def lower_of(ds, dt):
        return b_recv[slot(ds, dt), 0]

    def upper_of(ds, dt):
        return pltpu.roll(b_recv[slot(ds, dt), 0], 4, 0)

    def pieces_of(tiles):
        back = jnp.concatenate([jnp.where(sub8 < 3, tile, 0.0) for tile in tiles], axis=1)
        hi = back.astype(BF16).astype(F32)
        return jnp.concatenate([hi, back - hi], axis=0).astype(BF16)

    back = pieces_of(
        (
            upper_of(-1, 0),
            lower_of(1, 0),
            upper_of(-1, 1),
            lower_of(1, 1),
            upper_of(-1, -1),
            lower_of(1, -1),
            between(b_recv[slot(0, 1), 1], b_recv[slot(0, -1), 1]),
        )
    )
    added0 = mm_nt(back, hot0[...])
    added1 = mm_nt(back[:, 0 : 2 * LANES], hot1[...])
    arriving = pieces_of(
        (
            pltpu.roll(m_send[0], 4, 0),
            lower_of(2, 0),
            upper_of(0, 1),
            lower_of(2, 1),
            upper_of(0, -1),
            lower_of(2, -1),
            between(b_recv[slot(1, 1), 1], b_recv[slot(1, -1), 1]),
            p_recv[...],
        )
    )
    added2 = mm_nt(arriving, arr_hot[...])
    force0 = -(grad0 + added0[0:8, :] + added0[8:16, :])[0:3, :]
    velocity0 = half_velocity[:, 0:LANES] + kick_factor * force0
    force1 = -(grad1 + added1[0:8, :] + added1[8:16, :])[0:3, :]
    velocity1 = half_velocity[:, LANES:] + kick_factor * force1
    force2 = -(added2[0:8, :] + added2[8:16, :])[0:3, :]
    state = w_recv[...]
    out_vel[:, 0:LANES] = velocity0 * rows_of(keep0, 3)
    out_force[:, 0:LANES] = force0 * rows_of(keep0, 3)
    out_vel[:, LANES:] = velocity1 * rows_of(keep1, 3)
    out_force[:, LANES:] = force1 * rows_of(keep1, 3)
    for q, value in enumerate(
        (state[0:3, 0:16], state[4:7, 0:16] + kick_factor * force2, force2)
    ):
        out_arr[q] = jnp.where(s_me < n_shock - 1, value, 0.0)
    drain(forward)
    drain(backward)
    drain(extra)


def kept(shape):
    return pltpu.VMEM(shape, F32)


def in_place(x):
    return pltpu.with_memory_space_constraint(x, pltpu.VMEM)


def finish(*refs):
    for i in range(5):
        refs[5 + i][...] = refs[i][...]


def whole_step(n_shock, n_trans, *args):
    (disp, vel, force, beta, alpha, live, trans_idx, shock_idx, block, lane, leave, count) = args
    table = contraction_table()
    inputs = (
        disp,
        vel,
        force,
        beta.reshape(1, 50),
        alpha,
        trans_idx,
        shock_idx,
        block,
        lane,
        leave.reshape(1, 16),
        jnp.asarray(lattice_rows()),
        jnp.asarray(table, BF16),
        jnp.asarray(table.T, BF16),
    )
    vmem = pl.BlockSpec(memory_space=pltpu.VMEM)
    tile = (8, LANES)
    shapes = ((3, 256), (3, 256), (3, 256), (1, 256), (3, 3, 16))
    outs = pl.pallas_call(
        functools.partial(kernel, n_shock, n_trans),
        out_shape=tuple(kept(shape) for shape in shapes),
        in_specs=[pl.BlockSpec(memory_space=pltpu.HBM)] * N_IN
        + [pl.BlockSpec(memory_space=pltpu.SMEM)] * 2,
        out_specs=(vmem,) * 5,
        scratch_shapes=[
            pltpu.VMEM(x.shape, x.dtype) for x in inputs
        ]
        + [
            pltpu.SemaphoreType.DMA((N_IN,)),
            pltpu.VMEM(tile, F32),
            pltpu.VMEM(tile, F32),
            pltpu.VMEM((NEAR, *tile), F32),
            pltpu.VMEM((2, *tile), F32),
            pltpu.VMEM((len(DIRS), 2, *tile), F32),
            pltpu.VMEM(tile, F32),
            pltpu.VMEM(tile, F32),
            pltpu.VMEM(tile, F32),
            pltpu.VMEM(tile, F32),
            pltpu.VMEM(tile, F32),
            pltpu.VMEM(tile, F32),
            pltpu.SemaphoreType.DMA((NEAR,)),
            pltpu.SemaphoreType.DMA((NEAR,)),
            pltpu.SemaphoreType.DMA((len(DIRS),)),
            pltpu.SemaphoreType.DMA((len(DIRS),)),
            pltpu.SemaphoreType.DMA((3,)),
            pltpu.SemaphoreType.DMA((3,)),
            pltpu.VMEM((7, *tile), F32),
            pltpu.VMEM((ROWS, LANES), jnp.int32),
            pltpu.VMEM((ROWS, LANES), jnp.int32),
            pltpu.VMEM(tile, jnp.int32),
            pltpu.VMEM((3, ROWS, LANES), F32),
            pltpu.VMEM((12, ROWS, LANES), F32),
            pltpu.VMEM((4 * len(BASIS), *tile), F32),
            pltpu.VMEM((4 * MROWS, 256), F32),
            pltpu.VMEM((4 * MROWS, 256), F32),
            pltpu.VMEM((LANES, 26 * 256), BF16),
            pltpu.VMEM((LANES, LANES), F32),
            pltpu.VMEM((LANES, 7 * LANES), BF16),
            pltpu.VMEM((LANES, 2 * LANES), BF16),
            pltpu.VMEM((16, 8 * LANES), BF16),
            pltpu.VMEM((3, ROWS, LANES), F32),
            pltpu.VMEM((2, *tile), F32),
        ],
        compiler_params=pltpu.CompilerParams(collective_id=0, has_side_effects=True),
        name="whole_step",
    )(*inputs, live, count)
    outs = [in_place(x) for x in outs]
    outs = pl.pallas_call(
        finish,
        out_shape=tuple(jax.ShapeDtypeStruct(shape, F32) for shape in shapes),
        in_specs=[vmem] * 5,
        out_specs=(vmem,) * 5,
        name="finish",
    )(*outs)
    return outs[0], outs[1], outs[2], outs[3].reshape(256), outs[4]


def solution(mesh):
    split_1 = P(None, ("shock", "trans"))
    split_0 = P(("shock", "trans"))
    in_specs = (
        split_1,
        split_1,
        split_1,
        P(),
        P(),
        split_0,
        split_1,
        split_1,
        split_1,
        split_1,
        split_0,
        split_0,
    )
    out_specs = (split_1, split_1, split_1, split_0, P(None, None, ("shock", "trans")))
    body = functools.partial(whole_step, mesh.shape["shock"], mesh.shape["trans"])
    return jax.shard_map(body, mesh=mesh, in_specs=in_specs, out_specs=out_specs, check_vma=False)
```

```python
import functools
import math

import jax
import jax.numpy as jnp
import numpy as np
from jax import lax
from jax.experimental import pallas as pl
from jax.experimental.pallas import tpu as pltpu
from jax.sharding import PartitionSpec as P

F32 = jnp.float32
BF16 = jnp.bfloat16
MESH = pl.DeviceIdType.MESH

kick_factor = 0.5
drift_step = 0.02
cutoff_radius = 4.2
radial_width = 0.35
radial_centers = (1.4, 1.9, 2.4, 2.9)
moment_scale = 0.25
spacing = radial_centers[1] - radial_centers[0]
pair_list = ((0, 0), (0, 1), (0, 2), (0, 3), (1, 1), (1, 2), (1, 3), (2, 2), (2, 3), (3, 3))
LANES = 128
ROWS = 56
CHUNKS = ((0, 8), (8, 16), (16, 32), (32, 48), (48, 56))
MROWS = 40
DROWS = 64


def exponents():
    triples = []
    for degree in range(5):
        for p in range(degree, -1, -1):
            for q in range(degree - p, -1, -1):
                triples.append((p, q, degree - p - q))
    return triples


TRIPLES = exponents()
INDEX = {t: i for i, t in enumerate(TRIPLES)}
BASIS = [t for t in TRIPLES if t[2] < 2]
PLACE = {t: i for i, t in enumerate(BASIS)}


def reduced(t):
    p, q, w = t
    return (p, q, w - 2), (p + 2, q, w - 2), (p, q + 2, w - 2)


def lattice_rows():
    entries = []
    for number in range(8):
        entries.append(
            [1.0 - 2.0 * (number >> 2 & 1), 1.0 - 2.0 * (number >> 1 & 1), 1.0 - 2.0 * (number & 1)]
        )
    for axis_pick in range(3):
        for signed in (2.0, -2.0):
            vector = [0.0, 0.0, 0.0]
            vector[axis_pick] = signed
            entries.append(vector)
    for zero_pick in (2, 1, 0):
        others = [axis_pick for axis_pick in range(3) if axis_pick != zero_pick]
        for leading in (2.0, -2.0):
            for trailing in (2.0, -2.0):
                vector = [0.0, 0.0, 0.0]
                vector[others[0]] = leading
                vector[others[1]] = trailing
                entries.append(vector)
    while len(entries) < ROWS // 2:
        entries.append([1.0, 1.0, 1.0])
    table = np.repeat(np.array(entries, dtype=np.float32), 2, axis=0).T
    return np.broadcast_to(table[:, :, None], (3, ROWS, LANES)).copy()


def multiplicity(t):
    p, q, w = t
    return math.factorial(p + q + w) / (math.factorial(p) * math.factorial(q) * math.factorial(w))


def weight_rows():
    rows = np.zeros((MROWS, 2 * LANES), dtype=np.float32)
    for m, t in enumerate(TRIPLES):
        rows[m] = multiplicity(t)
    return rows


def selection_table():
    table = np.zeros((DROWS, len(pair_list) * MROWS), dtype=np.float32)
    for i in range(len(pair_list)):
        for m, t in enumerate(TRIPLES):
            table[5 * i + sum(t), MROWS * i + m] = 1.0
    return table


def split(x):
    hi = x.astype(BF16)
    lo = (x - hi.astype(F32)).astype(BF16)
    return hi, lo


def mm(a, b):
    return lax.dot_general(a, b, (((1,), (0,)), ((), ())), preferred_element_type=F32)


def mm_nt(a, b):
    return lax.dot_general(a, b, (((1,), (1,)), ((), ())), preferred_element_type=F32)


def lane_gather(x, index):
    numbers = lax.GatherDimensionNumbers(
        offset_dims=(),
        collapsed_slice_dims=(1,),
        start_index_map=(1,),
        operand_batching_dims=(0,),
        start_indices_batching_dims=(0,),
    )
    return lax.gather(
        x,
        index[:, :, None],
        numbers,
        slice_sizes=(1, 1),
        mode=lax.GatherScatterMode.PROMISE_IN_BOUNDS,
    )


def rows_of(row, count):
    return jnp.broadcast_to(row, (count, row.shape[1]))


def over(tile, count):
    return jnp.concatenate([tile] * count, axis=0) if count > 1 else tile


def row_sums(x):
    total = x[0:8, :]
    for i in range(8, x.shape[0], 8):
        total = total + x[i : i + 8, :]
    total = total + pltpu.roll(total, 4, 0)
    return total + pltpu.roll(total, 2, 0)


def horner(x, value, slope, term):
    if value is None:
        return term, None
    slope = value if slope is None else slope * x + value
    return value * x + term, slope


def sin_of(u):
    s = u * u
    r = -1.0 / 39916800.0
    for c in (1.0 / 362880.0, -1.0 / 5040.0, 1.0 / 120.0, -1.0 / 6.0, 1.0):
        r = r * s + c
    return r * u


def cos_of(u):
    s = u * u
    r = 1.0 / 479001600.0
    for c in (-1.0 / 3628800.0, 1.0 / 40320.0, -1.0 / 720.0, 1.0 / 24.0, -0.5, 1.0):
        r = r * s + c
    return r


DIRS = (
    (1, 1),
    (1, -1),
    (-1, 1),
    (-1, -1),
    (0, 1),
    (0, -1),
    (1, 0),
    (-1, 0),
    (-2, 1),
    (-2, -1),
    (-2, 0),
)
NEAR = 8
N_IN = 13


def kernel(n_shock, n_trans, *refs):
    hbm = refs[:N_IN]
    live, leave_count = refs[N_IN : N_IN + 2]
    out_disp, out_vel, out_force, out_energy, out_arr = refs[N_IN + 2 : N_IN + 7]
    (
        disp,
        vel,
        force,
        beta,
        alpha,
        trans_idx,
        shock_idx,
        nb_block,
        nb_lane,
        leave_idx,
        offs,
        weight,
        chosen,
        in_sems,
        t_send,
        s_send,
        f_recv,
        m_send,
        b_recv,
        w_send,
        w_recv,
        c_send,
        c_recv,
        p_send,
        p_recv,
        f_send_sems,
        f_recv_sems,
        b_send_sems,
        b_recv_sems,
        x_send_sems,
        x_recv_sems,
        ext,
        blk,
        lan,
        idx_pad,
        near_own,
        geom,
        tiles,
        mom,
        dmom,
        mixing,
        by_descriptor,
        onehot,
        apad,
        hot0,
        hot1,
        arr_hot,
        grads,
        own_sum,
    ) = refs[N_IN + 7 :]
    local = (
        disp,
        vel,
        force,
        beta,
        alpha,
        trans_idx,
        shock_idx,
        nb_block,
        nb_lane,
        leave_idx,
        offs,
        weight,
        chosen,
    )
    loads = [
        pltpu.make_async_copy(src, dst, in_sems.at[i])
        for i, (src, dst) in enumerate(zip(hbm, local, strict=True))
    ]
    s_me = lax.axis_index("shock")
    t_me = lax.axis_index("trans")

    t_near = {
        -1: jnp.where(t_me > 0, t_me - 1, n_trans - 1),
        0: t_me,
        1: jnp.where(t_me < n_trans - 1, t_me + 1, 0),
    }

    def place(ds, dt):
        return s_me + ds, t_near[dt]

    inside = {
        -2: s_me > 1,
        -1: s_me > 0,
        0: None,
        1: s_me < n_shock - 1,
        2: s_me < n_shock - 2,
    }

    def where_inside(ds, action):
        if inside[ds] is None:
            action()
        else:
            pl.when(inside[ds])(action)

    def clear(ds):
        def action():
            for dt in (-1, 0, 1):
                k = DIRS.index((-ds, -dt))
                b_recv[k] = jnp.zeros((2, 8, LANES), F32)
                if k < NEAR:
                    f_recv[k] = jnp.zeros((8, LANES), F32)
            if ds == 1:
                w_recv[...] = jnp.zeros((8, LANES), F32)
                c_recv[...] = jnp.zeros((8, LANES), F32)
                p_recv[...] = jnp.zeros((8, LANES), F32)

        pl.when(jnp.logical_not(inside[ds]))(action)

    barrier = pltpu.get_barrier_semaphore()

    def greet(ds):
        def action():
            for dt in (-1, 0, 1):
                if (ds, dt) != (0, 0):
                    pl.semaphore_signal(
                        barrier, inc=1, device_id=place(ds, dt), device_id_type=MESH
                    )

        return action

    for ds in (0, 1, -1, 2, -2):
        where_inside(ds, greet(ds))
    for i in (0, 1, 2, 5, 6, 7, 8, 9, 4, 3, 10, 11, 12):
        loads[i].start()
    peers = 2
    for ds in (1, -1, 2, -2):
        peers = peers + jnp.where(inside[ds], 3, 0)

    def remote(src, dst, send_sem, recv_sem, where):
        return pltpu.make_async_remote_copy(
            src_ref=src,
            dst_ref=dst,
            send_sem=send_sem,
            recv_sem=recv_sem,
            device_id=place(*where),
            device_id_type=MESH,
        )

    forward = [
        (
            ds,
            remote(
                s_send if dt == 0 else t_send,
                f_recv.at[k],
                f_send_sems.at[k],
                f_recv_sems.at[k],
                (ds, dt),
            ),
        )
        for k, (ds, dt) in enumerate(DIRS[:NEAR])
    ]
    backward = [
        (
            ds,
            remote(
                m_send if whole else m_send.at[0],
                b_recv.at[k] if whole else b_recv.at[k, 0],
                b_send_sems.at[k],
                b_recv_sems.at[k],
                (ds, dt),
            ),
        )
        for k, (ds, dt) in enumerate(DIRS)
        for whole in (dt != 0 and ds in (0, -1),)
    ]
    extra = [
        (-1, remote(src, dst, x_send_sems.at[i], x_recv_sems.at[i], (-1, 0)))
        for i, (src, dst) in enumerate(((w_send, w_recv), (c_send, c_recv), (p_send, p_recv)))
    ]

    def start(copies):
        for ds in (1, -1, 0, -2):
            chosen = [copy for at, copy in copies if at == ds]

            def action(chosen=chosen):
                for copy in chosen:
                    copy.start()

            if chosen:
                where_inside(ds, action)

    def receive(copies):
        for ds in (0, 1, -1, -2):
            chosen = [copy for at, copy in copies if at == ds]

            def action(chosen=chosen):
                for copy in chosen:
                    copy.wait_recv()

            if chosen:
                where_inside(-ds, action)

    def drain(copies):
        for ds in (0, 1, -1, -2):
            chosen = [copy for at, copy in copies if at == ds]

            def action(chosen=chosen):
                for copy in chosen:
                    copy.wait_send()

            if chosen:
                where_inside(ds, action)

    def slot(ds, dt):
        return DIRS.index((-ds, -dt))

    lane_row = lax.broadcasted_iota(jnp.int32, (1, LANES), 1)
    lane8 = lax.broadcasted_iota(jnp.int32, (8, LANES), 1)
    sub8 = lax.broadcasted_iota(jnp.int32, (8, LANES), 0)

    idx_pad[...] = jnp.zeros_like(idx_pad)
    ext[...] = jnp.zeros_like(ext)
    for i in (0, 1, 2, 5, 6):
        loads[i].wait()
    half_velocity = vel[...] + kick_factor * force[...]
    displaced = disp[...] + drift_step * half_velocity
    for h in range(2):
        ext[h, 0:3, :] = displaced[:, h * LANES : (h + 1) * LANES]
    idx_pad[0:1, 0:32] = trans_idx[1:2, :]
    idx_pad[1:2, 0:32] = trans_idx[0:1, :]
    idx_pad[2:4, :] = pltpu.roll(shock_idx[...], 64, 1)
    t_row = jnp.where(lane_row < 32, idx_pad[0:1, :], pltpu.roll(idx_pad[1:2, :], 32, 1))
    shock8 = jnp.where(sub8 < 4, rows_of(idx_pad[2:3, :], 8), rows_of(idx_pad[3:4, :], 8))
    shock_block = shock8 >> 7
    shock_lane = shock8 & 127
    doubled = [jnp.where(sub8 < 4, ext[b], pltpu.roll(ext[b], 4, 0)) for b in range(2)]
    t_send[...] = lane_gather(ext[0], rows_of(t_row, 8))
    t_send[4:6, :] = idx_pad[2:4, :].astype(F32)
    s_own = jnp.where(
        shock_block == 0,
        lane_gather(doubled[0], shock_lane),
        jnp.where(shock_block == 1, lane_gather(doubled[1], shock_lane), 0.0),
    )
    s_send[...] = jnp.where((sub8 & 3) == 3, shock8.astype(F32), s_own)

    pl.semaphore_wait(barrier, peers)
    start(forward)
    for ds in (-1, 1, 2):
        clear(ds)

    loads[9].wait()
    idx_pad[4:5, 0:16] = leave_idx[...]
    leave_row = idx_pad[4:5, :]
    sending = jnp.where(lane_row < leave_count[0], 1.0, 0.0)
    for h in range(2):
        ext[5 + h, 0:3, :] = half_velocity[:, h * LANES : (h + 1) * LANES]
    leaving = jnp.where(sub8 < 4, ext[0], pltpu.roll(ext[5], 4, 0))
    w_send[...] = lane_gather(leaving, rows_of(leave_row, 8)) * rows_of(sending, 8)
    start(extra[0:1])

    for i in (7, 8, 4, 3):
        loads[i].wait()
    blk[...] = jnp.full_like(blk, -1)
    lan[...] = jnp.zeros_like(lan)
    for h in range(2):
        hs = slice(h * LANES, (h + 1) * LANES)
        blk[pl.ds(h, 26, stride=2), :] = nb_block[:, hs]
        lan[pl.ds(h, 26, stride=2), :] = nb_lane[:, hs] & 127

    column128 = lax.broadcasted_iota(jnp.int32, (LANES, LANES), 0)

    def fill_onehot(k, carry):
        for h in range(2):
            row = lan[pl.ds(2 * k + h, 1), :]
            hot = jnp.where(column128 == rows_of(row, LANES), 1.0, 0.0).astype(BF16)
            at = pl.multiple_of((2 * k + h) * LANES, LANES)
            onehot[:, pl.ds(at, LANES)] = hot
        return carry

    lax.fori_loop(0, 26, fill_onehot, 0)
    for i in (10, 11, 12):
        loads[i].wait()
    even = (sub8 & 1) == 0
    block = blk[...]
    lane = lan[...]
    for c in range(3):
        own = jnp.where(even, rows_of(ext[0, c : c + 1, :], 8), rows_of(ext[1, c : c + 1, :], 8))
        parts = [lane_gather(rows_of(ext[b, c : c + 1, :], ROWS), lane) for b in range(2)]
        near_own[c] = (
            offs[c]
            - over(own, ROWS // 8)
            + jnp.where(block == 0, parts[0], jnp.where(block == 1, parts[1], 0.0))
        )

    leave_hot = jnp.where(column128 == rows_of(leave_row, LANES), 1.0, 0.0).astype(BF16)
    departed = mm_nt(rows_of(sending, 16).astype(BF16), leave_hot)[0:1, :]
    keep0 = jnp.where(lane_row < live[0], 1.0, 0.0) * (1.0 - departed)
    keep1 = jnp.where(lane_row + LANES < live[0], 1.0, 0.0)
    out_disp[:, 0:LANES] = displaced[:, 0:LANES] * rows_of(keep0, 3)
    out_disp[:, LANES:] = displaced[:, LANES:] * rows_of(keep1, 3)

    apad[...] = jnp.zeros_like(apad)
    apad[0:50, 0:50] = alpha[...]
    sym = 0.5 * (apad[...] + apad[...].T)
    sym_hi, sym_lo = split(sym[0:DROWS, 0:DROWS])
    mixed_hi, mixed_lo = split(mm(sym_hi, chosen[...]) + mm(sym_lo, chosen[...]))
    mixing[0:DROWS, :] = mixed_lo
    mixing[DROWS : 2 * DROWS, :] = mixed_hi
    mixing[2 * DROWS : 3 * DROWS, :] = chosen[...]
    apad[0:1, :] = jnp.zeros((1, LANES), F32)
    apad[0:1, 0:50] = beta[...]
    beta_col = rows_of(apad[0:1, :], LANES).T[0:DROWS, :]
    beta_col = jnp.concatenate([beta_col, beta_col], axis=1)
    for n in range(4):
        mom[n * MROWS + 32 : (n + 1) * MROWS, :] = jnp.zeros((8, 2 * LANES), F32)

    receive(forward)

    def between(lower, upper):
        return jnp.where(lane8 < 32, lower, jnp.where(lane8 < 64, upper, 0.0))

    t_ghost = between(f_recv[slot(0, -1)], f_recv[slot(0, 1)])
    from_low = f_recv[slot(-1, 0)]
    from_up = f_recv[slot(1, 0)]
    lists = jnp.where(sub8 < 4, rows_of(from_low[7:8, :], 8), rows_of(from_up[3:4, :], 8))
    lists = lists.astype(jnp.int32)
    across = jnp.where(
        sub8 < 4,
        between(f_recv[slot(-1, -1)], f_recv[slot(-1, 1)]),
        pltpu.roll(between(f_recv[slot(1, -1)], f_recv[slot(1, 1)]), 4, 0),
    )
    direct = jnp.where(sub8 < 4, pltpu.roll(from_low, 4, 0), pltpu.roll(from_up, 4, 0))
    both = jnp.where(lists >= 256, lane_gather(across, lists & 127), direct)
    swapped = pltpu.roll(both, 4, 0)
    ext[2] = jnp.where(lane8 < 64, t_ghost, both)
    ext[3] = jnp.where(lane8 < 64, both, swapped)
    ext[4] = swapped

    table = jnp.where(
        sub8 < 4, pltpu.roll(f_recv[slot(0, 1)], 6, 0), f_recv[slot(0, -1)]
    ).astype(jnp.int32)
    through = lane_gather(rows_of(t_row, 8), table & 127)
    first_of = jnp.where(sub8 < 4, 256, 288)
    through = jnp.where(table >= first_of, jnp.where(table < first_of + 32, through, -1), -1)
    direct = idx_pad[2:4, :]
    c_send[...] = through.astype(F32)
    c_send[0:2, :] = jnp.where(direct < 256, direct, -1).astype(F32)
    c_send[6:7, :] = jnp.where(lane_row < 64, t_row, -1).astype(F32)
    c_send[7:8, :] = jnp.where(sending > 0.0, leave_row, -2).astype(F32)

    block = blk[...]
    lane = lan[...]
    parts = []
    for c in range(3):
        found = jnp.zeros((ROWS, LANES), F32)
        for b in range(2, 5):
            value = lane_gather(rows_of(ext[b, c : c + 1, :], ROWS), lane)
            found = jnp.where(block == b, value, found)
        parts.append(near_own[c] + found)
    px, py, pz = parts
    square = px * px + py * py + pz * pz
    inverse = lax.rsqrt(square)
    distance = square * inverse
    ux, uy, uz = px * inverse, py * inverse, pz * inverse
    angle = (0.5 * math.pi) - (0.5 * math.pi / cutoff_radius) * distance
    sine, cosine = sin_of(angle), cos_of(angle)
    sine_live = jnp.where(block >= 0, moment_scale * sine, 0.0)
    first_z = (distance - radial_centers[0]) * (1.0 / radial_width)
    radial = []
    for n, center in enumerate(radial_centers):
        z = (distance - center) * (1.0 / radial_width)
        weighted = sine_live * jnp.exp(-(z * z))
        radial.append(sine * weighted)
        geom[n] = weighted
    geom[4] = (-math.pi / cutoff_radius) * cosine - (2.0 / radial_width) * first_z * sine
    geom[5] = (2.0 * spacing / radial_width**2) * sine
    geom[6] = sine * inverse
    geom[8] = ux
    geom[9] = uy
    geom[10] = uz
    values = {}
    sums = {}
    for t in TRIPLES:
        p, q, w = t
        m = INDEX[t]
        if w > 1:
            low, left, right = reduced(t)
            for n in range(4):
                sums[(n, t)] = sums[(n, low)] - sums[(n, left)] - sums[(n, right)]
        else:
            if p > 0:
                prior, factor = values[(p - 1, q, w)], ux
            elif q > 0:
                prior, factor = values[(p, q - 1, w)], uy
            elif w > 0:
                prior, factor = values[(p, q, w - 1)], uz
            else:
                prior, factor = None, None
            value = factor if prior is None else prior * factor
            values[t] = value
            for n in range(4):
                sums[(n, t)] = row_sums(radial[n] if value is None else radial[n] * value)
        for n in range(4):
            at = n * MROWS + m
            mom[at : at + 1, 0:LANES] = sums[(n, t)][0:1, :]
            mom[at : at + 1, LANES:] = sums[(n, t)][1:2, :]

    moments = [mom[n * MROWS : (n + 1) * MROWS, :] for n in range(4)]
    heavy = [weight[...] * value for value in moments]
    products = jnp.concatenate([moments[n] * heavy[o] for n, o in pair_list], axis=0)
    prod_hi, prod_lo = split(products)
    high = mm(mixing[...], prod_hi)
    low = mm(mixing[DROWS : 3 * DROWS, :], prod_lo)
    by_descriptor[...] = beta_col + (
        high[0:DROWS, :] + high[DROWS : 2 * DROWS, :] + low[0:DROWS, :]
    )
    descriptor = high[2 * DROWS : 3 * DROWS, :] + low[DROWS : 2 * DROWS, :]
    energy = 0.5 * jnp.sum(descriptor * (beta_col + by_descriptor[...]), axis=0, keepdims=True)
    sub_wide = lax.broadcasted_iota(jnp.int32, (8, 2 * LANES), 0)
    totals = [None] * 4
    for i, (a, b) in enumerate(pair_list):
        r = [rows_of(by_descriptor[5 * i + l : 5 * i + l + 1, :], 8) for l in range(5)]
        spread_rows = jnp.concatenate(
            [
                jnp.where(sub_wide < 1, r[0], jnp.where(sub_wide < 4, r[1], r[2])),
                jnp.where(sub_wide < 2, r[2], r[3]),
                jnp.where(sub_wide < 4, r[3], r[4]),
                r[4],
                r[4],
            ],
            axis=0,
        )
        if a == b:
            terms = ((a, 2.0 * spread_rows * heavy[a]),)
        else:
            terms = ((a, spread_rows * heavy[b]), (b, spread_rows * heavy[a]))
        for n, term in terms:
            totals[n] = term if totals[n] is None else totals[n] + term
    for n in range(4):
        dmom[n * MROWS : (n + 1) * MROWS, :] = totals[n]

    for n in range(4):
        slopes = {}
        for t in TRIPLES:
            at = n * MROWS + INDEX[t]
            slopes[t] = jnp.where(
                even,
                rows_of(dmom[at : at + 1, 0:LANES], 8),
                rows_of(dmom[at : at + 1, LANES:], 8),
            )
        for t in sorted(TRIPLES, key=lambda t: -t[2]):
            if t[2] > 1:
                low, left, right = reduced(t)
                slopes[low] = slopes[low] + slopes[t]
                slopes[left] = slopes[left] - slopes[t]
                slopes[right] = slopes[right] - slopes[t]
        for t in BASIS:
            tiles[n * len(BASIS) + PLACE[t]] = slopes[t]

    part8 = sub8 & 3
    half_block = sub8 >> 2
    own_total = [None] * 3

    def pair_gradients(begin, end):
        count = (end - begin) // 8
        at = slice(begin, end)
        weighted = [geom[n, at, :] for n in range(4)]
        unit = [geom[8 + c, at, :] for c in range(3)]
        ux, uy, uz = unit
        found = []
        for w in range(2):
            size = 4 - w
            value_x = slope_x = slope_y = graded_x = None
            for p in range(size, -1, -1):
                value = slope = graded = None
                for q in range(size - p, -1, -1):
                    total = graded_total = None
                    for n in range(3, -1, -1):
                        b = over(tiles[n * len(BASIS) + PLACE[(p, q, w)]], count)
                        term = b * weighted[n]
                        total = term if total is None else total + term
                        if n > 0:
                            graded_total = total if graded_total is None else graded_total + total
                    value, slope = horner(uy, value, slope, total)
                    graded = graded_total if graded is None else graded * uy + graded_total
                value_x, slope_x = horner(ux, value_x, slope_x, value)
                graded_x = graded if graded_x is None else graded_x * ux + graded
                if slope is not None:
                    slope_y = slope if slope_y is None else slope_y * ux + slope
            found.append((value_x, slope_x, slope_y, graded_x))
        scaled = geom[6, at, :]
        tangent = [
            (found[0][1] + uz * found[1][1]) * scaled,
            (found[0][2] + uz * found[1][2]) * scaled,
            found[1][0] * scaled,
        ]
        along = geom[4, at, :] * (found[0][0] + uz * found[1][0])
        along = along + geom[5, at, :] * (found[0][3] + uz * found[1][3])
        along = along - (ux * tangent[0] + uy * tangent[1] + uz * tangent[2])
        for c in range(3):
            g = tangent[c] + unit[c] * along
            grads[c, at, :] = g
            for i in range(count):
                row = g[8 * i : 8 * i + 8, :]
                own_total[c] = row if own_total[c] is None else own_total[c] + row

    def spread_sums(begin, end):
        columns = []
        for r in range(begin, min(end, 52)):
            gx, gy, gz = (rows_of(grads[c, r : r + 1, :], 8) for c in range(3))
            value = jnp.where(part8 == 0, gx, jnp.where(part8 == 1, gy, gz))
            hi = value.astype(BF16).astype(F32)
            lo = value - hi
            place_of = rows_of(blk[r : r + 1, :], 8) - half_block
            masks = [place_of == 2 * i for i in range(3)]
            columns.append(
                jnp.concatenate(
                    [jnp.where(mask, x, 0.0) for x in (hi, lo) for mask in masks], axis=0
                ).astype(BF16)
            )
        last = min(end, 52)
        return mm_nt(jnp.concatenate(columns, axis=1), onehot[:, begin * LANES : last * LANES])

    spread = jnp.zeros((48, LANES), F32)
    pair_gradients(*CHUNKS[0])
    for at in range(len(CHUNKS)):
        if at + 1 < len(CHUNKS):
            pair_gradients(*CHUNKS[at + 1])
        spread = spread + spread_sums(*CHUNKS[at])
    for c in range(3):
        total = own_total[c] + pltpu.roll(own_total[c], 4, 0)
        total = total + pltpu.roll(total, 2, 0)
        for h in range(2):
            own_sum[h, c : c + 1, :] = total[h : h + 1, :]
    spread = spread[0:24, :] + spread[24:48, :]
    first = spread[0:8, :]
    second = spread[8:16, :]
    third = spread[16:24, :]
    shifted = jnp.where(sub8 < 4, pltpu.roll(second, 4, 0), pltpu.roll(third, 4, 0))
    grad0 = first - own_sum[0]
    m_send[1] = second
    m_send[0] = jnp.where(lane8 < 64, shifted, second)
    p_send[...] = jnp.where(sub8 < 3, grad0, 0.0)
    start(backward)
    start(extra[1:3])

    rows = [c_send[i : i + 1, :].astype(jnp.int32) for i in range(7)]
    for i, row in enumerate(rows):
        at = slice(i * LANES, (i + 1) * LANES)
        hot0[:, at] = jnp.where(column128 == rows_of(row, LANES), 1.0, 0.0).astype(BF16)
        if i < 2:
            hot1[:, at] = jnp.where(
                column128 + LANES == rows_of(row, LANES), 1.0, 0.0
            ).astype(BF16)
    out_energy[:, 0:LANES] = energy[:, 0:LANES] * keep0
    out_energy[:, LANES:] = energy[:, LANES:] * keep1
    grad1 = pltpu.roll(first, 4, 0) - own_sum[1]

    receive(extra[0:2])
    slots = rows_of(c_recv[7:8, :], LANES).T[0:16, :]
    for i in range(8):
        row = lane_row.astype(F32) if i == 7 else c_recv[i : i + 1, :]
        arr_hot[:, i * LANES : (i + 1) * LANES] = jnp.where(
            rows_of(row, 16) == slots, 1.0, 0.0
        ).astype(BF16)

    receive(backward)
    receive(extra[2:3])

    def lower_of(ds, dt):
        return b_recv[slot(ds, dt), 0]

    def upper_of(ds, dt):
        return pltpu.roll(b_recv[slot(ds, dt), 0], 4, 0)

    def pieces_of(tiles):
        back = jnp.concatenate([jnp.where(sub8 < 3, tile, 0.0) for tile in tiles], axis=1)
        hi = back.astype(BF16).astype(F32)
        return jnp.concatenate([hi, back - hi], axis=0).astype(BF16)

    back = pieces_of(
        (
            upper_of(-1, 0),
            lower_of(1, 0),
            upper_of(-1, 1),
            lower_of(1, 1),
            upper_of(-1, -1),
            lower_of(1, -1),
            between(b_recv[slot(0, 1), 1], b_recv[slot(0, -1), 1]),
        )
    )
    added0 = mm_nt(back, hot0[...])
    added1 = mm_nt(back[:, 0 : 2 * LANES], hot1[...])
    arriving = pieces_of(
        (
            pltpu.roll(m_send[0], 4, 0),
            lower_of(2, 0),
            upper_of(0, 1),
            lower_of(2, 1),
            upper_of(0, -1),
            lower_of(2, -1),
            between(b_recv[slot(1, 1), 1], b_recv[slot(1, -1), 1]),
            p_recv[...],
        )
    )
    added2 = mm_nt(arriving, arr_hot[...])
    force0 = -(grad0 + added0[0:8, :] + added0[8:16, :])[0:3, :]
    velocity0 = half_velocity[:, 0:LANES] + kick_factor * force0
    force1 = -(grad1 + added1[0:8, :] + added1[8:16, :])[0:3, :]
    velocity1 = half_velocity[:, LANES:] + kick_factor * force1
    force2 = -(added2[0:8, :] + added2[8:16, :])[0:3, :]
    state = w_recv[...]
    out_vel[:, 0:LANES] = velocity0 * rows_of(keep0, 3)
    out_force[:, 0:LANES] = force0 * rows_of(keep0, 3)
    out_vel[:, LANES:] = velocity1 * rows_of(keep1, 3)
    out_force[:, LANES:] = force1 * rows_of(keep1, 3)
    for q, value in enumerate(
        (state[0:3, 0:16], state[4:7, 0:16] + kick_factor * force2, force2)
    ):
        out_arr[q] = jnp.where(s_me < n_shock - 1, value, 0.0)
    drain(forward)
    drain(backward)
    drain(extra)


def kept(shape):
    return pltpu.VMEM(shape, F32)


def in_place(x):
    return pltpu.with_memory_space_constraint(x, pltpu.VMEM)


def finish(*refs):
    for i in range(5):
        refs[5 + i][...] = refs[i][...]


def whole_step(n_shock, n_trans, *args):
    (disp, vel, force, beta, alpha, live, trans_idx, shock_idx, block, lane, leave, count) = args
    inputs = (
        disp,
        vel,
        force,
        beta.reshape(1, 50),
        alpha,
        trans_idx,
        shock_idx,
        block,
        lane,
        leave.reshape(1, 16),
        jnp.asarray(lattice_rows()),
        jnp.asarray(weight_rows()),
        jnp.asarray(selection_table(), BF16),
    )
    vmem = pl.BlockSpec(memory_space=pltpu.VMEM)
    tile = (8, LANES)
    shapes = ((3, 256), (3, 256), (3, 256), (1, 256), (3, 3, 16))
    outs = pl.pallas_call(
        functools.partial(kernel, n_shock, n_trans),
        out_shape=tuple(kept(shape) for shape in shapes),
        in_specs=[pl.BlockSpec(memory_space=pltpu.HBM)] * N_IN
        + [pl.BlockSpec(memory_space=pltpu.SMEM)] * 2,
        out_specs=(vmem,) * 5,
        scratch_shapes=[
            pltpu.VMEM(x.shape, x.dtype) for x in inputs
        ]
        + [
            pltpu.SemaphoreType.DMA((N_IN,)),
            pltpu.VMEM(tile, F32),
            pltpu.VMEM(tile, F32),
            pltpu.VMEM((NEAR, *tile), F32),
            pltpu.VMEM((2, *tile), F32),
            pltpu.VMEM((len(DIRS), 2, *tile), F32),
            pltpu.VMEM(tile, F32),
            pltpu.VMEM(tile, F32),
            pltpu.VMEM(tile, F32),
            pltpu.VMEM(tile, F32),
            pltpu.VMEM(tile, F32),
            pltpu.VMEM(tile, F32),
            pltpu.SemaphoreType.DMA((NEAR,)),
            pltpu.SemaphoreType.DMA((NEAR,)),
            pltpu.SemaphoreType.DMA((len(DIRS),)),
            pltpu.SemaphoreType.DMA((len(DIRS),)),
            pltpu.SemaphoreType.DMA((3,)),
            pltpu.SemaphoreType.DMA((3,)),
            pltpu.VMEM((7, *tile), F32),
            pltpu.VMEM((ROWS, LANES), jnp.int32),
            pltpu.VMEM((ROWS, LANES), jnp.int32),
            pltpu.VMEM(tile, jnp.int32),
            pltpu.VMEM((3, ROWS, LANES), F32),
            pltpu.VMEM((11, ROWS, LANES), F32),
            pltpu.VMEM((4 * len(BASIS), *tile), F32),
            pltpu.VMEM((4 * MROWS, 256), F32),
            pltpu.VMEM((4 * MROWS, 256), F32),
            pltpu.VMEM((3 * DROWS, 10 * MROWS), BF16),
            pltpu.VMEM((DROWS, 256), F32),
            pltpu.VMEM((LANES, 26 * 256), BF16),
            pltpu.VMEM((LANES, LANES), F32),
            pltpu.VMEM((LANES, 7 * LANES), BF16),
            pltpu.VMEM((LANES, 2 * LANES), BF16),
            pltpu.VMEM((16, 8 * LANES), BF16),
            pltpu.VMEM((3, ROWS, LANES), F32),
            pltpu.VMEM((2, *tile), F32),
        ],
        compiler_params=pltpu.CompilerParams(collective_id=0, has_side_effects=True),
        name="whole_step",
    )(*inputs, live, count)
    outs = [in_place(x) for x in outs]
    outs = pl.pallas_call(
        finish,
        out_shape=tuple(jax.ShapeDtypeStruct(shape, F32) for shape in shapes),
        in_specs=[vmem] * 5,
        out_specs=(vmem,) * 5,
        name="finish",
    )(*outs)
    return outs[0], outs[1], outs[2], outs[3].reshape(256), outs[4]


def solution(mesh):
    split_1 = P(None, ("shock", "trans"))
    split_0 = P(("shock", "trans"))
    in_specs = (
        split_1,
        split_1,
        split_1,
        P(),
        P(),
        split_0,
        split_1,
        split_1,
        split_1,
        split_1,
        split_0,
        split_0,
    )
    out_specs = (split_1, split_1, split_1, split_0, P(None, None, ("shock", "trans")))
    body = functools.partial(whole_step, mesh.shape["shock"], mesh.shape["trans"])
    return jax.shard_map(body, mesh=mesh, in_specs=in_specs, out_specs=out_specs, check_vma=False)
```

```python
import functools
import math

import jax
import jax.numpy as jnp
import numpy as np
from jax import lax
from jax.experimental import pallas as pl
from jax.experimental.pallas import tpu as pltpu
from jax.sharding import PartitionSpec as P

F32 = jnp.float32
BF16 = jnp.bfloat16
MESH = pl.DeviceIdType.MESH

kick_factor = 0.5
drift_step = 0.02
cutoff_radius = 4.2
radial_width = 0.35
radial_centers = (1.4, 1.9, 2.4, 2.9)
moment_scale = 0.25
spacing = radial_centers[1] - radial_centers[0]
pair_list = ((0, 0), (0, 1), (0, 2), (0, 3), (1, 1), (1, 2), (1, 3), (2, 2), (2, 3), (3, 3))
LANES = 128
ROWS = 56
CHUNKS = ((0, 8), (8, 16), (16, 32), (32, 48), (48, 56))
MROWS = 40
DROWS = 64


def exponents():
    triples = []
    for degree in range(5):
        for p in range(degree, -1, -1):
            for q in range(degree - p, -1, -1):
                triples.append((p, q, degree - p - q))
    return triples


TRIPLES = exponents()
INDEX = {t: i for i, t in enumerate(TRIPLES)}
BASIS = [t for t in TRIPLES if t[2] < 2]
PLACE = {t: i for i, t in enumerate(BASIS)}


def reduced(t):
    p, q, w = t
    return (p, q, w - 2), (p + 2, q, w - 2), (p, q + 2, w - 2)


def lattice_rows():
    entries = []
    for number in range(8):
        entries.append(
            [1.0 - 2.0 * (number >> 2 & 1), 1.0 - 2.0 * (number >> 1 & 1), 1.0 - 2.0 * (number & 1)]
        )
    for axis_pick in range(3):
        for signed in (2.0, -2.0):
            vector = [0.0, 0.0, 0.0]
            vector[axis_pick] = signed
            entries.append(vector)
    for zero_pick in (2, 1, 0):
        others = [axis_pick for axis_pick in range(3) if axis_pick != zero_pick]
        for leading in (2.0, -2.0):
            for trailing in (2.0, -2.0):
                vector = [0.0, 0.0, 0.0]
                vector[others[0]] = leading
                vector[others[1]] = trailing
                entries.append(vector)
    while len(entries) < ROWS // 2:
        entries.append([1.0, 1.0, 1.0])
    table = np.repeat(np.array(entries, dtype=np.float32), 2, axis=0).T
    return np.broadcast_to(table[:, :, None], (3, ROWS, LANES)).copy()


def multiplicity(t):
    p, q, w = t
    return math.factorial(p + q + w) / (math.factorial(p) * math.factorial(q) * math.factorial(w))


def weight_rows():
    rows = np.zeros((MROWS, 2 * LANES), dtype=np.float32)
    for m, t in enumerate(TRIPLES):
        rows[m] = multiplicity(t)
    return rows


def selection_table():
    table = np.zeros((DROWS, len(pair_list) * MROWS), dtype=np.float32)
    for i in range(len(pair_list)):
        for m, t in enumerate(TRIPLES):
            table[5 * i + sum(t), MROWS * i + m] = 1.0
    return table


def split(x):
    hi = x.astype(BF16)
    lo = (x - hi.astype(F32)).astype(BF16)
    return hi, lo


def mm(a, b):
    return lax.dot_general(a, b, (((1,), (0,)), ((), ())), preferred_element_type=F32)


def mm_nt(a, b):
    return lax.dot_general(a, b, (((1,), (1,)), ((), ())), preferred_element_type=F32)


def lane_gather(x, index):
    numbers = lax.GatherDimensionNumbers(
        offset_dims=(),
        collapsed_slice_dims=(1,),
        start_index_map=(1,),
        operand_batching_dims=(0,),
        start_indices_batching_dims=(0,),
    )
    return lax.gather(
        x,
        index[:, :, None],
        numbers,
        slice_sizes=(1, 1),
        mode=lax.GatherScatterMode.PROMISE_IN_BOUNDS,
    )


def rows_of(row, count):
    return jnp.broadcast_to(row, (count, row.shape[1]))


def over(tile, count):
    return jnp.concatenate([tile] * count, axis=0) if count > 1 else tile


def row_sums(x):
    total = x[0:8, :]
    for i in range(8, x.shape[0], 8):
        total = total + x[i : i + 8, :]
    total = total + pltpu.roll(total, 4, 0)
    return total + pltpu.roll(total, 2, 0)


def horner(x, value, slope, term):
    if value is None:
        return term, None
    slope = value if slope is None else slope * x + value
    return value * x + term, slope


def sin_of(u):
    s = u * u
    r = -1.0 / 39916800.0
    for c in (1.0 / 362880.0, -1.0 / 5040.0, 1.0 / 120.0, -1.0 / 6.0, 1.0):
        r = r * s + c
    return r * u


def cos_of(u):
    s = u * u
    r = 1.0 / 479001600.0
    for c in (-1.0 / 3628800.0, 1.0 / 40320.0, -1.0 / 720.0, 1.0 / 24.0, -0.5, 1.0):
        r = r * s + c
    return r


DIRS = (
    (1, 1),
    (1, -1),
    (-1, 1),
    (-1, -1),
    (0, 1),
    (0, -1),
    (1, 0),
    (-1, 0),
    (-2, 1),
    (-2, -1),
    (-2, 0),
)
NEAR = 8
N_IN = 13


def kernel(n_shock, n_trans, *refs):
    hbm = refs[:N_IN]
    live, leave_count = refs[N_IN : N_IN + 2]
    out_disp, out_vel, out_force, out_energy, out_arr = refs[N_IN + 2 : N_IN + 7]
    (
        disp,
        vel,
        force,
        beta,
        alpha,
        trans_idx,
        shock_idx,
        nb_block,
        nb_lane,
        leave_idx,
        offs,
        weight,
        chosen,
        in_sems,
        t_send,
        s_send,
        f_recv,
        m_send,
        b_recv,
        w_send,
        w_recv,
        c_send,
        c_recv,
        p_send,
        p_recv,
        f_send_sems,
        f_recv_sems,
        b_send_sems,
        b_recv_sems,
        x_send_sems,
        x_recv_sems,
        ext,
        blk,
        lan,
        idx_pad,
        joined,
        near_own,
        geom,
        tiles,
        mom,
        dmom,
        mixing,
        by_descriptor,
        onehot,
        apad,
        hot0,
        hot1,
        arr_hot,
        grads,
        own_sum,
    ) = refs[N_IN + 7 :]
    local = (
        disp,
        vel,
        force,
        beta,
        alpha,
        trans_idx,
        shock_idx,
        nb_block,
        nb_lane,
        leave_idx,
        offs,
        weight,
        chosen,
    )
    loads = [
        pltpu.make_async_copy(src, dst, in_sems.at[i])
        for i, (src, dst) in enumerate(zip(hbm, local, strict=True))
    ]
    s_me = lax.axis_index("shock")
    t_me = lax.axis_index("trans")

    t_near = {
        -1: jnp.where(t_me > 0, t_me - 1, n_trans - 1),
        0: t_me,
        1: jnp.where(t_me < n_trans - 1, t_me + 1, 0),
    }

    def place(ds, dt):
        return s_me + ds, t_near[dt]

    inside = {
        -2: s_me > 1,
        -1: s_me > 0,
        0: None,
        1: s_me < n_shock - 1,
        2: s_me < n_shock - 2,
    }

    def where_inside(ds, action):
        if inside[ds] is None:
            action()
        else:
            pl.when(inside[ds])(action)

    def clear(ds):
        def action():
            for dt in (-1, 0, 1):
                k = DIRS.index((-ds, -dt))
                b_recv[k] = jnp.zeros((2, 4, LANES), F32)
                if k < NEAR:
                    f_recv[k] = jnp.zeros((2, 4, LANES), F32)
            if ds == 1:
                w_recv[...] = jnp.zeros((8, LANES), F32)
                c_recv[...] = jnp.zeros((8, LANES), F32)
                p_recv[...] = jnp.zeros((4, LANES), F32)

        pl.when(jnp.logical_not(inside[ds]))(action)

    barrier = pltpu.get_barrier_semaphore()

    def greet(ds):
        def action():
            for dt in (-1, 0, 1):
                if (ds, dt) != (0, 0):
                    pl.semaphore_signal(
                        barrier, inc=1, device_id=place(ds, dt), device_id_type=MESH
                    )

        return action

    for ds in (0, 1, -1, 2, -2):
        where_inside(ds, greet(ds))
    for i in (0, 1, 2, 5, 6, 7, 8, 9, 4, 3, 10, 11, 12):
        loads[i].start()
    peers = 2
    for ds in (1, -1, 2, -2):
        peers = peers + jnp.where(inside[ds], 3, 0)

    def remote(src, dst, send_sem, recv_sem, where):
        return pltpu.make_async_remote_copy(
            src_ref=src,
            dst_ref=dst,
            send_sem=send_sem,
            recv_sem=recv_sem,
            device_id=place(*where),
            device_id_type=MESH,
        )

    forward = [
        (
            ds,
            remote(
                s_send.at[(1 + ds) // 2] if dt == 0 else t_send if ds == 0 else t_send.at[0],
                f_recv.at[k] if ds == 0 else f_recv.at[k, 0],
                f_send_sems.at[k],
                f_recv_sems.at[k],
                (ds, dt),
            ),
        )
        for k, (ds, dt) in enumerate(DIRS[:NEAR])
    ]
    backward = [
        (
            ds,
            remote(
                m_send.at[part],
                b_recv.at[k, 0] if isinstance(part, int) else b_recv.at[k],
                b_send_sems.at[k],
                b_recv_sems.at[k],
                (ds, dt),
            ),
        )
        for k, (ds, dt) in enumerate(DIRS)
        for part in (
            0
            if ds == 1
            else pl.ds(0, 2)
            if ds == 0
            else pl.ds(1, 2)
            if ds == -1 and dt != 0
            else 2,
        )
    ]
    extra = [
        (-1, remote(src, dst, x_send_sems.at[i], x_recv_sems.at[i], (-1, 0)))
        for i, (src, dst) in enumerate(((w_send, w_recv), (c_send, c_recv), (p_send, p_recv)))
    ]

    def start(copies):
        for ds in (1, -1, 0, -2):
            chosen = [copy for at, copy in copies if at == ds]

            def action(chosen=chosen):
                for copy in chosen:
                    copy.start()

            if chosen:
                where_inside(ds, action)

    def receive(copies):
        for ds in (0, 1, -1, -2):
            chosen = [copy for at, copy in copies if at == ds]

            def action(chosen=chosen):
                for copy in chosen:
                    copy.wait_recv()

            if chosen:
                where_inside(-ds, action)

    def drain(copies):
        for ds in (0, 1, -1, -2):
            chosen = [copy for at, copy in copies if at == ds]

            def action(chosen=chosen):
                for copy in chosen:
                    copy.wait_send()

            if chosen:
                where_inside(ds, action)

    def slot(ds, dt):
        return DIRS.index((-ds, -dt))

    lane_row = lax.broadcasted_iota(jnp.int32, (1, LANES), 1)
    lane8 = lax.broadcasted_iota(jnp.int32, (8, LANES), 1)
    sub8 = lax.broadcasted_iota(jnp.int32, (8, LANES), 0)

    idx_pad[...] = jnp.zeros_like(idx_pad)
    joined[...] = jnp.zeros_like(joined)
    ext[...] = jnp.zeros_like(ext)
    for i in (0, 1, 2, 5, 6):
        loads[i].wait()
    half_velocity = vel[...] + kick_factor * force[...]
    displaced = disp[...] + drift_step * half_velocity
    for h in range(2):
        ext[h, 0:3, :] = displaced[:, h * LANES : (h + 1) * LANES]
    idx_pad[0:1, 0:32] = trans_idx[1:2, :]
    idx_pad[1:2, 0:32] = trans_idx[0:1, :]
    idx_pad[2:4, :] = pltpu.roll(shock_idx[...], 64, 1)
    t_row = jnp.where(lane_row < 32, idx_pad[0:1, :], pltpu.roll(idx_pad[1:2, :], 32, 1))
    shock8 = jnp.where(sub8 < 4, rows_of(idx_pad[2:3, :], 8), rows_of(idx_pad[3:4, :], 8))
    shock_block = shock8 >> 7
    shock_lane = shock8 & 127
    doubled = [jnp.where(sub8 < 4, ext[b], pltpu.roll(ext[b], 4, 0)) for b in range(2)]
    t_send[0] = lane_gather(ext[0], rows_of(t_row, 8))[0:4, :]
    t_send[1] = jnp.zeros((4, LANES), F32)
    t_send[1, 0:2, :] = idx_pad[2:4, :].astype(F32)
    s_own = jnp.where(
        shock_block == 0,
        lane_gather(doubled[0], shock_lane),
        jnp.where(shock_block == 1, lane_gather(doubled[1], shock_lane), 0.0),
    )
    s_all = jnp.where((sub8 & 3) == 3, shock8.astype(F32), s_own)
    s_send[0] = s_all[0:4, :]
    s_send[1] = s_all[4:8, :]

    pl.semaphore_wait(barrier, peers)
    start(forward)
    for ds in (-1, 1, 2):
        clear(ds)

    loads[9].wait()
    idx_pad[4:5, 0:16] = leave_idx[...]
    leave_row = idx_pad[4:5, :]
    sending = jnp.where(lane_row < leave_count[0], 1.0, 0.0)
    for h in range(2):
        ext[5 + h, 0:3, :] = half_velocity[:, h * LANES : (h + 1) * LANES]
    leaving = jnp.where(sub8 < 4, ext[0], pltpu.roll(ext[5], 4, 0))
    w_send[...] = lane_gather(leaving, rows_of(leave_row, 8)) * rows_of(sending, 8)
    start(extra[0:1])

    for i in (7, 8, 4, 3):
        loads[i].wait()
    blk[...] = jnp.full_like(blk, -1)
    lan[...] = jnp.zeros_like(lan)
    for h in range(2):
        hs = slice(h * LANES, (h + 1) * LANES)
        blk[pl.ds(h, 26, stride=2), :] = nb_block[:, hs]
        lan[pl.ds(h, 26, stride=2), :] = nb_lane[:, hs] & 127

    column128 = lax.broadcasted_iota(jnp.int32, (LANES, LANES), 0)

    def fill_onehot(k, carry):
        for h in range(2):
            row = lan[pl.ds(2 * k + h, 1), :]
            hot = jnp.where(column128 == rows_of(row, LANES), 1.0, 0.0).astype(BF16)
            at = pl.multiple_of((2 * k + h) * LANES, LANES)
            onehot[:, pl.ds(at, LANES)] = hot
        return carry

    lax.fori_loop(0, 26, fill_onehot, 0)
    for i in (10, 11, 12):
        loads[i].wait()
    even = (sub8 & 1) == 0
    block = blk[...]
    lane = lan[...]
    for c in range(3):
        own = jnp.where(even, rows_of(ext[0, c : c + 1, :], 8), rows_of(ext[1, c : c + 1, :], 8))
        parts = [lane_gather(rows_of(ext[b, c : c + 1, :], ROWS), lane) for b in range(2)]
        near_own[c] = (
            offs[c]
            - over(own, ROWS // 8)
            + jnp.where(block == 0, parts[0], jnp.where(block == 1, parts[1], 0.0))
        )

    leave_hot = jnp.where(column128 == rows_of(leave_row, LANES), 1.0, 0.0).astype(BF16)
    departed = mm_nt(rows_of(sending, 16).astype(BF16), leave_hot)[0:1, :]
    keep0 = jnp.where(lane_row < live[0], 1.0, 0.0) * (1.0 - departed)
    keep1 = jnp.where(lane_row + LANES < live[0], 1.0, 0.0)
    out_disp[:, 0:LANES] = displaced[:, 0:LANES] * rows_of(keep0, 3)
    out_disp[:, LANES:] = displaced[:, LANES:] * rows_of(keep1, 3)

    apad[...] = jnp.zeros_like(apad)
    apad[0:50, 0:50] = alpha[...]
    sym = 0.5 * (apad[...] + apad[...].T)
    sym_hi, sym_lo = split(sym[0:DROWS, 0:DROWS])
    mixed_hi, mixed_lo = split(mm(sym_hi, chosen[...]) + mm(sym_lo, chosen[...]))
    mixing[0:DROWS, :] = mixed_lo
    mixing[DROWS : 2 * DROWS, :] = mixed_hi
    mixing[2 * DROWS : 3 * DROWS, :] = chosen[...]
    apad[0:1, :] = jnp.zeros((1, LANES), F32)
    apad[0:1, 0:50] = beta[...]
    beta_col = rows_of(apad[0:1, :], LANES).T[0:DROWS, :]
    beta_col = jnp.concatenate([beta_col, beta_col], axis=1)
    for n in range(4):
        mom[n * MROWS + 32 : (n + 1) * MROWS, :] = jnp.zeros((8, 2 * LANES), F32)

    receive(forward)

    lane4 = lane8[0:4, :]

    def between(lower, upper):
        return jnp.where(lane4 < 32, lower, jnp.where(lane4 < 64, upper, 0.0))

    joined[0, 0:4, :] = between(f_recv[slot(-1, -1), 0], f_recv[slot(-1, 1), 0])
    joined[0, 4:8, :] = between(f_recv[slot(1, -1), 0], f_recv[slot(1, 1), 0])
    joined[1, 0:4, :] = f_recv[slot(-1, 0), 0]
    joined[1, 4:8, :] = f_recv[slot(1, 0), 0]
    joined[2, 0:4, :] = between(f_recv[slot(0, -1), 0], f_recv[slot(0, 1), 0])
    joined[3, 2:4, :] = f_recv[slot(0, 1), 1][0:2, :]
    joined[3, 4:6, :] = f_recv[slot(0, -1), 1][0:2, :]
    across = joined[0]
    direct = joined[1]
    t_ghost = joined[2]
    lists = jnp.where(sub8 < 4, rows_of(direct[3:4, :], 8), rows_of(direct[7:8, :], 8))
    lists = lists.astype(jnp.int32)
    both = jnp.where(lists >= 256, lane_gather(across, lists & 127), direct)
    swapped = pltpu.roll(both, 4, 0)
    ext[2] = jnp.where(lane8 < 64, t_ghost, both)
    ext[3] = jnp.where(lane8 < 64, both, swapped)
    ext[4] = swapped

    table = joined[3].astype(jnp.int32)
    through = lane_gather(rows_of(t_row, 8), table & 127)
    first_of = jnp.where(sub8 < 4, 256, 288)
    through = jnp.where(table >= first_of, jnp.where(table < first_of + 32, through, -1), -1)
    direct = idx_pad[2:4, :]
    c_send[...] = through.astype(F32)
    c_send[0:2, :] = jnp.where(direct < 256, direct, -1).astype(F32)
    c_send[6:7, :] = jnp.where(lane_row < 64, t_row, -1).astype(F32)
    c_send[7:8, :] = jnp.where(sending > 0.0, leave_row, -2).astype(F32)

    block = blk[...]
    lane = lan[...]
    parts = []
    for c in range(3):
        found = jnp.zeros((ROWS, LANES), F32)
        for b in range(2, 5):
            value = lane_gather(rows_of(ext[b, c : c + 1, :], ROWS), lane)
            found = jnp.where(block == b, value, found)
        parts.append(near_own[c] + found)
    px, py, pz = parts
    square = px * px + py * py + pz * pz
    inverse = lax.rsqrt(square)
    distance = square * inverse
    ux, uy, uz = px * inverse, py * inverse, pz * inverse
    angle = (0.5 * math.pi) - (0.5 * math.pi / cutoff_radius) * distance
    sine, cosine = sin_of(angle), cos_of(angle)
    sine_live = jnp.where(block >= 0, moment_scale * sine, 0.0)
    first_z = (distance - radial_centers[0]) * (1.0 / radial_width)
    radial = []
    for n, center in enumerate(radial_centers):
        z = (distance - center) * (1.0 / radial_width)
        weighted = sine_live * jnp.exp(-(z * z))
        radial.append(sine * weighted)
        geom[n] = weighted
    geom[4] = (-math.pi / cutoff_radius) * cosine - (2.0 / radial_width) * first_z * sine
    geom[5] = (2.0 * spacing / radial_width**2) * sine
    geom[6] = sine * inverse
    geom[8] = ux
    geom[9] = uy
    geom[10] = uz
    values = {}
    sums = {}
    for t in TRIPLES:
        p, q, w = t
        m = INDEX[t]
        if w > 1:
            low, left, right = reduced(t)
            for n in range(4):
                sums[(n, t)] = sums[(n, low)] - sums[(n, left)] - sums[(n, right)]
        else:
            if p > 0:
                prior, factor = values[(p - 1, q, w)], ux
            elif q > 0:
                prior, factor = values[(p, q - 1, w)], uy
            elif w > 0:
                prior, factor = values[(p, q, w - 1)], uz
            else:
                prior, factor = None, None
            value = factor if prior is None else prior * factor
            values[t] = value
            for n in range(4):
                sums[(n, t)] = row_sums(radial[n] if value is None else radial[n] * value)
        for n in range(4):
            at = n * MROWS + m
            mom[at : at + 1, 0:LANES] = sums[(n, t)][0:1, :]
            mom[at : at + 1, LANES:] = sums[(n, t)][1:2, :]

    moments = [mom[n * MROWS : (n + 1) * MROWS, :] for n in range(4)]
    heavy = [weight[...] * value for value in moments]
    products = jnp.concatenate([moments[n] * heavy[o] for n, o in pair_list], axis=0)
    prod_hi, prod_lo = split(products)
    high = mm(mixing[...], prod_hi)
    low = mm(mixing[DROWS : 3 * DROWS, :], prod_lo)
    by_descriptor[...] = beta_col + (
        high[0:DROWS, :] + high[DROWS : 2 * DROWS, :] + low[0:DROWS, :]
    )
    descriptor = high[2 * DROWS : 3 * DROWS, :] + low[DROWS : 2 * DROWS, :]
    energy = 0.5 * jnp.sum(descriptor * (beta_col + by_descriptor[...]), axis=0, keepdims=True)
    sub_wide = lax.broadcasted_iota(jnp.int32, (8, 2 * LANES), 0)
    totals = [None] * 4
    for i, (a, b) in enumerate(pair_list):
        r = [rows_of(by_descriptor[5 * i + l : 5 * i + l + 1, :], 8) for l in range(5)]
        spread_rows = jnp.concatenate(
            [
                jnp.where(sub_wide < 1, r[0], jnp.where(sub_wide < 4, r[1], r[2])),
                jnp.where(sub_wide < 2, r[2], r[3]),
                jnp.where(sub_wide < 4, r[3], r[4]),
                r[4],
                r[4],
            ],
            axis=0,
        )
        if a == b:
            terms = ((a, 2.0 * spread_rows * heavy[a]),)
        else:
            terms = ((a, spread_rows * heavy[b]), (b, spread_rows * heavy[a]))
        for n, term in terms:
            totals[n] = term if totals[n] is None else totals[n] + term
    for n in range(4):
        dmom[n * MROWS : (n + 1) * MROWS, :] = totals[n]

    for n in range(4):
        slopes = {}
        for t in TRIPLES:
            at = n * MROWS + INDEX[t]
            slopes[t] = jnp.where(
                even,
                rows_of(dmom[at : at + 1, 0:LANES], 8),
                rows_of(dmom[at : at + 1, LANES:], 8),
            )
        for t in sorted(TRIPLES, key=lambda t: -t[2]):
            if t[2] > 1:
                low, left, right = reduced(t)
                slopes[low] = slopes[low] + slopes[t]
                slopes[left] = slopes[left] - slopes[t]
                slopes[right] = slopes[right] - slopes[t]
        for t in BASIS:
            tiles[n * len(BASIS) + PLACE[t]] = slopes[t]

    part8 = sub8 & 3
    half_block = sub8 >> 2
    own_total = [None] * 3

    def pair_gradients(begin, end):
        count = (end - begin) // 8
        at = slice(begin, end)
        weighted = [geom[n, at, :] for n in range(4)]
        unit = [geom[8 + c, at, :] for c in range(3)]
        ux, uy, uz = unit
        found = []
        for w in range(2):
            size = 4 - w
            value_x = slope_x = slope_y = graded_x = None
            for p in range(size, -1, -1):
                value = slope = graded = None
                for q in range(size - p, -1, -1):
                    total = graded_total = None
                    for n in range(3, -1, -1):
                        b = over(tiles[n * len(BASIS) + PLACE[(p, q, w)]], count)
                        term = b * weighted[n]
                        total = term if total is None else total + term
                        if n > 0:
                            graded_total = total if graded_total is None else graded_total + total
                    value, slope = horner(uy, value, slope, total)
                    graded = graded_total if graded is None else graded * uy + graded_total
                value_x, slope_x = horner(ux, value_x, slope_x, value)
                graded_x = graded if graded_x is None else graded_x * ux + graded
                if slope is not None:
                    slope_y = slope if slope_y is None else slope_y * ux + slope
            found.append((value_x, slope_x, slope_y, graded_x))
        scaled = geom[6, at, :]
        tangent = [
            (found[0][1] + uz * found[1][1]) * scaled,
            (found[0][2] + uz * found[1][2]) * scaled,
            found[1][0] * scaled,
        ]
        along = geom[4, at, :] * (found[0][0] + uz * found[1][0])
        along = along + geom[5, at, :] * (found[0][3] + uz * found[1][3])
        along = along - (ux * tangent[0] + uy * tangent[1] + uz * tangent[2])
        for c in range(3):
            g = tangent[c] + unit[c] * along
            grads[c, at, :] = g
            for i in range(count):
                row = g[8 * i : 8 * i + 8, :]
                own_total[c] = row if own_total[c] is None else own_total[c] + row

    def spread_sums(begin, end):
        columns = []
        for r in range(begin, min(end, 52)):
            gx, gy, gz = (rows_of(grads[c, r : r + 1, :], 8) for c in range(3))
            value = jnp.where(part8 == 0, gx, jnp.where(part8 == 1, gy, gz))
            hi = value.astype(BF16).astype(F32)
            lo = value - hi
            place_of = rows_of(blk[r : r + 1, :], 8) - half_block
            masks = [place_of == 2 * i for i in range(3)]
            columns.append(
                jnp.concatenate(
                    [jnp.where(mask, x, 0.0) for x in (hi, lo) for mask in masks], axis=0
                ).astype(BF16)
            )
        last = min(end, 52)
        return mm_nt(jnp.concatenate(columns, axis=1), onehot[:, begin * LANES : last * LANES])

    spread = jnp.zeros((48, LANES), F32)
    pair_gradients(*CHUNKS[0])
    for at in range(len(CHUNKS)):
        if at + 1 < len(CHUNKS):
            pair_gradients(*CHUNKS[at + 1])
        spread = spread + spread_sums(*CHUNKS[at])
    for c in range(3):
        total = own_total[c] + pltpu.roll(own_total[c], 4, 0)
        total = total + pltpu.roll(total, 2, 0)
        for h in range(2):
            own_sum[h, c : c + 1, :] = total[h : h + 1, :]
    spread = spread[0:24, :] + spread[24:48, :]
    first = spread[0:8, :]
    second = spread[8:16, :]
    third = spread[16:24, :]
    swapped = pltpu.roll(second, 4, 0)
    grad0 = first - own_sum[0]
    m_send[0] = jnp.where(lane8 < 64, third, swapped)[0:4, :]
    m_send[1] = second[0:4, :]
    m_send[2] = jnp.where(lane8 < 64, swapped, second)[0:4, :]
    p_send[...] = jnp.where(sub8 < 3, grad0, 0.0)[0:4, :]
    start(backward)
    start(extra[1:3])

    rows = [c_send[i : i + 1, :].astype(jnp.int32) for i in range(7)]
    for i, row in enumerate(rows):
        at = slice(i * LANES, (i + 1) * LANES)
        hot0[:, at] = jnp.where(column128 == rows_of(row, LANES), 1.0, 0.0).astype(BF16)
        if i < 2:
            hot1[:, at] = jnp.where(
                column128 + LANES == rows_of(row, LANES), 1.0, 0.0
            ).astype(BF16)
    out_energy[:, 0:LANES] = energy[:, 0:LANES] * keep0
    out_energy[:, LANES:] = energy[:, LANES:] * keep1
    grad1 = pltpu.roll(first, 4, 0) - own_sum[1]

    receive(extra[0:2])
    slots = rows_of(c_recv[7:8, :], LANES).T[0:16, :]
    for i in range(8):
        row = lane_row.astype(F32) if i == 7 else c_recv[i : i + 1, :]
        arr_hot[:, i * LANES : (i + 1) * LANES] = jnp.where(
            rows_of(row, 16) == slots, 1.0, 0.0
        ).astype(BF16)

    receive(backward)
    receive(extra[2:3])

    def piece(ds, dt, part=0):
        return b_recv[slot(ds, dt), part]

    def pieces_of(tiles):
        back = jnp.concatenate(tiles, axis=1)
        hi = back.astype(BF16).astype(F32)
        return jnp.concatenate([hi, back - hi], axis=0).astype(BF16)

    back = pieces_of(
        (
            piece(-1, 0),
            piece(1, 0),
            piece(-1, 1),
            piece(1, 1, 1),
            piece(-1, -1),
            piece(1, -1, 1),
            between(piece(0, 1, 1), piece(0, -1, 1)),
        )
    )
    added0 = mm_nt(back, hot0[...])
    added1 = mm_nt(back[:, 0 : 2 * LANES], hot1[...])
    arriving = pieces_of(
        (
            m_send[0],
            piece(2, 0),
            piece(0, 1),
            piece(2, 1),
            piece(0, -1),
            piece(2, -1),
            between(piece(1, 1), piece(1, -1)),
            p_recv[...],
        )
    )
    added2 = mm_nt(arriving, arr_hot[...])
    force0 = -(grad0 + added0 + pltpu.roll(added0, 4, 0))[0:3, :]
    velocity0 = half_velocity[:, 0:LANES] + kick_factor * force0
    force1 = -(grad1 + added1 + pltpu.roll(added1, 4, 0))[0:3, :]
    velocity1 = half_velocity[:, LANES:] + kick_factor * force1
    force2 = -(added2 + pltpu.roll(added2, 4, 0))[0:3, :]
    state = w_recv[...]
    out_vel[:, 0:LANES] = velocity0 * rows_of(keep0, 3)
    out_force[:, 0:LANES] = force0 * rows_of(keep0, 3)
    out_vel[:, LANES:] = velocity1 * rows_of(keep1, 3)
    out_force[:, LANES:] = force1 * rows_of(keep1, 3)
    for q, value in enumerate(
        (state[0:3, 0:16], state[4:7, 0:16] + kick_factor * force2, force2)
    ):
        out_arr[q] = jnp.where(s_me < n_shock - 1, value, 0.0)
    drain(forward)
    drain(backward)
    drain(extra)


def kept(shape):
    return pltpu.VMEM(shape, F32)


def in_place(x):
    return pltpu.with_memory_space_constraint(x, pltpu.VMEM)


def finish(*refs):
    for i in range(5):
        refs[5 + i][...] = refs[i][...]


def whole_step(n_shock, n_trans, *args):
    (disp, vel, force, beta, alpha, live, trans_idx, shock_idx, block, lane, leave, count) = args
    inputs = (
        disp,
        vel,
        force,
        beta.reshape(1, 50),
        alpha,
        trans_idx,
        shock_idx,
        block,
        lane,
        leave.reshape(1, 16),
        jnp.asarray(lattice_rows()),
        jnp.asarray(weight_rows()),
        jnp.asarray(selection_table(), BF16),
    )
    vmem = pl.BlockSpec(memory_space=pltpu.VMEM)
    tile = (8, LANES)
    half_tile = (4, LANES)
    shapes = ((3, 256), (3, 256), (3, 256), (1, 256), (3, 3, 16))
    outs = pl.pallas_call(
        functools.partial(kernel, n_shock, n_trans),
        out_shape=tuple(kept(shape) for shape in shapes),
        in_specs=[pl.BlockSpec(memory_space=pltpu.HBM)] * N_IN
        + [pl.BlockSpec(memory_space=pltpu.SMEM)] * 2,
        out_specs=(vmem,) * 5,
        scratch_shapes=[
            pltpu.VMEM(x.shape, x.dtype) for x in inputs
        ]
        + [
            pltpu.SemaphoreType.DMA((N_IN,)),
            pltpu.VMEM((2, *half_tile), F32),
            pltpu.VMEM((2, *half_tile), F32),
            pltpu.VMEM((NEAR, 2, *half_tile), F32),
            pltpu.VMEM((3, *half_tile), F32),
            pltpu.VMEM((len(DIRS), 2, *half_tile), F32),
            pltpu.VMEM(tile, F32),
            pltpu.VMEM(tile, F32),
            pltpu.VMEM(tile, F32),
            pltpu.VMEM(tile, F32),
            pltpu.VMEM(half_tile, F32),
            pltpu.VMEM(half_tile, F32),
            pltpu.SemaphoreType.DMA((NEAR,)),
            pltpu.SemaphoreType.DMA((NEAR,)),
            pltpu.SemaphoreType.DMA((len(DIRS),)),
            pltpu.SemaphoreType.DMA((len(DIRS),)),
            pltpu.SemaphoreType.DMA((3,)),
            pltpu.SemaphoreType.DMA((3,)),
            pltpu.VMEM((7, *tile), F32),
            pltpu.VMEM((ROWS, LANES), jnp.int32),
            pltpu.VMEM((ROWS, LANES), jnp.int32),
            pltpu.VMEM(tile, jnp.int32),
            pltpu.VMEM((4, *tile), F32),
            pltpu.VMEM((3, ROWS, LANES), F32),
            pltpu.VMEM((11, ROWS, LANES), F32),
            pltpu.VMEM((4 * len(BASIS), *tile), F32),
            pltpu.VMEM((4 * MROWS, 256), F32),
            pltpu.VMEM((4 * MROWS, 256), F32),
            pltpu.VMEM((3 * DROWS, 10 * MROWS), BF16),
            pltpu.VMEM((DROWS, 256), F32),
            pltpu.VMEM((LANES, 26 * 256), BF16),
            pltpu.VMEM((LANES, LANES), F32),
            pltpu.VMEM((LANES, 7 * LANES), BF16),
            pltpu.VMEM((LANES, 2 * LANES), BF16),
            pltpu.VMEM((16, 8 * LANES), BF16),
            pltpu.VMEM((3, ROWS, LANES), F32),
            pltpu.VMEM((2, *tile), F32),
        ],
        compiler_params=pltpu.CompilerParams(collective_id=0, has_side_effects=True),
        name="whole_step",
    )(*inputs, live, count)
    outs = [in_place(x) for x in outs]
    outs = pl.pallas_call(
        finish,
        out_shape=tuple(jax.ShapeDtypeStruct(shape, F32) for shape in shapes),
        in_specs=[vmem] * 5,
        out_specs=(vmem,) * 5,
        name="finish",
    )(*outs)
    return outs[0], outs[1], outs[2], outs[3].reshape(256), outs[4]


def solution(mesh):
    split_1 = P(None, ("shock", "trans"))
    split_0 = P(("shock", "trans"))
    in_specs = (
        split_1,
        split_1,
        split_1,
        P(),
        P(),
        split_0,
        split_1,
        split_1,
        split_1,
        split_1,
        split_0,
        split_0,
    )
    out_specs = (split_1, split_1, split_1, split_0, P(None, None, ("shock", "trans")))
    body = functools.partial(whole_step, mesh.shape["shock"], mesh.shape["trans"])
    return jax.shard_map(body, mesh=mesh, in_specs=in_specs, out_specs=out_specs, check_vma=False)
```

```python
import functools
import math

import jax
import jax.numpy as jnp
import numpy as np
from jax import lax
from jax.experimental import pallas as pl
from jax.experimental.pallas import tpu as pltpu
from jax.sharding import PartitionSpec as P

F32 = jnp.float32
BF16 = jnp.bfloat16
MESH = pl.DeviceIdType.MESH

kick_factor = 0.5
drift_step = 0.02
cutoff_radius = 4.2
radial_width = 0.35
radial_centers = (1.4, 1.9, 2.4, 2.9)
moment_scale = 0.25
spacing = radial_centers[1] - radial_centers[0]
pair_list = ((0, 0), (0, 1), (0, 2), (0, 3), (1, 1), (1, 2), (1, 3), (2, 2), (2, 3), (3, 3))
LANES = 128
ROWS = 56
CHUNKS = ((0, 8), (8, 16), (16, 32), (32, 48), (48, 56))
MROWS = 40
DROWS = 64


def exponents():
    triples = []
    for degree in range(5):
        for p in range(degree, -1, -1):
            for q in range(degree - p, -1, -1):
                triples.append((p, q, degree - p - q))
    return triples


TRIPLES = exponents()
INDEX = {t: i for i, t in enumerate(TRIPLES)}
BASIS = [t for t in TRIPLES if t[2] < 2]
PLACE = {t: i for i, t in enumerate(BASIS)}


def reduced(t):
    p, q, w = t
    return (p, q, w - 2), (p + 2, q, w - 2), (p, q + 2, w - 2)


def lattice_rows():
    entries = []
    for number in range(8):
        entries.append(
            [1.0 - 2.0 * (number >> 2 & 1), 1.0 - 2.0 * (number >> 1 & 1), 1.0 - 2.0 * (number & 1)]
        )
    for axis_pick in range(3):
        for signed in (2.0, -2.0):
            vector = [0.0, 0.0, 0.0]
            vector[axis_pick] = signed
            entries.append(vector)
    for zero_pick in (2, 1, 0):
        others = [axis_pick for axis_pick in range(3) if axis_pick != zero_pick]
        for leading in (2.0, -2.0):
            for trailing in (2.0, -2.0):
                vector = [0.0, 0.0, 0.0]
                vector[others[0]] = leading
                vector[others[1]] = trailing
                entries.append(vector)
    while len(entries) < ROWS // 2:
        entries.append([1.0, 1.0, 1.0])
    table = np.repeat(np.array(entries, dtype=np.float32), 2, axis=0).T
    return np.broadcast_to(table[:, :, None], (3, ROWS, LANES)).copy()


def multiplicity(t):
    p, q, w = t
    return math.factorial(p + q + w) / (math.factorial(p) * math.factorial(q) * math.factorial(w))


def weight_rows():
    rows = np.zeros((MROWS, 2 * LANES), dtype=np.float32)
    for m, t in enumerate(TRIPLES):
        rows[m] = multiplicity(t)
    return rows


def selection_table():
    table = np.zeros((DROWS, len(pair_list) * MROWS), dtype=np.float32)
    for i in range(len(pair_list)):
        for m, t in enumerate(TRIPLES):
            table[5 * i + sum(t), MROWS * i + m] = 1.0
    return table


def split(x):
    hi = x.astype(BF16)
    lo = (x - hi.astype(F32)).astype(BF16)
    return hi, lo


def mm(a, b):
    return lax.dot_general(a, b, (((1,), (0,)), ((), ())), preferred_element_type=F32)


def mm_nt(a, b):
    return lax.dot_general(a, b, (((1,), (1,)), ((), ())), preferred_element_type=F32)


def lane_gather(x, index):
    numbers = lax.GatherDimensionNumbers(
        offset_dims=(),
        collapsed_slice_dims=(1,),
        start_index_map=(1,),
        operand_batching_dims=(0,),
        start_indices_batching_dims=(0,),
    )
    return lax.gather(
        x,
        index[:, :, None],
        numbers,
        slice_sizes=(1, 1),
        mode=lax.GatherScatterMode.PROMISE_IN_BOUNDS,
    )


def rows_of(row, count):
    return jnp.broadcast_to(row, (count, row.shape[1]))


def over(tile, count):
    return jnp.concatenate([tile] * count, axis=0) if count > 1 else tile


def row_sums(x):
    total = x[0:8, :]
    for i in range(8, x.shape[0], 8):
        total = total + x[i : i + 8, :]
    total = total + pltpu.roll(total, 4, 0)
    return total + pltpu.roll(total, 2, 0)


def horner(x, value, slope, term):
    if value is None:
        return term, None
    slope = value if slope is None else slope * x + value
    return value * x + term, slope


def sin_of(u):
    s = u * u
    r = -1.0 / 39916800.0
    for c in (1.0 / 362880.0, -1.0 / 5040.0, 1.0 / 120.0, -1.0 / 6.0, 1.0):
        r = r * s + c
    return r * u


def cos_of(u):
    s = u * u
    r = 1.0 / 479001600.0
    for c in (-1.0 / 3628800.0, 1.0 / 40320.0, -1.0 / 720.0, 1.0 / 24.0, -0.5, 1.0):
        r = r * s + c
    return r


DIRS = (
    (1, 1),
    (1, -1),
    (-1, 1),
    (-1, -1),
    (0, 1),
    (0, -1),
    (1, 0),
    (-1, 0),
    (-2, 1),
    (-2, -1),
    (-2, 0),
)
GROUPS = (1, -1, 0, -2)
NEAR = 8
N_IN = 13


def kernel(n_shock, n_trans, *refs):
    hbm = refs[:N_IN]
    live, leave_count = refs[N_IN : N_IN + 2]
    out_disp, out_vel, out_force, out_energy, out_arr = refs[N_IN + 2 : N_IN + 7]
    (
        disp,
        vel,
        force,
        beta,
        alpha,
        trans_idx,
        shock_idx,
        nb_block,
        nb_lane,
        leave_idx,
        offs,
        weight,
        chosen,
        in_sems,
        t_send,
        s_send,
        f_recv,
        m_send,
        b_recv,
        w_send,
        w_recv,
        c_send,
        c_recv,
        p_send,
        p_recv,
        send_sems,
        recv_sems,
        ext,
        blk,
        lan,
        idx_pad,
        joined,
        near_own,
        geom,
        tiles,
        mom,
        dmom,
        mixing,
        by_descriptor,
        onehot,
        apad,
        hot0,
        hot1,
        arr_hot,
        grads,
        own_sum,
    ) = refs[N_IN + 7 :]
    local = (
        disp,
        vel,
        force,
        beta,
        alpha,
        trans_idx,
        shock_idx,
        nb_block,
        nb_lane,
        leave_idx,
        offs,
        weight,
        chosen,
    )
    loads = [
        pltpu.make_async_copy(src, dst, in_sems.at[i])
        for i, (src, dst) in enumerate(zip(hbm, local, strict=True))
    ]
    s_me = lax.axis_index("shock")
    t_me = lax.axis_index("trans")

    t_near = {
        -1: jnp.where(t_me > 0, t_me - 1, n_trans - 1),
        0: t_me,
        1: jnp.where(t_me < n_trans - 1, t_me + 1, 0),
    }

    def place(ds, dt):
        return s_me + ds, t_near[dt]

    inside = {
        -2: s_me > 1,
        -1: s_me > 0,
        0: None,
        1: s_me < n_shock - 1,
        2: s_me < n_shock - 2,
    }

    def where_inside(ds, action):
        if inside[ds] is None:
            action()
        else:
            pl.when(inside[ds])(action)

    def clear(ds):
        def action():
            for dt in (-1, 0, 1):
                k = DIRS.index((-ds, -dt))
                b_recv[k] = jnp.zeros((2, 4, LANES), F32)
                if k < NEAR:
                    f_recv[k] = jnp.zeros((2, 4, LANES), F32)
            if ds == 1:
                w_recv[...] = jnp.zeros((8, LANES), F32)
                c_recv[...] = jnp.zeros((8, LANES), F32)
                p_recv[...] = jnp.zeros((8, LANES), F32)

        pl.when(jnp.logical_not(inside[ds]))(action)

    barrier = pltpu.get_barrier_semaphore()

    def greet(ds):
        def action():
            for dt in (-1, 0, 1):
                if (ds, dt) != (0, 0):
                    pl.semaphore_signal(
                        barrier, inc=1, device_id=place(ds, dt), device_id_type=MESH
                    )

        return action

    for ds in (0, 1, -1, 2, -2):
        where_inside(ds, greet(ds))
    for i in (0, 1, 2, 5, 6, 7, 8, 9, 4, 3, 10, 11, 12):
        loads[i].start()
    peers = 2
    for ds in (1, -1, 2, -2):
        peers = peers + jnp.where(inside[ds], 3, 0)

    def remote(src, dst, send_sem, recv_sem, where):
        return pltpu.make_async_remote_copy(
            src_ref=src,
            dst_ref=dst,
            send_sem=send_sem,
            recv_sem=recv_sem,
            device_id=place(*where),
            device_id_type=MESH,
        )

    forward = [
        (
            ds,
            remote(
                s_send.at[(1 + ds) // 2] if dt == 0 else t_send if ds == 0 else t_send.at[0],
                f_recv.at[k] if ds == 0 else f_recv.at[k, 0],
                send_sems.at[GROUPS.index(ds)],
                recv_sems.at[GROUPS.index(ds)],
                (ds, dt),
            ),
        )
        for k, (ds, dt) in enumerate(DIRS[:NEAR])
    ]
    backward = [
        (
            ds,
            remote(
                m_send.at[part],
                b_recv.at[k, 0] if isinstance(part, int) else b_recv.at[k],
                send_sems.at[GROUPS.index(ds)],
                recv_sems.at[4 + GROUPS.index(ds)],
                (ds, dt),
            ),
        )
        for k, (ds, dt) in enumerate(DIRS)
        for part in (
            0
            if ds == 1
            else pl.ds(0, 2)
            if ds == 0
            else pl.ds(1, 2)
            if ds == -1 and dt != 0
            else 2,
        )
    ]
    extra = [
        (
            -1,
            remote(src, dst, send_sems.at[GROUPS.index(-1)], recv_sems.at[(3, 3, 5)[i]], (-1, 0)),
        )
        for i, (src, dst) in enumerate(((w_send, w_recv), (c_send, c_recv), (p_send, p_recv)))
    ]

    def start(copies):
        for ds in (1, -1, 0, -2):
            chosen = [copy for at, copy in copies if at == ds]

            def action(chosen=chosen):
                for copy in chosen:
                    copy.start()

            if chosen:
                where_inside(ds, action)

    def pieces(count):
        if count > len(DIRS):
            return b_recv.at[pl.ds(0, count // 2)]
        return b_recv.at[pl.ds(0, count), 0]

    def waited(count, k):
        return remote(pieces(count), pieces(count), send_sems.at[k % 4], recv_sems.at[k], (0, 1))

    def receive(counts):
        for k, ds, count in counts:
            where_inside(-ds, lambda k=k, count=count: waited(count, k).wait_recv())

    def drain():
        for k, (ds, count) in enumerate(zip(GROUPS, (6, 14, 8, 3), strict=True)):
            where_inside(ds, lambda k=k, count=count: waited(count, k).wait_send())

    def slot(ds, dt):
        return DIRS.index((-ds, -dt))

    lane_row = lax.broadcasted_iota(jnp.int32, (1, LANES), 1)
    lane8 = lax.broadcasted_iota(jnp.int32, (8, LANES), 1)
    sub8 = lax.broadcasted_iota(jnp.int32, (8, LANES), 0)

    idx_pad[...] = jnp.zeros_like(idx_pad)
    joined[...] = jnp.zeros_like(joined)
    ext[...] = jnp.zeros_like(ext)
    for i in (0, 1, 2, 5, 6):
        loads[i].wait()
    half_velocity = vel[...] + kick_factor * force[...]
    displaced = disp[...] + drift_step * half_velocity
    for h in range(2):
        ext[h, 0:3, :] = displaced[:, h * LANES : (h + 1) * LANES]
    idx_pad[0:1, 0:32] = trans_idx[1:2, :]
    idx_pad[1:2, 0:32] = trans_idx[0:1, :]
    idx_pad[2:4, :] = pltpu.roll(shock_idx[...], 64, 1)
    t_row = jnp.where(lane_row < 32, idx_pad[0:1, :], pltpu.roll(idx_pad[1:2, :], 32, 1))
    shock8 = jnp.where(sub8 < 4, rows_of(idx_pad[2:3, :], 8), rows_of(idx_pad[3:4, :], 8))
    shock_block = shock8 >> 7
    shock_lane = shock8 & 127
    doubled = [jnp.where(sub8 < 4, ext[b], pltpu.roll(ext[b], 4, 0)) for b in range(2)]
    t_send[0] = lane_gather(ext[0], rows_of(t_row, 8))[0:4, :]
    t_send[1] = jnp.zeros((4, LANES), F32)
    t_send[1, 0:2, :] = idx_pad[2:4, :].astype(F32)
    s_own = jnp.where(
        shock_block == 0,
        lane_gather(doubled[0], shock_lane),
        jnp.where(shock_block == 1, lane_gather(doubled[1], shock_lane), 0.0),
    )
    s_all = jnp.where((sub8 & 3) == 3, shock8.astype(F32), s_own)
    s_send[0] = s_all[0:4, :]
    s_send[1] = s_all[4:8, :]

    pl.semaphore_wait(barrier, peers)
    start(forward)
    for ds in (-1, 1, 2):
        clear(ds)

    loads[9].wait()
    idx_pad[4:5, 0:16] = leave_idx[...]
    leave_row = idx_pad[4:5, :]
    sending = jnp.where(lane_row < leave_count[0], 1.0, 0.0)
    for h in range(2):
        ext[5 + h, 0:3, :] = half_velocity[:, h * LANES : (h + 1) * LANES]
    leaving = jnp.where(sub8 < 4, ext[0], pltpu.roll(ext[5], 4, 0))
    w_send[...] = lane_gather(leaving, rows_of(leave_row, 8)) * rows_of(sending, 8)
    start(extra[0:1])

    for i in (7, 8, 4, 3):
        loads[i].wait()
    blk[...] = jnp.full_like(blk, -1)
    lan[...] = jnp.zeros_like(lan)
    for h in range(2):
        hs = slice(h * LANES, (h + 1) * LANES)
        blk[pl.ds(h, 26, stride=2), :] = nb_block[:, hs]
        lan[pl.ds(h, 26, stride=2), :] = nb_lane[:, hs] & 127

    column128 = lax.broadcasted_iota(jnp.int32, (LANES, LANES), 0)

    def fill_onehot(k, carry):
        for h in range(2):
            row = lan[pl.ds(2 * k + h, 1), :]
            hot = jnp.where(column128 == rows_of(row, LANES), 1.0, 0.0).astype(BF16)
            at = pl.multiple_of((2 * k + h) * LANES, LANES)
            onehot[:, pl.ds(at, LANES)] = hot
        return carry

    lax.fori_loop(0, 26, fill_onehot, 0)
    for i in (10, 11, 12):
        loads[i].wait()
    even = (sub8 & 1) == 0
    block = blk[...]
    lane = lan[...]
    for c in range(3):
        own = jnp.where(even, rows_of(ext[0, c : c + 1, :], 8), rows_of(ext[1, c : c + 1, :], 8))
        parts = [lane_gather(rows_of(ext[b, c : c + 1, :], ROWS), lane) for b in range(2)]
        near_own[c] = (
            offs[c]
            - over(own, ROWS // 8)
            + jnp.where(block == 0, parts[0], jnp.where(block == 1, parts[1], 0.0))
        )

    leave_hot = jnp.where(column128 == rows_of(leave_row, LANES), 1.0, 0.0).astype(BF16)
    departed = mm_nt(rows_of(sending, 16).astype(BF16), leave_hot)[0:1, :]
    keep0 = jnp.where(lane_row < live[0], 1.0, 0.0) * (1.0 - departed)
    keep1 = jnp.where(lane_row + LANES < live[0], 1.0, 0.0)
    out_disp[:, 0:LANES] = displaced[:, 0:LANES] * rows_of(keep0, 3)
    out_disp[:, LANES:] = displaced[:, LANES:] * rows_of(keep1, 3)

    apad[...] = jnp.zeros_like(apad)
    apad[0:50, 0:50] = alpha[...]
    sym = 0.5 * (apad[...] + apad[...].T)
    sym_hi, sym_lo = split(sym[0:DROWS, 0:DROWS])
    mixed_hi, mixed_lo = split(mm(sym_hi, chosen[...]) + mm(sym_lo, chosen[...]))
    mixing[0:DROWS, :] = mixed_lo
    mixing[DROWS : 2 * DROWS, :] = mixed_hi
    mixing[2 * DROWS : 3 * DROWS, :] = chosen[...]
    apad[0:1, :] = jnp.zeros((1, LANES), F32)
    apad[0:1, 0:50] = beta[...]
    beta_col = rows_of(apad[0:1, :], LANES).T[0:DROWS, :]
    beta_col = jnp.concatenate([beta_col, beta_col], axis=1)
    for n in range(4):
        mom[n * MROWS + 32 : (n + 1) * MROWS, :] = jnp.zeros((8, 2 * LANES), F32)

    receive(((2, 0, 4), (0, 1, 3), (1, -1, 3)))

    lane4 = lane8[0:4, :]

    def between(lower, upper):
        return jnp.where(lane4 < 32, lower, jnp.where(lane4 < 64, upper, 0.0))

    joined[0, 0:4, :] = between(f_recv[slot(-1, -1), 0], f_recv[slot(-1, 1), 0])
    joined[0, 4:8, :] = between(f_recv[slot(1, -1), 0], f_recv[slot(1, 1), 0])
    joined[1, 0:4, :] = f_recv[slot(-1, 0), 0]
    joined[1, 4:8, :] = f_recv[slot(1, 0), 0]
    joined[2, 0:4, :] = between(f_recv[slot(0, -1), 0], f_recv[slot(0, 1), 0])
    joined[3, 2:4, :] = f_recv[slot(0, 1), 1][0:2, :]
    joined[3, 4:6, :] = f_recv[slot(0, -1), 1][0:2, :]
    across = joined[0]
    direct = joined[1]
    t_ghost = joined[2]
    lists = jnp.where(sub8 < 4, rows_of(direct[3:4, :], 8), rows_of(direct[7:8, :], 8))
    lists = lists.astype(jnp.int32)
    both = jnp.where(lists >= 256, lane_gather(across, lists & 127), direct)
    swapped = pltpu.roll(both, 4, 0)
    ext[2] = jnp.where(lane8 < 64, t_ghost, both)
    ext[3] = jnp.where(lane8 < 64, both, swapped)
    ext[4] = swapped

    table = joined[3].astype(jnp.int32)
    through = lane_gather(rows_of(t_row, 8), table & 127)
    first_of = jnp.where(sub8 < 4, 256, 288)
    through = jnp.where(table >= first_of, jnp.where(table < first_of + 32, through, -1), -1)
    direct = idx_pad[2:4, :]
    c_send[...] = through.astype(F32)
    c_send[0:2, :] = jnp.where(direct < 256, direct, -1).astype(F32)
    c_send[6:7, :] = jnp.where(lane_row < 64, t_row, -1).astype(F32)
    c_send[7:8, :] = jnp.where(sending > 0.0, leave_row, -2).astype(F32)

    block = blk[...]
    lane = lan[...]
    parts = []
    for c in range(3):
        found = jnp.zeros((ROWS, LANES), F32)
        for b in range(2, 5):
            value = lane_gather(rows_of(ext[b, c : c + 1, :], ROWS), lane)
            found = jnp.where(block == b, value, found)
        parts.append(near_own[c] + found)
    px, py, pz = parts
    square = px * px + py * py + pz * pz
    inverse = lax.rsqrt(square)
    distance = square * inverse
    ux, uy, uz = px * inverse, py * inverse, pz * inverse
    angle = (0.5 * math.pi) - (0.5 * math.pi / cutoff_radius) * distance
    sine, cosine = sin_of(angle), cos_of(angle)
    sine_live = jnp.where(block >= 0, moment_scale * sine, 0.0)
    first_z = (distance - radial_centers[0]) * (1.0 / radial_width)
    radial = []
    for n, center in enumerate(radial_centers):
        z = (distance - center) * (1.0 / radial_width)
        weighted = sine_live * jnp.exp(-(z * z))
        radial.append(sine * weighted)
        geom[n] = weighted
    geom[4] = (-math.pi / cutoff_radius) * cosine - (2.0 / radial_width) * first_z * sine
    geom[5] = (2.0 * spacing / radial_width**2) * sine
    geom[6] = sine * inverse
    geom[8] = ux
    geom[9] = uy
    geom[10] = uz
    values = {}
    sums = {}
    for t in TRIPLES:
        p, q, w = t
        m = INDEX[t]
        if w > 1:
            low, left, right = reduced(t)
            for n in range(4):
                sums[(n, t)] = sums[(n, low)] - sums[(n, left)] - sums[(n, right)]
        else:
            if p > 0:
                prior, factor = values[(p - 1, q, w)], ux
            elif q > 0:
                prior, factor = values[(p, q - 1, w)], uy
            elif w > 0:
                prior, factor = values[(p, q, w - 1)], uz
            else:
                prior, factor = None, None
            value = factor if prior is None else prior * factor
            values[t] = value
            for n in range(4):
                sums[(n, t)] = row_sums(radial[n] if value is None else radial[n] * value)
        for n in range(4):
            at = n * MROWS + m
            mom[at : at + 1, 0:LANES] = sums[(n, t)][0:1, :]
            mom[at : at + 1, LANES:] = sums[(n, t)][1:2, :]

    moments = [mom[n * MROWS : (n + 1) * MROWS, :] for n in range(4)]
    heavy = [weight[...] * value for value in moments]
    products = jnp.concatenate([moments[n] * heavy[o] for n, o in pair_list], axis=0)
    prod_hi, prod_lo = split(products)
    high = mm(mixing[...], prod_hi)
    low = mm(mixing[DROWS : 3 * DROWS, :], prod_lo)
    by_descriptor[...] = beta_col + (
        high[0:DROWS, :] + high[DROWS : 2 * DROWS, :] + low[0:DROWS, :]
    )
    descriptor = high[2 * DROWS : 3 * DROWS, :] + low[DROWS : 2 * DROWS, :]
    energy = 0.5 * jnp.sum(descriptor * (beta_col + by_descriptor[...]), axis=0, keepdims=True)
    sub_wide = lax.broadcasted_iota(jnp.int32, (8, 2 * LANES), 0)
    totals = [None] * 4
    for i, (a, b) in enumerate(pair_list):
        r = [rows_of(by_descriptor[5 * i + l : 5 * i + l + 1, :], 8) for l in range(5)]
        spread_rows = jnp.concatenate(
            [
                jnp.where(sub_wide < 1, r[0], jnp.where(sub_wide < 4, r[1], r[2])),
                jnp.where(sub_wide < 2, r[2], r[3]),
                jnp.where(sub_wide < 4, r[3], r[4]),
                r[4],
                r[4],
            ],
            axis=0,
        )
        if a == b:
            terms = ((a, 2.0 * spread_rows * heavy[a]),)
        else:
            terms = ((a, spread_rows * heavy[b]), (b, spread_rows * heavy[a]))
        for n, term in terms:
            totals[n] = term if totals[n] is None else totals[n] + term
    for n in range(4):
        dmom[n * MROWS : (n + 1) * MROWS, :] = totals[n]

    for n in range(4):
        slopes = {}
        for t in TRIPLES:
            at = n * MROWS + INDEX[t]
            slopes[t] = jnp.where(
                even,
                rows_of(dmom[at : at + 1, 0:LANES], 8),
                rows_of(dmom[at : at + 1, LANES:], 8),
            )
        for t in sorted(TRIPLES, key=lambda t: -t[2]):
            if t[2] > 1:
                low, left, right = reduced(t)
                slopes[low] = slopes[low] + slopes[t]
                slopes[left] = slopes[left] - slopes[t]
                slopes[right] = slopes[right] - slopes[t]
        for t in BASIS:
            tiles[n * len(BASIS) + PLACE[t]] = slopes[t]

    part8 = sub8 & 3
    half_block = sub8 >> 2
    own_total = [None] * 3

    def pair_gradients(begin, end):
        count = (end - begin) // 8
        at = slice(begin, end)
        weighted = [geom[n, at, :] for n in range(4)]
        unit = [geom[8 + c, at, :] for c in range(3)]
        ux, uy, uz = unit
        found = []
        for w in range(2):
            size = 4 - w
            value_x = slope_x = slope_y = graded_x = None
            for p in range(size, -1, -1):
                value = slope = graded = None
                for q in range(size - p, -1, -1):
                    total = graded_total = None
                    for n in range(3, -1, -1):
                        b = over(tiles[n * len(BASIS) + PLACE[(p, q, w)]], count)
                        term = b * weighted[n]
                        total = term if total is None else total + term
                        if n > 0:
                            graded_total = total if graded_total is None else graded_total + total
                    value, slope = horner(uy, value, slope, total)
                    graded = graded_total if graded is None else graded * uy + graded_total
                value_x, slope_x = horner(ux, value_x, slope_x, value)
                graded_x = graded if graded_x is None else graded_x * ux + graded
                if slope is not None:
                    slope_y = slope if slope_y is None else slope_y * ux + slope
            found.append((value_x, slope_x, slope_y, graded_x))
        scaled = geom[6, at, :]
        tangent = [
            (found[0][1] + uz * found[1][1]) * scaled,
            (found[0][2] + uz * found[1][2]) * scaled,
            found[1][0] * scaled,
        ]
        along = geom[4, at, :] * (found[0][0] + uz * found[1][0])
        along = along + geom[5, at, :] * (found[0][3] + uz * found[1][3])
        along = along - (ux * tangent[0] + uy * tangent[1] + uz * tangent[2])
        for c in range(3):
            g = tangent[c] + unit[c] * along
            grads[c, at, :] = g
            for i in range(count):
                row = g[8 * i : 8 * i + 8, :]
                own_total[c] = row if own_total[c] is None else own_total[c] + row

    def spread_sums(begin, end):
        columns = []
        for r in range(begin, min(end, 52)):
            gx, gy, gz = (rows_of(grads[c, r : r + 1, :], 8) for c in range(3))
            value = jnp.where(part8 == 0, gx, jnp.where(part8 == 1, gy, gz))
            hi = value.astype(BF16).astype(F32)
            lo = value - hi
            place_of = rows_of(blk[r : r + 1, :], 8) - half_block
            masks = [place_of == 2 * i for i in range(3)]
            columns.append(
                jnp.concatenate(
                    [jnp.where(mask, x, 0.0) for x in (hi, lo) for mask in masks], axis=0
                ).astype(BF16)
            )
        last = min(end, 52)
        return mm_nt(jnp.concatenate(columns, axis=1), onehot[:, begin * LANES : last * LANES])

    spread = jnp.zeros((48, LANES), F32)
    pair_gradients(*CHUNKS[0])
    for at in range(len(CHUNKS)):
        if at + 1 < len(CHUNKS):
            pair_gradients(*CHUNKS[at + 1])
        spread = spread + spread_sums(*CHUNKS[at])
    for c in range(3):
        total = own_total[c] + pltpu.roll(own_total[c], 4, 0)
        total = total + pltpu.roll(total, 2, 0)
        for h in range(2):
            own_sum[h, c : c + 1, :] = total[h : h + 1, :]
    spread = spread[0:24, :] + spread[24:48, :]
    first = spread[0:8, :]
    second = spread[8:16, :]
    third = spread[16:24, :]
    swapped = pltpu.roll(second, 4, 0)
    grad0 = first - own_sum[0]
    m_send[0] = jnp.where(lane8 < 64, third, swapped)[0:4, :]
    m_send[1] = second[0:4, :]
    m_send[2] = jnp.where(lane8 < 64, swapped, second)[0:4, :]
    p_send[...] = jnp.where(sub8 < 3, grad0, 0.0)
    start(backward)
    start(extra[1:3])

    rows = [c_send[i : i + 1, :].astype(jnp.int32) for i in range(7)]
    for i, row in enumerate(rows):
        at = slice(i * LANES, (i + 1) * LANES)
        hot0[:, at] = jnp.where(column128 == rows_of(row, LANES), 1.0, 0.0).astype(BF16)
        if i < 2:
            hot1[:, at] = jnp.where(
                column128 + LANES == rows_of(row, LANES), 1.0, 0.0
            ).astype(BF16)
    out_energy[:, 0:LANES] = energy[:, 0:LANES] * keep0
    out_energy[:, LANES:] = energy[:, LANES:] * keep1
    grad1 = pltpu.roll(first, 4, 0) - own_sum[1]

    receive(((3, -1, 4),))
    slots = rows_of(c_recv[7:8, :], LANES).T[0:16, :]
    for i in range(8):
        row = lane_row.astype(F32) if i == 7 else c_recv[i : i + 1, :]
        arr_hot[:, i * LANES : (i + 1) * LANES] = jnp.where(
            rows_of(row, 16) == slots, 1.0, 0.0
        ).astype(BF16)

    receive(((6, 0, 4), (4, 1, 3), (5, -1, 7), (7, -2, 3)))

    def piece(ds, dt, part=0):
        return b_recv[slot(ds, dt), part]

    def pieces_of(tiles):
        back = jnp.concatenate(tiles, axis=1)
        hi = back.astype(BF16).astype(F32)
        return jnp.concatenate([hi, back - hi], axis=0).astype(BF16)

    back = pieces_of(
        (
            piece(-1, 0),
            piece(1, 0),
            piece(-1, 1),
            piece(1, 1, 1),
            piece(-1, -1),
            piece(1, -1, 1),
            between(piece(0, 1, 1), piece(0, -1, 1)),
        )
    )
    added0 = mm_nt(back, hot0[...])
    added1 = mm_nt(back[:, 0 : 2 * LANES], hot1[...])
    arriving = pieces_of(
        (
            m_send[0],
            piece(2, 0),
            piece(0, 1),
            piece(2, 1),
            piece(0, -1),
            piece(2, -1),
            between(piece(1, 1), piece(1, -1)),
            p_recv[0:4, :],
        )
    )
    added2 = mm_nt(arriving, arr_hot[...])
    force0 = -(grad0 + added0 + pltpu.roll(added0, 4, 0))[0:3, :]
    velocity0 = half_velocity[:, 0:LANES] + kick_factor * force0
    force1 = -(grad1 + added1 + pltpu.roll(added1, 4, 0))[0:3, :]
    velocity1 = half_velocity[:, LANES:] + kick_factor * force1
    force2 = -(added2 + pltpu.roll(added2, 4, 0))[0:3, :]
    state = w_recv[...]
    out_vel[:, 0:LANES] = velocity0 * rows_of(keep0, 3)
    out_force[:, 0:LANES] = force0 * rows_of(keep0, 3)
    out_vel[:, LANES:] = velocity1 * rows_of(keep1, 3)
    out_force[:, LANES:] = force1 * rows_of(keep1, 3)
    for q, value in enumerate(
        (state[0:3, 0:16], state[4:7, 0:16] + kick_factor * force2, force2)
    ):
        out_arr[q] = jnp.where(s_me < n_shock - 1, value, 0.0)
    drain()


def kept(shape):
    return pltpu.VMEM(shape, F32)


def in_place(x):
    return pltpu.with_memory_space_constraint(x, pltpu.VMEM)


def finish(*refs):
    for i in range(5):
        refs[5 + i][...] = refs[i][...]


def whole_step(n_shock, n_trans, *args):
    (disp, vel, force, beta, alpha, live, trans_idx, shock_idx, block, lane, leave, count) = args
    inputs = (
        disp,
        vel,
        force,
        beta.reshape(1, 50),
        alpha,
        trans_idx,
        shock_idx,
        block,
        lane,
        leave.reshape(1, 16),
        jnp.asarray(lattice_rows()),
        jnp.asarray(weight_rows()),
        jnp.asarray(selection_table(), BF16),
    )
    vmem = pl.BlockSpec(memory_space=pltpu.VMEM)
    tile = (8, LANES)
    half_tile = (4, LANES)
    shapes = ((3, 256), (3, 256), (3, 256), (1, 256), (3, 3, 16))
    outs = pl.pallas_call(
        functools.partial(kernel, n_shock, n_trans),
        out_shape=tuple(kept(shape) for shape in shapes),
        in_specs=[pl.BlockSpec(memory_space=pltpu.HBM)] * N_IN
        + [pl.BlockSpec(memory_space=pltpu.SMEM)] * 2,
        out_specs=(vmem,) * 5,
        scratch_shapes=[
            pltpu.VMEM(x.shape, x.dtype) for x in inputs
        ]
        + [
            pltpu.SemaphoreType.DMA((N_IN,)),
            pltpu.VMEM((2, *half_tile), F32),
            pltpu.VMEM((2, *half_tile), F32),
            pltpu.VMEM((NEAR, 2, *half_tile), F32),
            pltpu.VMEM((3, *half_tile), F32),
            pltpu.VMEM((len(DIRS), 2, *half_tile), F32),
            pltpu.VMEM(tile, F32),
            pltpu.VMEM(tile, F32),
            pltpu.VMEM(tile, F32),
            pltpu.VMEM(tile, F32),
            pltpu.VMEM(tile, F32),
            pltpu.VMEM(tile, F32),
            pltpu.SemaphoreType.DMA((4,)),
            pltpu.SemaphoreType.DMA((8,)),
            pltpu.VMEM((7, *tile), F32),
            pltpu.VMEM((ROWS, LANES), jnp.int32),
            pltpu.VMEM((ROWS, LANES), jnp.int32),
            pltpu.VMEM(tile, jnp.int32),
            pltpu.VMEM((4, *tile), F32),
            pltpu.VMEM((3, ROWS, LANES), F32),
            pltpu.VMEM((11, ROWS, LANES), F32),
            pltpu.VMEM((4 * len(BASIS), *tile), F32),
            pltpu.VMEM((4 * MROWS, 256), F32),
            pltpu.VMEM((4 * MROWS, 256), F32),
            pltpu.VMEM((3 * DROWS, 10 * MROWS), BF16),
            pltpu.VMEM((DROWS, 256), F32),
            pltpu.VMEM((LANES, 26 * 256), BF16),
            pltpu.VMEM((LANES, LANES), F32),
            pltpu.VMEM((LANES, 7 * LANES), BF16),
            pltpu.VMEM((LANES, 2 * LANES), BF16),
            pltpu.VMEM((16, 8 * LANES), BF16),
            pltpu.VMEM((3, ROWS, LANES), F32),
            pltpu.VMEM((2, *tile), F32),
        ],
        compiler_params=pltpu.CompilerParams(collective_id=0, has_side_effects=True),
        name="whole_step",
    )(*inputs, live, count)
    outs = [in_place(x) for x in outs]
    outs = pl.pallas_call(
        finish,
        out_shape=tuple(jax.ShapeDtypeStruct(shape, F32) for shape in shapes),
        in_specs=[vmem] * 5,
        out_specs=(vmem,) * 5,
        name="finish",
    )(*outs)
    return outs[0], outs[1], outs[2], outs[3].reshape(256), outs[4]


def solution(mesh):
    split_1 = P(None, ("shock", "trans"))
    split_0 = P(("shock", "trans"))
    in_specs = (
        split_1,
        split_1,
        split_1,
        P(),
        P(),
        split_0,
        split_1,
        split_1,
        split_1,
        split_1,
        split_0,
        split_0,
    )
    out_specs = (split_1, split_1, split_1, split_0, P(None, None, ("shock", "trans")))
    body = functools.partial(whole_step, mesh.shape["shock"], mesh.shape["trans"])
    return jax.shard_map(body, mesh=mesh, in_specs=in_specs, out_specs=out_specs, check_vma=False)
```

```python
import functools
import math

import jax
import jax.numpy as jnp
import numpy as np
from jax import lax
from jax.experimental import pallas as pl
from jax.experimental.pallas import tpu as pltpu
from jax.sharding import PartitionSpec as P

F32 = jnp.float32
BF16 = jnp.bfloat16
MESH = pl.DeviceIdType.MESH

kick_factor = 0.5
drift_step = 0.02
cutoff_radius = 4.2
radial_width = 0.35
radial_centers = (1.4, 1.9, 2.4, 2.9)
moment_scale = 0.25
spacing = radial_centers[1] - radial_centers[0]
pair_list = ((0, 0), (0, 1), (0, 2), (0, 3), (1, 1), (1, 2), (1, 3), (2, 2), (2, 3), (3, 3))
LANES = 128
ROWS = 56
CHUNKS = ((0, 8), (8, 16), (16, 32), (32, 48), (48, 56))
MROWS = 40
DROWS = 64


def exponents():
    triples = []
    for degree in range(5):
        for p in range(degree, -1, -1):
            for q in range(degree - p, -1, -1):
                triples.append((p, q, degree - p - q))
    return triples


TRIPLES = exponents()
INDEX = {t: i for i, t in enumerate(TRIPLES)}
BASIS = [t for t in TRIPLES if t[2] < 2]
PLACE = {t: i for i, t in enumerate(BASIS)}


def reduced(t):
    p, q, w = t
    return (p, q, w - 2), (p + 2, q, w - 2), (p, q + 2, w - 2)


def lattice_rows():
    entries = []
    for number in range(8):
        entries.append(
            [1.0 - 2.0 * (number >> 2 & 1), 1.0 - 2.0 * (number >> 1 & 1), 1.0 - 2.0 * (number & 1)]
        )
    for axis_pick in range(3):
        for signed in (2.0, -2.0):
            vector = [0.0, 0.0, 0.0]
            vector[axis_pick] = signed
            entries.append(vector)
    for zero_pick in (2, 1, 0):
        others = [axis_pick for axis_pick in range(3) if axis_pick != zero_pick]
        for leading in (2.0, -2.0):
            for trailing in (2.0, -2.0):
                vector = [0.0, 0.0, 0.0]
                vector[others[0]] = leading
                vector[others[1]] = trailing
                entries.append(vector)
    while len(entries) < ROWS // 2:
        entries.append([1.0, 1.0, 1.0])
    table = np.repeat(np.array(entries, dtype=np.float32), 2, axis=0).T
    return np.broadcast_to(table[:, :, None], (3, ROWS, LANES)).copy()


def multiplicity(t):
    p, q, w = t
    return math.factorial(p + q + w) / (math.factorial(p) * math.factorial(q) * math.factorial(w))


def weight_rows():
    rows = np.zeros((MROWS, 2 * LANES), dtype=np.float32)
    for m, t in enumerate(TRIPLES):
        rows[m] = multiplicity(t)
    return rows


def selection_table():
    table = np.zeros((DROWS, len(pair_list) * MROWS), dtype=np.float32)
    for i in range(len(pair_list)):
        for m, t in enumerate(TRIPLES):
            table[5 * i + sum(t), MROWS * i + m] = 1.0
    return table


def split(x):
    hi = x.astype(BF16)
    lo = (x - hi.astype(F32)).astype(BF16)
    return hi, lo


def mm(a, b):
    return lax.dot_general(a, b, (((1,), (0,)), ((), ())), preferred_element_type=F32)


def mm_nt(a, b):
    return lax.dot_general(a, b, (((1,), (1,)), ((), ())), preferred_element_type=F32)


def lane_gather(x, index):
    numbers = lax.GatherDimensionNumbers(
        offset_dims=(),
        collapsed_slice_dims=(1,),
        start_index_map=(1,),
        operand_batching_dims=(0,),
        start_indices_batching_dims=(0,),
    )
    return lax.gather(
        x,
        index[:, :, None],
        numbers,
        slice_sizes=(1, 1),
        mode=lax.GatherScatterMode.PROMISE_IN_BOUNDS,
    )


def rows_of(row, count):
    return jnp.broadcast_to(row, (count, row.shape[1]))


def over(tile, count):
    return jnp.concatenate([tile] * count, axis=0) if count > 1 else tile


def row_sums(x):
    total = x[0:8, :]
    for i in range(8, x.shape[0], 8):
        total = total + x[i : i + 8, :]
    total = total + pltpu.roll(total, 4, 0)
    return total + pltpu.roll(total, 2, 0)


def horner(x, value, slope, term):
    if value is None:
        return term, None
    slope = value if slope is None else slope * x + value
    return value * x + term, slope


def sin_of(u):
    s = u * u
    r = -1.0 / 39916800.0
    for c in (1.0 / 362880.0, -1.0 / 5040.0, 1.0 / 120.0, -1.0 / 6.0, 1.0):
        r = r * s + c
    return r * u


def cos_of(u):
    s = u * u
    r = 1.0 / 479001600.0
    for c in (-1.0 / 3628800.0, 1.0 / 40320.0, -1.0 / 720.0, 1.0 / 24.0, -0.5, 1.0):
        r = r * s + c
    return r


DIRS = (
    (1, 1),
    (1, -1),
    (-1, 1),
    (-1, -1),
    (0, 1),
    (0, -1),
    (1, 0),
    (-1, 0),
    (-2, 1),
    (-2, -1),
    (-2, 0),
)
GROUPS = (1, -1, 0, -2)
NEAR = 8
N_IN = 13


def kernel(n_shock, n_trans, *refs):
    hbm = refs[:N_IN]
    live, leave_count = refs[N_IN : N_IN + 2]
    out_disp, out_vel, out_force, out_energy, out_arr = refs[N_IN + 2 : N_IN + 7]
    (
        disp,
        vel,
        force,
        beta,
        alpha,
        trans_idx,
        shock_idx,
        nb_block,
        nb_lane,
        leave_idx,
        offs,
        weight,
        chosen,
        in_sems,
        t_send,
        s_send,
        f_recv,
        m_send,
        b_recv,
        w_send,
        w_recv,
        c_send,
        c_recv,
        p_send,
        p_recv,
        send_sems,
        recv_sems,
        ext,
        blk,
        lan,
        idx_pad,
        joined,
        near_own,
        geom,
        tiles,
        mom,
        dmom,
        mixing,
        by_descriptor,
        onehot,
        apad,
        hot0,
        hot1,
        arr_hot,
        grads,
        own_sum,
    ) = refs[N_IN + 7 :]
    local = (
        disp,
        vel,
        force,
        beta,
        alpha,
        trans_idx,
        shock_idx,
        nb_block,
        nb_lane,
        leave_idx,
        offs,
        weight,
        chosen,
    )
    loads = [
        pltpu.make_async_copy(src, dst, in_sems.at[i])
        for i, (src, dst) in enumerate(zip(hbm, local, strict=True))
    ]
    s_me = lax.axis_index("shock")
    t_me = lax.axis_index("trans")

    t_near = {
        -1: jnp.where(t_me > 0, t_me - 1, n_trans - 1),
        0: t_me,
        1: jnp.where(t_me < n_trans - 1, t_me + 1, 0),
    }

    def place(ds, dt):
        return s_me + ds, t_near[dt]

    inside = {
        -2: s_me > 1,
        -1: s_me > 0,
        0: None,
        1: s_me < n_shock - 1,
        2: s_me < n_shock - 2,
    }

    def where_inside(ds, action):
        if inside[ds] is None:
            action()
        else:
            pl.when(inside[ds])(action)

    def clear(ds):
        def action():
            for dt in (-1, 0, 1):
                k = DIRS.index((-ds, -dt))
                b_recv[k] = jnp.zeros((2, 4, LANES), F32)
                if k < NEAR:
                    f_recv[k] = jnp.zeros((2, 4, LANES), F32)
            if ds == 1:
                w_recv[...] = jnp.zeros((8, LANES), F32)
                c_recv[...] = jnp.zeros((8, LANES), F32)
                p_recv[...] = jnp.zeros((8, LANES), F32)

        pl.when(jnp.logical_not(inside[ds]))(action)

    barrier = pltpu.get_barrier_semaphore()

    def greet(ds):
        def action():
            for dt in (-1, 0, 1):
                if (ds, dt) != (0, 0):
                    pl.semaphore_signal(
                        barrier, inc=1, device_id=place(ds, dt), device_id_type=MESH
                    )

        return action

    for ds in (0, 1, -1, 2, -2):
        where_inside(ds, greet(ds))
    for i in (0, 1, 2, 5, 6, 7, 8, 9, 4, 3, 10, 11, 12):
        loads[i].start()
    peers = 2
    for ds in (1, -1, 2, -2):
        peers = peers + jnp.where(inside[ds], 3, 0)

    def remote(src, dst, send_sem, recv_sem, where):
        return pltpu.make_async_remote_copy(
            src_ref=src,
            dst_ref=dst,
            send_sem=send_sem,
            recv_sem=recv_sem,
            device_id=place(*where),
            device_id_type=MESH,
        )

    forward = [
        (
            ds,
            remote(
                s_send.at[(1 + ds) // 2] if dt == 0 else t_send if ds == 0 else t_send.at[0],
                f_recv.at[k] if ds == 0 else f_recv.at[k, 0],
                send_sems.at[GROUPS.index(ds)],
                recv_sems.at[GROUPS.index(ds)],
                (ds, dt),
            ),
        )
        for k, (ds, dt) in enumerate(DIRS[:NEAR])
    ]
    backward = [
        (
            ds,
            remote(
                m_send.at[part],
                b_recv.at[k, 0] if isinstance(part, int) else b_recv.at[k],
                send_sems.at[GROUPS.index(ds)],
                recv_sems.at[4 + GROUPS.index(ds)],
                (ds, dt),
            ),
        )
        for k, (ds, dt) in enumerate(DIRS)
        for part in (
            0
            if ds == 1
            else pl.ds(0, 2)
            if ds == 0
            else pl.ds(1, 2)
            if ds == -1 and dt != 0
            else 2,
        )
    ]
    extra = [
        (
            -1,
            remote(src, dst, send_sems.at[GROUPS.index(-1)], recv_sems.at[(3, 3, 5)[i]], (-1, 0)),
        )
        for i, (src, dst) in enumerate(((w_send, w_recv), (c_send, c_recv), (p_send, p_recv)))
    ]

    def start(copies):
        for ds in (1, -1, 0, -2):
            chosen = [copy for at, copy in copies if at == ds]

            def action(chosen=chosen):
                for copy in chosen:
                    copy.start()

            if chosen:
                where_inside(ds, action)

    def pieces(count):
        if count > len(DIRS):
            return b_recv.at[pl.ds(0, count // 2)]
        return b_recv.at[pl.ds(0, count), 0]

    def waited(count, k):
        return remote(pieces(count), pieces(count), send_sems.at[k % 4], recv_sems.at[k], (0, 1))

    def receive(counts):
        for k, ds, count in counts:
            where_inside(-ds, lambda k=k, count=count: waited(count, k).wait_recv())

    def drain():
        for k, (ds, count) in enumerate(zip(GROUPS, (6, 14, 8, 3), strict=True)):
            where_inside(ds, lambda k=k, count=count: waited(count, k).wait_send())

    def slot(ds, dt):
        return DIRS.index((-ds, -dt))

    lane_row = lax.broadcasted_iota(jnp.int32, (1, LANES), 1)
    lane8 = lax.broadcasted_iota(jnp.int32, (8, LANES), 1)
    sub8 = lax.broadcasted_iota(jnp.int32, (8, LANES), 0)

    idx_pad[...] = jnp.zeros_like(idx_pad)
    joined[...] = jnp.zeros_like(joined)
    ext[...] = jnp.zeros_like(ext)
    for i in (0, 1, 2, 5, 6):
        loads[i].wait()
    half_velocity = vel[...] + kick_factor * force[...]
    displaced = disp[...] + drift_step * half_velocity
    for h in range(2):
        ext[h, 0:3, :] = displaced[:, h * LANES : (h + 1) * LANES]
    idx_pad[0:1, 0:32] = trans_idx[1:2, :]
    idx_pad[1:2, 0:32] = trans_idx[0:1, :]
    idx_pad[2:4, :] = pltpu.roll(shock_idx[...], 64, 1)
    t_row = jnp.where(lane_row < 32, idx_pad[0:1, :], pltpu.roll(idx_pad[1:2, :], 32, 1))
    shock8 = jnp.where(sub8 < 4, rows_of(idx_pad[2:3, :], 8), rows_of(idx_pad[3:4, :], 8))
    shock_block = shock8 >> 7
    shock_lane = shock8 & 127
    doubled = [jnp.where(sub8 < 4, ext[b], pltpu.roll(ext[b], 4, 0)) for b in range(2)]
    t_send[0] = lane_gather(ext[0], rows_of(t_row, 8))[0:4, :]
    t_send[1] = jnp.zeros((4, LANES), F32)
    t_send[1, 0:2, :] = idx_pad[2:4, :].astype(F32)
    s_own = jnp.where(
        shock_block == 0,
        lane_gather(doubled[0], shock_lane),
        jnp.where(shock_block == 1, lane_gather(doubled[1], shock_lane), 0.0),
    )
    s_all = jnp.where((sub8 & 3) == 3, shock8.astype(F32), s_own)
    s_send[0] = s_all[0:4, :]
    s_send[1] = s_all[4:8, :]

    pl.semaphore_wait(barrier, peers)
    start(forward[0:6])
    start(forward[6:8])
    for ds in (-1, 1, 2):
        clear(ds)

    loads[9].wait()
    idx_pad[4:5, 0:16] = leave_idx[...]
    leave_row = idx_pad[4:5, :]
    sending = jnp.where(lane_row < leave_count[0], 1.0, 0.0)
    for h in range(2):
        ext[5 + h, 0:3, :] = half_velocity[:, h * LANES : (h + 1) * LANES]
    leaving = jnp.where(sub8 < 4, ext[0], pltpu.roll(ext[5], 4, 0))
    w_send[...] = lane_gather(leaving, rows_of(leave_row, 8)) * rows_of(sending, 8)
    start(extra[0:1])

    for i in (7, 8, 4, 3):
        loads[i].wait()
    blk[...] = jnp.full_like(blk, -1)
    lan[...] = jnp.zeros_like(lan)
    for h in range(2):
        hs = slice(h * LANES, (h + 1) * LANES)
        blk[pl.ds(h, 26, stride=2), :] = nb_block[:, hs]
        lan[pl.ds(h, 26, stride=2), :] = nb_lane[:, hs] & 127

    column128 = lax.broadcasted_iota(jnp.int32, (LANES, LANES), 0)

    def fill_onehot(k, carry):
        for h in range(2):
            row = lan[pl.ds(2 * k + h, 1), :]
            hot = jnp.where(column128 == rows_of(row, LANES), 1.0, 0.0).astype(BF16)
            at = pl.multiple_of((2 * k + h) * LANES, LANES)
            onehot[:, pl.ds(at, LANES)] = hot
        return carry

    lax.fori_loop(0, 26, fill_onehot, 0)
    for i in (10, 11, 12):
        loads[i].wait()
    even = (sub8 & 1) == 0
    block = blk[...]
    lane = lan[...]
    for c in range(3):
        own = jnp.where(even, rows_of(ext[0, c : c + 1, :], 8), rows_of(ext[1, c : c + 1, :], 8))
        parts = [lane_gather(rows_of(ext[b, c : c + 1, :], ROWS), lane) for b in range(2)]
        near_own[c] = (
            offs[c]
            - over(own, ROWS // 8)
            + jnp.where(block == 0, parts[0], jnp.where(block == 1, parts[1], 0.0))
        )

    leave_hot = jnp.where(column128 == rows_of(leave_row, LANES), 1.0, 0.0).astype(BF16)
    departed = mm_nt(rows_of(sending, 16).astype(BF16), leave_hot)[0:1, :]
    keep0 = jnp.where(lane_row < live[0], 1.0, 0.0) * (1.0 - departed)
    keep1 = jnp.where(lane_row + LANES < live[0], 1.0, 0.0)
    out_disp[:, 0:LANES] = displaced[:, 0:LANES] * rows_of(keep0, 3)
    out_disp[:, LANES:] = displaced[:, LANES:] * rows_of(keep1, 3)

    apad[...] = jnp.zeros_like(apad)
    apad[0:50, 0:50] = alpha[...]
    sym = 0.5 * (apad[...] + apad[...].T)
    sym_hi, sym_lo = split(sym[0:DROWS, 0:DROWS])
    mixed_hi, mixed_lo = split(mm(sym_hi, chosen[...]) + mm(sym_lo, chosen[...]))
    mixing[0:DROWS, :] = mixed_lo
    mixing[DROWS : 2 * DROWS, :] = mixed_hi
    mixing[2 * DROWS : 3 * DROWS, :] = chosen[...]
    apad[0:1, :] = jnp.zeros((1, LANES), F32)
    apad[0:1, 0:50] = beta[...]
    beta_col = rows_of(apad[0:1, :], LANES).T[0:DROWS, :]
    beta_col = jnp.concatenate([beta_col, beta_col], axis=1)
    for n in range(4):
        mom[n * MROWS + 32 : (n + 1) * MROWS, :] = jnp.zeros((8, 2 * LANES), F32)

    receive(((2, 0, 4), (0, 1, 3), (1, -1, 3)))

    lane4 = lane8[0:4, :]

    def between(lower, upper):
        return jnp.where(lane4 < 32, lower, jnp.where(lane4 < 64, upper, 0.0))

    joined[0, 0:4, :] = between(f_recv[slot(-1, -1), 0], f_recv[slot(-1, 1), 0])
    joined[0, 4:8, :] = between(f_recv[slot(1, -1), 0], f_recv[slot(1, 1), 0])
    joined[1, 0:4, :] = f_recv[slot(-1, 0), 0]
    joined[1, 4:8, :] = f_recv[slot(1, 0), 0]
    joined[2, 0:4, :] = between(f_recv[slot(0, -1), 0], f_recv[slot(0, 1), 0])
    joined[3, 2:4, :] = f_recv[slot(0, 1), 1][0:2, :]
    joined[3, 4:6, :] = f_recv[slot(0, -1), 1][0:2, :]
    across = joined[0]
    direct = joined[1]
    t_ghost = joined[2]
    lists = jnp.where(sub8 < 4, rows_of(direct[3:4, :], 8), rows_of(direct[7:8, :], 8))
    lists = lists.astype(jnp.int32)
    both = jnp.where(lists >= 256, lane_gather(across, lists & 127), direct)
    swapped = pltpu.roll(both, 4, 0)
    ext[2] = jnp.where(lane8 < 64, t_ghost, both)
    ext[3] = jnp.where(lane8 < 64, both, swapped)
    ext[4] = swapped

    table = joined[3].astype(jnp.int32)
    through = lane_gather(rows_of(t_row, 8), table & 127)
    first_of = jnp.where(sub8 < 4, 256, 288)
    through = jnp.where(table >= first_of, jnp.where(table < first_of + 32, through, -1), -1)
    direct = idx_pad[2:4, :]
    c_send[...] = through.astype(F32)
    c_send[0:2, :] = jnp.where(direct < 256, direct, -1).astype(F32)
    c_send[6:7, :] = jnp.where(lane_row < 64, t_row, -1).astype(F32)
    c_send[7:8, :] = jnp.where(sending > 0.0, leave_row, -2).astype(F32)

    block = blk[...]
    lane = lan[...]
    parts = []
    for c in range(3):
        found = jnp.zeros((ROWS, LANES), F32)
        for b in range(2, 5):
            value = lane_gather(rows_of(ext[b, c : c + 1, :], ROWS), lane)
            found = jnp.where(block == b, value, found)
        parts.append(near_own[c] + found)
    px, py, pz = parts
    square = px * px + py * py + pz * pz
    inverse = lax.rsqrt(square)
    distance = square * inverse
    ux, uy, uz = px * inverse, py * inverse, pz * inverse
    angle = (0.5 * math.pi) - (0.5 * math.pi / cutoff_radius) * distance
    sine, cosine = sin_of(angle), cos_of(angle)
    sine_live = jnp.where(block >= 0, moment_scale * sine, 0.0)
    first_z = (distance - radial_centers[0]) * (1.0 / radial_width)
    radial = []
    for n, center in enumerate(radial_centers):
        z = (distance - center) * (1.0 / radial_width)
        weighted = sine_live * jnp.exp(-(z * z))
        radial.append(sine * weighted)
        geom[n] = weighted
    geom[4] = (-math.pi / cutoff_radius) * cosine - (2.0 / radial_width) * first_z * sine
    geom[5] = (2.0 * spacing / radial_width**2) * sine
    geom[6] = sine * inverse
    geom[8] = ux
    geom[9] = uy
    geom[10] = uz
    values = {}
    sums = {}
    for t in TRIPLES:
        p, q, w = t
        m = INDEX[t]
        if w > 1:
            low, left, right = reduced(t)
            for n in range(4):
                sums[(n, t)] = sums[(n, low)] - sums[(n, left)] - sums[(n, right)]
        else:
            if p > 0:
                prior, factor = values[(p - 1, q, w)], ux
            elif q > 0:
                prior, factor = values[(p, q - 1, w)], uy
            elif w > 0:
                prior, factor = values[(p, q, w - 1)], uz
            else:
                prior, factor = None, None
            value = factor if prior is None else prior * factor
            values[t] = value
            for n in range(4):
                sums[(n, t)] = row_sums(radial[n] if value is None else radial[n] * value)
        for n in range(4):
            at = n * MROWS + m
            mom[at : at + 1, 0:LANES] = sums[(n, t)][0:1, :]
            mom[at : at + 1, LANES:] = sums[(n, t)][1:2, :]

    moments = [mom[n * MROWS : (n + 1) * MROWS, :] for n in range(4)]
    heavy = [weight[...] * value for value in moments]
    products = jnp.concatenate([moments[n] * heavy[o] for n, o in pair_list], axis=0)
    prod_hi, prod_lo = split(products)
    high = mm(mixing[...], prod_hi)
    low = mm(mixing[DROWS : 3 * DROWS, :], prod_lo)
    by_descriptor[...] = beta_col + (
        high[0:DROWS, :] + high[DROWS : 2 * DROWS, :] + low[0:DROWS, :]
    )
    descriptor = high[2 * DROWS : 3 * DROWS, :] + low[DROWS : 2 * DROWS, :]
    energy = 0.5 * jnp.sum(descriptor * (beta_col + by_descriptor[...]), axis=0, keepdims=True)
    sub_wide = lax.broadcasted_iota(jnp.int32, (8, 2 * LANES), 0)
    totals = [None] * 4
    for i, (a, b) in enumerate(pair_list):
        r = [rows_of(by_descriptor[5 * i + l : 5 * i + l + 1, :], 8) for l in range(5)]
        spread_rows = jnp.concatenate(
            [
                jnp.where(sub_wide < 1, r[0], jnp.where(sub_wide < 4, r[1], r[2])),
                jnp.where(sub_wide < 2, r[2], r[3]),
                jnp.where(sub_wide < 4, r[3], r[4]),
                r[4],
                r[4],
            ],
            axis=0,
        )
        if a == b:
            terms = ((a, 2.0 * spread_rows * heavy[a]),)
        else:
            terms = ((a, spread_rows * heavy[b]), (b, spread_rows * heavy[a]))
        for n, term in terms:
            totals[n] = term if totals[n] is None else totals[n] + term
    for n in range(4):
        dmom[n * MROWS : (n + 1) * MROWS, :] = totals[n]

    for n in range(4):
        slopes = {}
        for t in TRIPLES:
            at = n * MROWS + INDEX[t]
            slopes[t] = jnp.where(
                even,
                rows_of(dmom[at : at + 1, 0:LANES], 8),
                rows_of(dmom[at : at + 1, LANES:], 8),
            )
        for t in sorted(TRIPLES, key=lambda t: -t[2]):
            if t[2] > 1:
                low, left, right = reduced(t)
                slopes[low] = slopes[low] + slopes[t]
                slopes[left] = slopes[left] - slopes[t]
                slopes[right] = slopes[right] - slopes[t]
        for t in BASIS:
            tiles[n * len(BASIS) + PLACE[t]] = slopes[t]

    part8 = sub8 & 3
    half_block = sub8 >> 2
    own_total = [None] * 3

    def pair_gradients(begin, end):
        count = (end - begin) // 8
        at = slice(begin, end)
        weighted = [geom[n, at, :] for n in range(4)]
        unit = [geom[8 + c, at, :] for c in range(3)]
        ux, uy, uz = unit
        found = []
        for w in range(2):
            size = 4 - w
            value_x = slope_x = slope_y = graded_x = None
            for p in range(size, -1, -1):
                value = slope = graded = None
                for q in range(size - p, -1, -1):
                    total = graded_total = None
                    for n in range(3, -1, -1):
                        b = over(tiles[n * len(BASIS) + PLACE[(p, q, w)]], count)
                        term = b * weighted[n]
                        total = term if total is None else total + term
                        if n > 0:
                            graded_total = total if graded_total is None else graded_total + total
                    value, slope = horner(uy, value, slope, total)
                    graded = graded_total if graded is None else graded * uy + graded_total
                value_x, slope_x = horner(ux, value_x, slope_x, value)
                graded_x = graded if graded_x is None else graded_x * ux + graded
                if slope is not None:
                    slope_y = slope if slope_y is None else slope_y * ux + slope
            found.append((value_x, slope_x, slope_y, graded_x))
        scaled = geom[6, at, :]
        tangent = [
            (found[0][1] + uz * found[1][1]) * scaled,
            (found[0][2] + uz * found[1][2]) * scaled,
            found[1][0] * scaled,
        ]
        along = geom[4, at, :] * (found[0][0] + uz * found[1][0])
        along = along + geom[5, at, :] * (found[0][3] + uz * found[1][3])
        along = along - (ux * tangent[0] + uy * tangent[1] + uz * tangent[2])
        for c in range(3):
            g = tangent[c] + unit[c] * along
            grads[c, at, :] = g
            for i in range(count):
                row = g[8 * i : 8 * i + 8, :]
                own_total[c] = row if own_total[c] is None else own_total[c] + row

    def spread_sums(begin, end):
        columns = []
        for r in range(begin, min(end, 52)):
            gx, gy, gz = (rows_of(grads[c, r : r + 1, :], 8) for c in range(3))
            value = jnp.where(part8 == 0, gx, jnp.where(part8 == 1, gy, gz))
            hi = value.astype(BF16).astype(F32)
            lo = value - hi
            place_of = rows_of(blk[r : r + 1, :], 8) - half_block
            masks = [place_of == 2 * i for i in range(3)]
            columns.append(
                jnp.concatenate(
                    [jnp.where(mask, x, 0.0) for x in (hi, lo) for mask in masks], axis=0
                ).astype(BF16)
            )
        last = min(end, 52)
        return mm_nt(jnp.concatenate(columns, axis=1), onehot[:, begin * LANES : last * LANES])

    spread = jnp.zeros((48, LANES), F32)
    pair_gradients(*CHUNKS[0])
    for at in range(len(CHUNKS)):
        if at + 1 < len(CHUNKS):
            pair_gradients(*CHUNKS[at + 1])
        spread = spread + spread_sums(*CHUNKS[at])
    for c in range(3):
        total = own_total[c] + pltpu.roll(own_total[c], 4, 0)
        total = total + pltpu.roll(total, 2, 0)
        for h in range(2):
            own_sum[h, c : c + 1, :] = total[h : h + 1, :]
    spread = spread[0:24, :] + spread[24:48, :]
    first = spread[0:8, :]
    second = spread[8:16, :]
    third = spread[16:24, :]
    swapped = pltpu.roll(second, 4, 0)
    grad0 = first - own_sum[0]
    m_send[0] = jnp.where(lane8 < 64, third, swapped)[0:4, :]
    m_send[1] = second[0:4, :]
    m_send[2] = jnp.where(lane8 < 64, swapped, second)[0:4, :]
    p_send[...] = jnp.where(sub8 < 3, grad0, 0.0)
    start(backward[0:6] + backward[8:10])
    start(backward[6:8] + backward[10:11])
    start(extra[1:3])

    rows = [c_send[i : i + 1, :].astype(jnp.int32) for i in range(7)]
    for i, row in enumerate(rows):
        at = slice(i * LANES, (i + 1) * LANES)
        hot0[:, at] = jnp.where(column128 == rows_of(row, LANES), 1.0, 0.0).astype(BF16)
        if i < 2:
            hot1[:, at] = jnp.where(
                column128 + LANES == rows_of(row, LANES), 1.0, 0.0
            ).astype(BF16)
    out_energy[:, 0:LANES] = energy[:, 0:LANES] * keep0
    out_energy[:, LANES:] = energy[:, LANES:] * keep1
    grad1 = pltpu.roll(first, 4, 0) - own_sum[1]

    receive(((3, -1, 4),))
    slots = rows_of(c_recv[7:8, :], LANES).T[0:16, :]
    for i in range(8):
        row = lane_row.astype(F32) if i == 7 else c_recv[i : i + 1, :]
        arr_hot[:, i * LANES : (i + 1) * LANES] = jnp.where(
            rows_of(row, 16) == slots, 1.0, 0.0
        ).astype(BF16)

    receive(((6, 0, 4), (4, 1, 3), (5, -1, 7), (7, -2, 3)))

    def piece(ds, dt, part=0):
        return b_recv[slot(ds, dt), part]

    def pieces_of(tiles):
        back = jnp.concatenate(tiles, axis=1)
        hi = back.astype(BF16).astype(F32)
        return jnp.concatenate([hi, back - hi], axis=0).astype(BF16)

    back = pieces_of(
        (
            piece(-1, 0),
            piece(1, 0),
            piece(-1, 1),
            piece(1, 1, 1),
            piece(-1, -1),
            piece(1, -1, 1),
            between(piece(0, 1, 1), piece(0, -1, 1)),
        )
    )
    added0 = mm_nt(back, hot0[...])
    added1 = mm_nt(back[:, 0 : 2 * LANES], hot1[...])
    arriving = pieces_of(
        (
            m_send[0],
            piece(2, 0),
            piece(0, 1),
            piece(2, 1),
            piece(0, -1),
            piece(2, -1),
            between(piece(1, 1), piece(1, -1)),
            p_recv[0:4, :],
        )
    )
    added2 = mm_nt(arriving, arr_hot[...])
    force0 = -(grad0 + added0 + pltpu.roll(added0, 4, 0))[0:3, :]
    velocity0 = half_velocity[:, 0:LANES] + kick_factor * force0
    force1 = -(grad1 + added1 + pltpu.roll(added1, 4, 0))[0:3, :]
    velocity1 = half_velocity[:, LANES:] + kick_factor * force1
    force2 = -(added2 + pltpu.roll(added2, 4, 0))[0:3, :]
    state = w_recv[...]
    out_vel[:, 0:LANES] = velocity0 * rows_of(keep0, 3)
    out_force[:, 0:LANES] = force0 * rows_of(keep0, 3)
    out_vel[:, LANES:] = velocity1 * rows_of(keep1, 3)
    out_force[:, LANES:] = force1 * rows_of(keep1, 3)
    for q, value in enumerate(
        (state[0:3, 0:16], state[4:7, 0:16] + kick_factor * force2, force2)
    ):
        out_arr[q] = jnp.where(s_me < n_shock - 1, value, 0.0)
    drain()


def kept(shape):
    return pltpu.VMEM(shape, F32)


def in_place(x):
    return pltpu.with_memory_space_constraint(x, pltpu.VMEM)


def finish(*refs):
    for i in range(5):
        refs[5 + i][...] = refs[i][...]


def whole_step(n_shock, n_trans, *args):
    (disp, vel, force, beta, alpha, live, trans_idx, shock_idx, block, lane, leave, count) = args
    inputs = (
        disp,
        vel,
        force,
        beta.reshape(1, 50),
        alpha,
        trans_idx,
        shock_idx,
        block,
        lane,
        leave.reshape(1, 16),
        jnp.asarray(lattice_rows()),
        jnp.asarray(weight_rows()),
        jnp.asarray(selection_table(), BF16),
    )
    vmem = pl.BlockSpec(memory_space=pltpu.VMEM)
    tile = (8, LANES)
    half_tile = (4, LANES)
    shapes = ((3, 256), (3, 256), (3, 256), (1, 256), (3, 3, 16))
    outs = pl.pallas_call(
        functools.partial(kernel, n_shock, n_trans),
        out_shape=tuple(kept(shape) for shape in shapes),
        in_specs=[pl.BlockSpec(memory_space=pltpu.HBM)] * N_IN
        + [pl.BlockSpec(memory_space=pltpu.SMEM)] * 2,
        out_specs=(vmem,) * 5,
        scratch_shapes=[
            pltpu.VMEM(x.shape, x.dtype) for x in inputs
        ]
        + [
            pltpu.SemaphoreType.DMA((N_IN,)),
            pltpu.VMEM((2, *half_tile), F32),
            pltpu.VMEM((2, *half_tile), F32),
            pltpu.VMEM((NEAR, 2, *half_tile), F32),
            pltpu.VMEM((3, *half_tile), F32),
            pltpu.VMEM((len(DIRS), 2, *half_tile), F32),
            pltpu.VMEM(tile, F32),
            pltpu.VMEM(tile, F32),
            pltpu.VMEM(tile, F32),
            pltpu.VMEM(tile, F32),
            pltpu.VMEM(tile, F32),
            pltpu.VMEM(tile, F32),
            pltpu.SemaphoreType.DMA((4,)),
            pltpu.SemaphoreType.DMA((8,)),
            pltpu.VMEM((7, *tile), F32),
            pltpu.VMEM((ROWS, LANES), jnp.int32),
            pltpu.VMEM((ROWS, LANES), jnp.int32),
            pltpu.VMEM(tile, jnp.int32),
            pltpu.VMEM((4, *tile), F32),
            pltpu.VMEM((3, ROWS, LANES), F32),
            pltpu.VMEM((11, ROWS, LANES), F32),
            pltpu.VMEM((4 * len(BASIS), *tile), F32),
            pltpu.VMEM((4 * MROWS, 256), F32),
            pltpu.VMEM((4 * MROWS, 256), F32),
            pltpu.VMEM((3 * DROWS, 10 * MROWS), BF16),
            pltpu.VMEM((DROWS, 256), F32),
            pltpu.VMEM((LANES, 26 * 256), BF16),
            pltpu.VMEM((LANES, LANES), F32),
            pltpu.VMEM((LANES, 7 * LANES), BF16),
            pltpu.VMEM((LANES, 2 * LANES), BF16),
            pltpu.VMEM((16, 8 * LANES), BF16),
            pltpu.VMEM((3, ROWS, LANES), F32),
            pltpu.VMEM((2, *tile), F32),
        ],
        compiler_params=pltpu.CompilerParams(collective_id=0, has_side_effects=True),
        name="whole_step",
    )(*inputs, live, count)
    outs = [in_place(x) for x in outs]
    outs = pl.pallas_call(
        finish,
        out_shape=tuple(jax.ShapeDtypeStruct(shape, F32) for shape in shapes),
        in_specs=[vmem] * 5,
        out_specs=(vmem,) * 5,
        name="finish",
    )(*outs)
    return outs[0], outs[1], outs[2], outs[3].reshape(256), outs[4]


def solution(mesh):
    split_1 = P(None, ("shock", "trans"))
    split_0 = P(("shock", "trans"))
    in_specs = (
        split_1,
        split_1,
        split_1,
        P(),
        P(),
        split_0,
        split_1,
        split_1,
        split_1,
        split_1,
        split_0,
        split_0,
    )
    out_specs = (split_1, split_1, split_1, split_0, P(None, None, ("shock", "trans")))
    body = functools.partial(whole_step, mesh.shape["shock"], mesh.shape["trans"])
    return jax.shard_map(body, mesh=mesh, in_specs=in_specs, out_specs=out_specs, check_vma=False)
```
